8 devices in a mesh: data: 1 (over z), seq: 2 (over y), stage: 4 (over x, core).
Axes of the slice: x: 2, y: 2, z: 1, core: 2. Of those that a mesh axis runs over, the one named last changes fastest.
Arguments:
- x_init: float32 [2, 256, 48], P('data', 'seq')
- h_init: bfloat16 [3, 2, 256, 768], P(None, 'data', 'seq')
- w_in: bfloat16 [48, 768], replicated
- w_out: bfloat16 [768, 48], replicated
- w_qkv: bfloat16 [4, 768, 2304], P('stage')
- w_o: bfloat16 [4, 12, 64, 768], P('stage')
- w_up: bfloat16 [4, 768, 3072], P('stage')
- w_down: bfloat16 [4, 3072, 768], P('stage')
- ada_mod: float32 [4, 4, 6, 768], P(None, 'stage')
- alpha_coef: float32 [4], replicated
- beta_coef: float32 [4], replicated
Outputs:
- output 1: float32 [2, 256, 48], P('data', 'seq')
- output 2: bfloat16 [4, 2, 256, 768], P('stage', 'data', 'seq')
All inputs are finite; a program needn't handle non-finite values.
Results may differ from the reference program's by a relative error of at most 0.02.
Values are sent between devices in bfloat16 or wider.
A program may use at most 1 GiB of HBM per device.

```python
import jax
import jax.numpy as jnp
from jax import lax

BATCH_ROWS = 2
NUM_TOKENS = 256
LATENT_DIM = 48
MODEL_DIM = 768
NUM_HEADS = 12
NUM_STAGES = 4
STAGE_LAYERS = 1
NUM_STEPS = 4

HEAD_DIM = MODEL_DIM // NUM_HEADS
NUM_LAYERS = NUM_STAGES * STAGE_LAYERS
LN_EPS = 1e-6


def setup_inputs(seed: int = 0, part: int = 0) -> dict:
    base_key = jax.random.key(seed)
    part_keys = jax.random.split(jax.random.fold_in(base_key, part), 2)
    shared_keys = jax.random.split(base_key, 10)
    x_init = jax.random.normal(part_keys[0], (BATCH_ROWS, NUM_TOKENS, LATENT_DIM), jnp.float32)
    h_init = jax.random.normal(part_keys[1], (NUM_STAGES - 1, BATCH_ROWS, NUM_TOKENS, MODEL_DIM), jnp.float32).astype(jnp.bfloat16)
    w_in = (jax.random.normal(shared_keys[0], (LATENT_DIM, MODEL_DIM), jnp.float32) * LATENT_DIM ** -0.5).astype(jnp.bfloat16)
    w_out = (jax.random.normal(shared_keys[1], (MODEL_DIM, LATENT_DIM), jnp.float32) * MODEL_DIM ** -0.5).astype(jnp.bfloat16)
    qk_part = jax.random.normal(shared_keys[2], (NUM_LAYERS, MODEL_DIM, 2 * MODEL_DIM), jnp.float32) * (2.0 * MODEL_DIM ** -0.5)
    v_part = jax.random.normal(shared_keys[3], (NUM_LAYERS, MODEL_DIM, MODEL_DIM), jnp.float32) * MODEL_DIM ** -0.5
    w_qkv = jnp.concatenate([qk_part, v_part], axis=2).astype(jnp.bfloat16)
    w_o = (jax.random.normal(shared_keys[4], (NUM_LAYERS, NUM_HEADS, HEAD_DIM, MODEL_DIM), jnp.float32) * MODEL_DIM ** -0.5).astype(jnp.bfloat16)
    w_up = (jax.random.normal(shared_keys[5], (NUM_LAYERS, MODEL_DIM, 4 * MODEL_DIM), jnp.float32) * MODEL_DIM ** -0.5).astype(jnp.bfloat16)
    w_down = (jax.random.normal(shared_keys[6], (NUM_LAYERS, 4 * MODEL_DIM, MODEL_DIM), jnp.float32) * (4 * MODEL_DIM) ** -0.5).astype(jnp.bfloat16)
    gate_size = NUM_LAYERS ** -0.5
    spread = jnp.array([0.2, 0.2, 0.4 * gate_size, 0.2, 0.2, 0.4 * gate_size], jnp.float32)
    offset = jnp.array([0.0, 0.0, 0.8 * gate_size, 0.0, 0.0, 0.8 * gate_size], jnp.float32)
    ada_mod = jax.random.normal(shared_keys[7], (NUM_STEPS, NUM_LAYERS, 6, MODEL_DIM), jnp.float32) * spread[:, None] + offset[:, None]
    alpha_coef = jax.random.uniform(shared_keys[8], (NUM_STEPS,), jnp.float32, 0.5, 0.8)
    beta_coef = jax.random.uniform(shared_keys[9], (NUM_STEPS,), jnp.float32, 0.3, 0.6)
    return {"x_init": x_init, "h_init": h_init, "w_in": w_in, "w_out": w_out, "w_qkv": w_qkv, "w_o": w_o, "w_up": w_up, "w_down": w_down, "ada_mod": ada_mod, "alpha_coef": alpha_coef, "beta_coef": beta_coef}


def layer_norm(hidden):
    mean_val = jnp.mean(hidden, axis=-1, keepdims=True)
    centered = hidden - mean_val
    variance = jnp.mean(centered * centered, axis=-1, keepdims=True)
    return centered * lax.rsqrt(variance + LN_EPS)


def dit_block(hidden, w_qkv, w_o, w_up, w_down, mod_row):
    tokens_all = BATCH_ROWS * NUM_TOKENS
    normed = (layer_norm(hidden) * (1.0 + mod_row[1]) + mod_row[0]).astype(jnp.bfloat16)
    qkv_proj = jnp.dot(normed.reshape(tokens_all, MODEL_DIM), w_qkv, preferred_element_type=jnp.float32)
    qkv_proj = qkv_proj.astype(jnp.bfloat16).astype(jnp.float32).reshape(BATCH_ROWS, NUM_TOKENS, 3, NUM_HEADS, HEAD_DIM)
    scores = jnp.einsum("bqhf,bkhf->bhqk", qkv_proj[:, :, 0], qkv_proj[:, :, 1]) * HEAD_DIM ** -0.5
    attn_probs = jax.nn.softmax(scores, axis=-1).astype(jnp.bfloat16).astype(jnp.float32)
    attended = jnp.einsum("bhqk,bkhf->bqhf", attn_probs, qkv_proj[:, :, 2]).astype(jnp.bfloat16)
    attn_out = jnp.dot(attended.reshape(tokens_all, MODEL_DIM), w_o.reshape(MODEL_DIM, MODEL_DIM), preferred_element_type=jnp.float32)
    hidden = hidden + mod_row[2] * attn_out.reshape(BATCH_ROWS, NUM_TOKENS, MODEL_DIM)
    normed = (layer_norm(hidden) * (1.0 + mod_row[4]) + mod_row[3]).astype(jnp.bfloat16)
    up_proj = jax.nn.gelu(jnp.dot(normed.reshape(tokens_all, MODEL_DIM), w_up, preferred_element_type=jnp.float32), approximate=True).astype(jnp.bfloat16)
    mlp_out = jnp.dot(up_proj, w_down, preferred_element_type=jnp.float32)
    return hidden + mod_row[5] * mlp_out.reshape(BATCH_ROWS, NUM_TOKENS, MODEL_DIM)


def run_stage(stage_args):
    stage_in, qkv_s, o_s, up_s, down_s, mod_s = stage_args

    def layer_step(hidden, layer_args):
        w_qkv, w_o, w_up, w_down, mod_row = layer_args
        return dit_block(hidden, w_qkv, w_o, w_up, w_down, mod_row), None

    return lax.scan(layer_step, stage_in.astype(jnp.float32), (qkv_s, o_s, up_s, down_s, mod_s))[0]


def reference(x_init, h_init, w_in, w_out, w_qkv, w_o, w_up, w_down, ada_mod, alpha_coef, beta_coef):
    qkv_st = w_qkv.reshape(NUM_STAGES, STAGE_LAYERS, MODEL_DIM, 3 * MODEL_DIM)
    o_st = w_o.reshape(NUM_STAGES, STAGE_LAYERS, NUM_HEADS, HEAD_DIM, MODEL_DIM)
    up_st = w_up.reshape(NUM_STAGES, STAGE_LAYERS, MODEL_DIM, 4 * MODEL_DIM)
    down_st = w_down.reshape(NUM_STAGES, STAGE_LAYERS, 4 * MODEL_DIM, MODEL_DIM)

    def step_fn(state_carry, step_args):
        latent, prev_outs = state_carry
        mod_step, alpha_k, beta_k = step_args
        embedded = jnp.dot(latent.astype(jnp.bfloat16).reshape(BATCH_ROWS * NUM_TOKENS, LATENT_DIM), w_in, preferred_element_type=jnp.float32)
        embedded = embedded.astype(jnp.bfloat16).reshape(1, BATCH_ROWS, NUM_TOKENS, MODEL_DIM)
        stage_ins = jnp.concatenate([embedded, prev_outs[:-1]], axis=0)
        mod_st = mod_step.reshape(NUM_STAGES, STAGE_LAYERS, 6, MODEL_DIM)
        stage_outs = lax.map(run_stage, (stage_ins, qkv_st, o_st, up_st, down_st, mod_st)).astype(jnp.bfloat16)
        noise_pred = jnp.dot(stage_outs[-1].reshape(BATCH_ROWS * NUM_TOKENS, MODEL_DIM), w_out, preferred_element_type=jnp.float32)
        latent = alpha_k * latent + beta_k * noise_pred.reshape(BATCH_ROWS, NUM_TOKENS, LATENT_DIM)
        return (latent, stage_outs), None

    first_outs = jnp.concatenate([h_init, jnp.zeros((1, BATCH_ROWS, NUM_TOKENS, MODEL_DIM), jnp.bfloat16)], axis=0)
    final_carry = lax.scan(step_fn, (x_init, first_outs), (ada_mod, alpha_coef, beta_coef))[0]
    return final_carry[0], final_carry[1]
```

```python
import functools

import jax
import jax.numpy as jnp
from jax import lax
from jax.experimental import pallas as pl
from jax.experimental.pallas import tpu as pltpu
from jax.sharding import PartitionSpec as P

LN_EPS = 1e-6
MESH = pl.DeviceIdType.MESH
BF16 = jnp.bfloat16
F32 = jnp.float32

STEPS = 4
STAGES = 4
DIM = 768
FF = 3072
HEADS = 12
HD = 64
ROWS = 128
LAT = 48
EXP2_SCALE = HD ** -0.5 * 1.4426950408889634
GELU_C0 = 0.7978845608028654
GELU_C1 = GELU_C0 * 0.044715


def layer_norm(hidden):
    mean_val = jnp.mean(hidden, axis=-1, keepdims=True)
    centered = hidden - mean_val
    variance = jnp.mean(centered * centered, axis=-1, keepdims=True)
    return centered * lax.rsqrt(variance + LN_EPS)


def gelu(val):
    half = 0.5 * val
    return half + half * jnp.tanh(val * (GELU_C0 + GELU_C1 * (val * val)))


def mm(lhs, rhs):
    return jnp.dot(lhs, rhs, preferred_element_type=F32)


def kernel(x_hbm, h_hbm, win_hbm, wout_hbm, wqkv_hbm, wo_hbm, wup_hbm, wdown_hbm, mod_hbm, alpha_ref, beta_ref,
           xo_ref, ho_hbm,
           wqkv, wo, wup, wdown, win, wout, mod, xraw, hin, outb, xbt, xbt_out, xs, xfin_out, xfin,
           hres, unorm, qkv, vt, attn, act,
           w_sem, small_sem, init_send, init_recv, st_send, st_recv, x_send, x_recv, xf_send, xf_recv, ho_sem, ho_send, ho_recv):
    y = lax.axis_index("seq")
    s = lax.axis_index("stage")
    z = lax.axis_index("data")
    oy = 1 - y
    is_first = s == 0
    is_last = s == STAGES - 1
    uses_x = jnp.logical_or(is_first, is_last)
    h_idx = jnp.maximum(s - 1, 0)

    def local(src, dst, sem):
        return pltpu.make_async_copy(src, dst, sem)

    def remote(src, dst, ssem, rsem, yy, ss):
        return pltpu.make_async_remote_copy(src_ref=src, dst_ref=dst, send_sem=ssem, recv_sem=rsem,
                                            device_id=(z, yy, ss), device_id_type=MESH)

    cp_h = local(h_hbm.at[h_idx, y], hin.at[0, 1], small_sem.at[0])
    cp_x = local(x_hbm.at[y], xraw.at[1], small_sem.at[1])
    cp_mod = local(mod_hbm, mod, small_sem.at[2])
    cp_win = local(win_hbm, win, small_sem.at[3])
    cp_wout = local(wout_hbm, wout, small_sem.at[4])
    cp_wqkv = local(wqkv_hbm, wqkv, w_sem.at[0])
    cp_wo = local(wo_hbm, wo, w_sem.at[1])
    cp_wup = local(wup_hbm, wup, w_sem.at[2])
    cp_wdown = local(wdown_hbm, wdown, w_sem.at[3])
    rc_h = remote(h_hbm.at[h_idx, oy], hin.at[0, 0], init_send.at[0], init_recv.at[0], oy, s)
    rc_x = remote(x_hbm.at[oy], xraw.at[0], init_send.at[1], init_recv.at[1], oy, s)

    @pl.when(jnp.logical_not(is_first))
    def _():
        cp_h.start()

    cp_x.start()
    cp_mod.start()
    cp_win.start()
    cp_wout.start()
    cp_wqkv.start()

    barrier = pltpu.get_barrier_semaphore()
    for dy in range(2):
        for ds in range(STAGES):
            if dy == 0 and ds == 0:
                continue
            pl.semaphore_signal(barrier, inc=1, device_id=(z, (y + dy) % 2, (s + ds) % STAGES), device_id_type=MESH)
    pl.semaphore_wait(barrier, 2 * STAGES - 1)

    @pl.when(jnp.logical_not(is_first))
    def _():
        rc_h.start()

    @pl.when(uses_x)
    def _():
        rc_x.start()

    cp_wo.start()
    cp_wup.start()
    cp_wdown.start()
    cp_x.wait()
    cp_mod.wait()
    cp_win.wait()
    cp_wout.wait()

    @pl.when(jnp.logical_not(is_first))
    def _():
        cp_h.wait()
        rc_h.wait_recv()

    @pl.when(uses_x)
    def _():
        rc_x.wait_recv()
        for c in range(2):
            xs[c] = xraw[c]
            xbt[0, c] = xraw[c].astype(BF16)

    cp_wqkv.wait()

    def stage_copy(k, c):
        return remote(outb.at[k, c], hin.at[k + 1, c], st_send.at[k, c], st_recv.at[k, c], y, s + 1)

    def x_copy(k, c):
        return remote(xbt_out.at[k, c], xbt.at[k + 1, c], x_send.at[k, c], x_recv.at[k, c], y, 0)

    def step(k, _):
        kprev = jnp.maximum(k - 1, 0)
        for c in range(2):
            @pl.when(jnp.logical_and(k > 0, jnp.logical_not(is_first)))
            def _():
                stage_copy(kprev, c).wait_recv()

            @pl.when(is_first)
            def _():
                @pl.when(k > 0)
                def _():
                    x_copy(kprev, c).wait_recv()
                xb = xbt[k, c].astype(F32).T.astype(BF16)
                hin[k, c] = mm(xb, win[...]).astype(BF16)

            h0 = hin[k, c].astype(F32)
            unorm[c] = (layer_norm(h0) * (1.0 + mod[k, 1]) + mod[k, 0]).astype(BF16)
            for n in range(0, 3 * DIM, 768):
                qkv[pl.ds(c * ROWS, ROWS), n:n + 768] = mm(unorm[c], wqkv[:, n:n + 768]).astype(BF16)

        for p in range(HEADS // 2):
            v2 = qkv[:, 2 * DIM + p * 128:2 * DIM + (p + 1) * 128]
            vt[pl.ds(p * 128, 128), :] = v2.T

        @pl.when(k == 0)
        def _():
            cp_wo.wait()
            cp_wup.wait()
            cp_wdown.wait()

        lane = lax.broadcasted_iota(jnp.int32, (ROWS, 128), 1)
        for c in range(2):
            rows = pl.ds(c * ROWS, ROWS)
            for p in range(HEADS // 2):
                q2 = qkv[rows, p * 128:(p + 1) * 128]
                k2 = qkv[:, DIM + p * 128:DIM + (p + 1) * 128]
                zero = jnp.zeros_like(q2)
                qq = jnp.concatenate([jnp.where(lane < HD, q2, zero), jnp.where(lane < HD, zero, q2)], axis=0)
                st = lax.dot_general(k2, qq, (((1,), (1,)), ((), ())), preferred_element_type=F32)
                mx = jnp.max(st, axis=0, keepdims=True)
                ex = jnp.exp2((st - mx) * EXP2_SCALE)
                inv = 1.0 / jnp.sum(ex, axis=0, keepdims=True)
                pt = (ex * inv).astype(BF16)
                ot = mm(vt[pl.ds(p * 128, 128), :], pt)
                o2 = jnp.concatenate([ot[:HD, :ROWS], ot[HD:, ROWS:]], axis=0)
                attn[:, p * 128:(p + 1) * 128] = o2.T.astype(BF16)
            h1 = hin[k, c].astype(F32) + mod[k, 2] * mm(attn[...], wo[...])
            hres[...] = h1
            u2 = (layer_norm(h1) * (1.0 + mod[k, 4]) + mod[k, 3]).astype(BF16)
            unorm[c] = u2
            for n in range(0, FF, 512):
                act[:, n:n + 512] = gelu(mm(unorm[c], wup[:, n:n + 512])).astype(BF16)
            h2 = hres[...] + mod[k, 5] * mm(act[...], wdown[...])
            out = h2.astype(BF16)
            outb[k, c] = out

            @pl.when(jnp.logical_and(k < STEPS - 1, jnp.logical_not(is_last)))
            def _():
                stage_copy(k, c).start()

            if c == 0:
                @pl.when(k == STEPS - 1)
                def _():
                    remote(outb.at[k, c], ho_hbm.at[y], ho_send, ho_recv, oy, s).start()
            else:
                @pl.when(k == STEPS - 1)
                def _():
                    local(outb.at[k, c], ho_hbm.at[y], ho_sem).start()

            @pl.when(is_last)
            def _():
                eps = lax.dot_general(wout[...], outb[k, c], (((1,), (1,)), ((), ())), preferred_element_type=F32)
                xn = alpha_ref[k] * xs[c] + beta_ref[k] * eps
                xs[c] = xn

                @pl.when(k < STEPS - 1)
                def _():
                    xbt_out[k, c] = xn.astype(BF16)
                    x_copy(k, c).start()

                @pl.when(k == STEPS - 1)
                def _():
                    xfin_out[c] = xn
                    if c == 0:
                        for t in range(STAGES):
                            remote(xfin_out.at[c], xfin.at[y], xf_send.at[t], xf_recv.at[y], oy, t).start()
                    else:
                        for t in range(STAGES - 1):
                            remote(xfin_out.at[c], xfin.at[y], xf_send.at[STAGES + t], xf_recv.at[y], y, t).start()
                        xfin[y] = xn
        return 0

    lax.fori_loop(0, STEPS, step, 0)

    remote(xfin_out.at[0], xfin.at[oy], xf_send.at[0], xf_recv.at[oy], oy, s).wait_recv()

    @pl.when(jnp.logical_not(is_last))
    def _():
        remote(xfin_out.at[0], xfin.at[y], xf_send.at[0], xf_recv.at[y], y, s).wait_recv()

    for b in range(2):
        xo_ref[b] = xfin[b]

    @pl.when(is_last)
    def _():
        for t in range(STAGES):
            remote(xfin_out.at[0], xfin.at[y], xf_send.at[t], xf_recv.at[y], oy, t).wait_send()
        for t in range(STAGES - 1):
            remote(xfin_out.at[1], xfin.at[y], xf_send.at[STAGES + t], xf_recv.at[y], y, t).wait_send()
        for k in range(STEPS - 1):
            for c in range(2):
                x_copy(k, c).wait_send()

    @pl.when(jnp.logical_not(is_last))
    def _():
        for k in range(STEPS - 1):
            for c in range(2):
                stage_copy(k, c).wait_send()

    @pl.when(jnp.logical_not(is_first))
    def _():
        rc_h.wait_send()

    @pl.when(uses_x)
    def _():
        rc_x.wait_send()

    local(outb.at[STEPS - 1, 1], ho_hbm.at[y], ho_sem).wait()
    last = remote(outb.at[STEPS - 1, 0], ho_hbm.at[oy], ho_send, ho_recv, oy, s)
    last.wait_send()
    last.wait_recv()


def solution(mesh):
    hbm = pl.BlockSpec(memory_space=pltpu.HBM)
    smem = pl.BlockSpec(memory_space=pltpu.SMEM)
    vmem = pl.BlockSpec(memory_space=pltpu.VMEM)
    dma = pltpu.SemaphoreType.DMA
    scratch = [
        pltpu.VMEM((DIM, 3 * DIM), BF16),
        pltpu.VMEM((DIM, DIM), BF16),
        pltpu.VMEM((DIM, FF), BF16),
        pltpu.VMEM((FF, DIM), BF16),
        pltpu.VMEM((LAT, DIM), BF16),
        pltpu.VMEM((LAT, DIM), BF16),
        pltpu.VMEM((STEPS, 6, 1, DIM), F32),
        pltpu.VMEM((2, LAT, ROWS), F32),
        pltpu.VMEM((STEPS, 2, ROWS, DIM), BF16),
        pltpu.VMEM((STEPS, 2, ROWS, DIM), BF16),
        pltpu.VMEM((STEPS, 2, LAT, ROWS), BF16),
        pltpu.VMEM((STEPS, 2, LAT, ROWS), BF16),
        pltpu.VMEM((2, LAT, ROWS), F32),
        pltpu.VMEM((2, LAT, ROWS), F32),
        pltpu.VMEM((2, LAT, ROWS), F32),
        pltpu.VMEM((ROWS, DIM), F32),
        pltpu.VMEM((2, ROWS, DIM), BF16),
        pltpu.VMEM((2 * ROWS, 3 * DIM), BF16),
        pltpu.VMEM((DIM, 2 * ROWS), BF16),
        pltpu.VMEM((ROWS, DIM), BF16),
        pltpu.VMEM((ROWS, FF), BF16),
        dma((4,)), dma((5,)), dma((2,)), dma((2,)),
        dma((STEPS - 1, 2)), dma((STEPS - 1, 2)), dma((STEPS - 1, 2)), dma((STEPS - 1, 2)),
        dma((2 * STAGES - 1,)), dma((2,)), dma, dma, dma,
    ]

    def device_fn(x_init, h_init, w_in, w_out, w_qkv, w_o, w_up, w_down, ada_mod, alpha_coef, beta_coef):
        call = pl.pallas_call(
            kernel,
            name="dit_steps",
            out_shape=(jax.ShapeDtypeStruct((2, LAT, ROWS), F32), jax.ShapeDtypeStruct((2, ROWS, DIM), BF16)),
            in_specs=[hbm] * 9 + [smem] * 2,
            out_specs=(vmem, hbm),
            scratch_shapes=scratch,
            compiler_params=pltpu.CompilerParams(collective_id=0, has_side_effects=True, vmem_limit_bytes=60 * 1024 * 1024),
        )
        x_final, h_final = call(x_init.swapaxes(1, 2), h_init, w_in, w_out.T, w_qkv.reshape(DIM, 3 * DIM), w_o.reshape(DIM, DIM),
                                w_up.reshape(DIM, FF), w_down.reshape(FF, DIM), ada_mod.swapaxes(1, 2), alpha_coef, beta_coef)
        return x_final.swapaxes(1, 2), h_final[None]

    weight_spec = P("stage", None, None)
    return jax.shard_map(
        device_fn,
        mesh=mesh,
        in_specs=(P("data", "seq", None), P(None, "data", "seq", None), P(), P(), weight_spec, P("stage", None, None, None), weight_spec, weight_spec, P(None, "stage", None, None), P(), P()),
        out_specs=(P("data", "seq", None), P("stage", "data", "seq", None)),
        check_vma=False,
    )
```

```python
import functools

import jax
import jax.numpy as jnp
from jax import lax
from jax.experimental import pallas as pl
from jax.experimental.pallas import tpu as pltpu
from jax.sharding import PartitionSpec as P

LN_EPS = 1e-6
MESH = pl.DeviceIdType.MESH
BF16 = jnp.bfloat16
F32 = jnp.float32

STEPS = 4
STAGES = 4
DIM = 768
FF = 3072
HEADS = 12
HD = 64
ROWS = 128
LAT = 48
EXP2_SCALE = HD ** -0.5 * 1.4426950408889634
GELU_C0 = 0.7978845608028654
GELU_C1 = GELU_C0 * 0.044715


def layer_norm(hidden):
    mean_val = jnp.mean(hidden, axis=-1, keepdims=True)
    centered = hidden - mean_val
    variance = jnp.mean(centered * centered, axis=-1, keepdims=True)
    return centered * lax.rsqrt(variance + LN_EPS)


def gelu(val):
    half = 0.5 * val
    return half + half * jnp.tanh(val * (GELU_C0 + GELU_C1 * (val * val)))


def mm(lhs, rhs):
    return jnp.dot(lhs, rhs, preferred_element_type=F32)


def interleave(*streams):
    order = []
    for idx, pieces in enumerate(streams):
        for pos in range(len(pieces)):
            order.append(((pos + 0.5) / len(pieces), idx, pos))
    for _, idx, pos in sorted(order):
        streams[idx][pos]()


def kernel(x_hbm, h_hbm, win_hbm, wout_hbm, wqkv_hbm, wo_hbm, wup_hbm, wdown_hbm, mod_hbm, alpha_ref, beta_ref,
           xo_ref, ho_hbm,
           wqkv, wo, wup, wdown, win, wout, mod, xraw, hin, outb, xbt, xbt_out, xs, xfin_out, xfin,
           hres, unorm, qs, ks, vt, attn, act, s_a, s_b, p_a, p_b,
           w_sem, small_sem, init_send, init_recv, st_send, st_recv, x_send, x_recv, xf_send, xf_recv, ho_sem, ho_send, ho_recv, go_sem):
    y = lax.axis_index("seq")
    s = lax.axis_index("stage")
    z = lax.axis_index("data")
    oy = 1 - y
    is_first = s == 0
    is_last = s == STAGES - 1
    is_waiter = s == STAGES - 2
    uses_x = jnp.logical_or(is_first, is_last)
    h_idx = jnp.maximum(s - 1, 0)

    def local(src, dst, sem):
        return pltpu.make_async_copy(src, dst, sem)

    def remote(src, dst, ssem, rsem, yy, ss):
        return pltpu.make_async_remote_copy(src_ref=src, dst_ref=dst, send_sem=ssem, recv_sem=rsem,
                                            device_id=(z, yy, ss), device_id_type=MESH)

    cp_h = local(h_hbm.at[h_idx, y], hin.at[0, 1], small_sem.at[0])
    cp_x = local(x_hbm.at[y], xraw.at[1], small_sem.at[1])
    cp_mod = local(mod_hbm, mod, small_sem.at[2])
    cp_win = local(win_hbm, win, small_sem.at[3])
    cp_wout = local(wout_hbm, wout, small_sem.at[4])
    cp_wqkv = [local(wqkv_hbm.at[:, pl.ds(j * DIM, DIM)], wqkv.at[j], w_sem.at[j]) for j in range(3)]
    cp_rest = [local(wo_hbm, wo, w_sem.at[3])]
    cp_rest += [local(wup_hbm.at[:, pl.ds(j * DIM, DIM)], wup.at[j], w_sem.at[4 + j]) for j in range(4)]
    cp_rest += [local(wdown_hbm, wdown, w_sem.at[8])]
    rc_h = remote(h_hbm.at[h_idx, oy], hin.at[0, 0], init_send.at[0], init_recv.at[0], oy, s)
    rc_x = remote(x_hbm.at[oy], xraw.at[0], init_send.at[1], init_recv.at[1], oy, s)

    @pl.when(jnp.logical_not(is_first))
    def _():
        cp_h.start()

    cp_x.start()
    cp_mod.start()
    cp_win.start()
    cp_wout.start()
    for j in (1, 2, 0):
        cp_wqkv[j].start()

    barrier = pltpu.get_barrier_semaphore()
    for dy in range(2):
        for ds in range(STAGES):
            if dy == 0 and ds == 0:
                continue
            pl.semaphore_signal(barrier, inc=1, device_id=(z, (y + dy) % 2, (s + ds) % STAGES), device_id_type=MESH)
    pl.semaphore_wait(barrier, 2 * STAGES - 1)

    @pl.when(uses_x)
    def _():
        rc_x.start()

    @pl.when(jnp.logical_not(jnp.logical_or(is_first, is_waiter)))
    def _():
        rc_h.start()

    for cp in cp_rest:
        cp.start()

    @pl.when(is_last)
    def _():
        rc_h.wait_send()
        pl.semaphore_signal(go_sem, inc=1, device_id=(z, y, s - 1), device_id_type=MESH)

    @pl.when(is_waiter)
    def _():
        pl.semaphore_wait(go_sem, 1)
        rc_h.start()

    cp_x.wait()
    cp_mod.wait()
    cp_win.wait()
    cp_wout.wait()

    @pl.when(jnp.logical_not(is_first))
    def _():
        cp_h.wait()

    @pl.when(uses_x)
    def _():
        xs[1] = xraw[1]
        xbt[0, 1] = xraw[1].astype(BF16)

    for cp in cp_wqkv:
        cp.wait()

    def stage_copy(k, c):
        return remote(outb.at[k, c], hin.at[k + 1, c], st_send.at[k, c], st_recv.at[k, c], y, s + 1)

    def x_copy(k, c):
        return remote(xbt_out.at[k, c], xbt.at[k + 1, c], x_send.at[k, c], x_recv.at[k, c], y, 0)

    lane = lax.broadcasted_iota(jnp.int32, (ROWS, 128), 1)
    PAIRS = HEADS // 2
    LNB = 32

    def embed(k, c):
        @pl.when(is_first)
        def _():
            xb = xbt[k, c].astype(F32).T.astype(BF16)
            hin[k, c] = mm(xb, win[...]).astype(BF16)

    def ln1_pieces(k, c):
        def piece(r):
            def run():
                rows = pl.ds(r, LNB)
                h0 = hin[k, c, rows].astype(F32)
                unorm[c, rows] = (layer_norm(h0) * (1.0 + mod[k, 1]) + mod[k, 0]).astype(BF16)
            return run
        return [piece(r) for r in range(0, ROWS, LNB)]

    def q_pieces(c):
        def piece(n):
            def run():
                qs[c, :, n:n + 256] = mm(unorm[c], wqkv[0, :, n:n + 256]).astype(BF16)
            return run
        return [piece(n) for n in range(0, DIM, 256)]

    def k_pieces(c):
        def piece(n):
            def run():
                ks[c, :, n:n + 256] = mm(unorm[c], wqkv[1, :, n:n + 256]).astype(BF16)
            return run
        return [piece(n) for n in range(0, DIM, 256)]

    def v_pieces(c):
        def piece(n):
            def run():
                val = mm(unorm[c], wqkv[2, :, n:n + 256])
                vt[c, n:n + 256, :] = val.T.astype(BF16)
            return run
        return [piece(n) for n in range(0, DIM, 256)]

    def attn_pieces(c):
        s_scr, p_scr = (s_a, s_b), (p_a, p_b)

        def scores(p):
            cols = slice(p * 128, (p + 1) * 128)
            q2 = qs[c, :, cols]
            zero = jnp.zeros_like(q2)
            qq = jnp.concatenate([jnp.where(lane < HD, q2, zero), jnp.where(lane < HD, zero, q2)], axis=0)
            k2 = jnp.concatenate([ks[0, :, cols], ks[1, :, cols]], axis=0)
            s_scr[p % 2][...] = lax.dot_general(k2, qq, (((1,), (1,)), ((), ())), preferred_element_type=F32)

        def softmax(p, half):
            cols = slice(half * ROWS, (half + 1) * ROWS)
            st = s_scr[p % 2][:, cols]
            mx = jnp.max(st, axis=0, keepdims=True)
            ex = jnp.exp2((st - mx) * EXP2_SCALE)
            inv = 1.0 / jnp.sum(ex, axis=0, keepdims=True)
            p_scr[p % 2][:, cols] = (ex * inv).astype(BF16)

        def values(p):
            cols = slice(p * 128, (p + 1) * 128)
            v2 = jnp.concatenate([vt[0, cols, :], vt[1, cols, :]], axis=1)
            ot = mm(v2, p_scr[p % 2][...])
            o2 = jnp.concatenate([ot[:HD, :ROWS], ot[HD:, ROWS:]], axis=0)
            attn[c, :, cols] = o2.T.astype(BF16)

        pieces = [functools.partial(scores, 0)]
        for p in range(PAIRS):
            if p + 1 < PAIRS:
                pieces.append(functools.partial(scores, p + 1))
            pieces.append(functools.partial(softmax, p, 0))
            pieces.append(functools.partial(softmax, p, 1))
            pieces.append(functools.partial(values, p))
        return pieces

    def wo_pieces(c):
        def piece(n):
            def run():
                hres[c, :, n:n + 256] = mm(attn[c], wo[:, n:n + 256])
            return run
        return [piece(n) for n in range(0, DIM, 256)]

    def ln2_pieces(k, c):
        def piece(r):
            def run():
                rows = pl.ds(r, LNB)
                h1 = hin[k, c, rows].astype(F32) + mod[k, 2] * hres[c, rows]
                hres[c, rows] = h1
                unorm[c, rows] = (layer_norm(h1) * (1.0 + mod[k, 4]) + mod[k, 3]).astype(BF16)
            return run
        return [piece(r) for r in range(0, ROWS, LNB)]

    def up_pieces(c):
        def piece(n):
            def run():
                j, m = divmod(n, DIM)
                act[c, :, n:n + 256] = gelu(mm(unorm[c], wup[j, :, m:m + 256])).astype(BF16)
            return run
        return [piece(n) for n in range(0, FF, 256)]

    def down_pieces(k, c):
        def store(n, res):
            out = hres[c, :, n:n + 256] + mod[k, 5][:, n:n + 256] * res
            outb[k, c, :, n:n + 256] = out.astype(BF16)

        def full(n):
            def run():
                store(n, mm(act[c], wdown[:, n:n + 256]))
            return run

        def halves(n):
            def run():
                lo = mm(act[c, :, :FF // 2], wdown[:FF // 2, n:n + 256])
                hi = mm(act[c, :, FF // 2:], wdown[FF // 2:, n:n + 256])
                store(n, lo + hi)
            return run
        return [full(0), full(256), halves(512)]

    def finish(k, c):
        @pl.when(jnp.logical_and(k < STEPS - 1, jnp.logical_not(is_last)))
        def _():
            stage_copy(k, c).start()

        if c == 0:
            @pl.when(k == STEPS - 1)
            def _():
                remote(outb.at[k, c], ho_hbm.at[y], ho_send, ho_recv, oy, s).start()
        else:
            @pl.when(k == STEPS - 1)
            def _():
                local(outb.at[k, c], ho_hbm.at[y], ho_sem).start()

        @pl.when(is_last)
        def _():
            eps = lax.dot_general(wout[...], outb[k, c], (((1,), (1,)), ((), ())), preferred_element_type=F32)
            xn = alpha_ref[k] * xs[c] + beta_ref[k] * eps
            xs[c] = xn

            @pl.when(k < STEPS - 1)
            def _():
                xbt_out[k, c] = xn.astype(BF16)
                x_copy(k, c).start()

            @pl.when(k == STEPS - 1)
            def _():
                xfin_out[c] = xn
                if c == 0:
                    for t in range(STAGES):
                        remote(xfin_out.at[c], xfin.at[y], xf_send.at[t], xf_recv.at[y], oy, t).start()
                else:
                    for t in range(STAGES - 1):
                        remote(xfin_out.at[c], xfin.at[y], xf_send.at[STAGES + t], xf_recv.at[y], y, t).start()
                    xfin[y] = xn

    def step(k, _):
        kprev = jnp.maximum(k - 1, 0)
        ca = jnp.where(k == 0, 1, 0)
        cb = 1 - ca

        @pl.when(jnp.logical_and(k > 0, jnp.logical_not(is_first)))
        def _():
            stage_copy(kprev, ca).wait_recv()

        @pl.when(jnp.logical_and(k > 0, is_first))
        def _():
            x_copy(kprev, ca).wait_recv()

        embed(k, ca)
        interleave(ln1_pieces(k, ca))
        interleave(k_pieces(ca) + v_pieces(ca))

        @pl.when(jnp.logical_and(k > 0, jnp.logical_not(is_first)))
        def _():
            stage_copy(kprev, cb).wait_recv()

        @pl.when(jnp.logical_and(k > 0, is_first))
        def _():
            x_copy(kprev, cb).wait_recv()

        @pl.when(k == 0)
        def _():
            @pl.when(jnp.logical_not(is_first))
            def _():
                rc_h.wait_recv()

            @pl.when(uses_x)
            def _():
                rc_x.wait_recv()
                xs[0] = xraw[0]
                xbt[0, 0] = xraw[0].astype(BF16)

            for cp in cp_rest:
                cp.wait()

        embed(k, cb)
        interleave(q_pieces(ca), ln1_pieces(k, cb))
        interleave(k_pieces(cb))
        interleave(q_pieces(cb))
        interleave(v_pieces(cb))
        interleave(attn_pieces(0))
        att1 = attn_pieces(1)
        interleave(wo_pieces(0) + ln2_pieces(k, 0), att1[:8])
        interleave(up_pieces(0))
        interleave(down_pieces(k, 0), att1[8:])
        finish(k, 0)
        interleave(wo_pieces(1))
        interleave(ln2_pieces(k, 1))
        interleave(up_pieces(1))
        interleave(down_pieces(k, 1))
        finish(k, 1)
        return 0

    lax.fori_loop(0, STEPS, step, 0)

    remote(xfin_out.at[0], xfin.at[oy], xf_send.at[0], xf_recv.at[oy], oy, s).wait_recv()

    @pl.when(jnp.logical_not(is_last))
    def _():
        remote(xfin_out.at[0], xfin.at[y], xf_send.at[0], xf_recv.at[y], y, s).wait_recv()

    for b in range(2):
        xo_ref[b] = xfin[b]

    @pl.when(is_last)
    def _():
        for t in range(STAGES):
            remote(xfin_out.at[0], xfin.at[y], xf_send.at[t], xf_recv.at[y], oy, t).wait_send()
        for t in range(STAGES - 1):
            remote(xfin_out.at[1], xfin.at[y], xf_send.at[STAGES + t], xf_recv.at[y], y, t).wait_send()
        for k in range(STEPS - 1):
            for c in range(2):
                x_copy(k, c).wait_send()

    @pl.when(jnp.logical_not(is_last))
    def _():
        for k in range(STEPS - 1):
            for c in range(2):
                stage_copy(k, c).wait_send()

    @pl.when(jnp.logical_not(jnp.logical_or(is_first, is_last)))
    def _():
        rc_h.wait_send()

    @pl.when(uses_x)
    def _():
        rc_x.wait_send()

    local(outb.at[STEPS - 1, 1], ho_hbm.at[y], ho_sem).wait()
    last = remote(outb.at[STEPS - 1, 0], ho_hbm.at[oy], ho_send, ho_recv, oy, s)
    last.wait_send()
    last.wait_recv()


def solution(mesh):
    hbm = pl.BlockSpec(memory_space=pltpu.HBM)
    smem = pl.BlockSpec(memory_space=pltpu.SMEM)
    vmem = pl.BlockSpec(memory_space=pltpu.VMEM)
    dma = pltpu.SemaphoreType.DMA
    scratch = [
        pltpu.VMEM((3, DIM, DIM), BF16),
        pltpu.VMEM((DIM, DIM), BF16),
        pltpu.VMEM((4, DIM, DIM), BF16),
        pltpu.VMEM((FF, DIM), BF16),
        pltpu.VMEM((LAT, DIM), BF16),
        pltpu.VMEM((LAT, DIM), BF16),
        pltpu.VMEM((STEPS, 6, 1, DIM), F32),
        pltpu.VMEM((2, LAT, ROWS), F32),
        pltpu.VMEM((STEPS, 2, ROWS, DIM), BF16),
        pltpu.VMEM((STEPS, 2, ROWS, DIM), BF16),
        pltpu.VMEM((STEPS, 2, LAT, ROWS), BF16),
        pltpu.VMEM((STEPS, 2, LAT, ROWS), BF16),
        pltpu.VMEM((2, LAT, ROWS), F32),
        pltpu.VMEM((2, LAT, ROWS), F32),
        pltpu.VMEM((2, LAT, ROWS), F32),
        pltpu.VMEM((2, ROWS, DIM), F32),
        pltpu.VMEM((2, ROWS, DIM), BF16),
        pltpu.VMEM((2, ROWS, DIM), BF16),
        pltpu.VMEM((2, ROWS, DIM), BF16),
        pltpu.VMEM((2, DIM, ROWS), BF16),
        pltpu.VMEM((2, ROWS, DIM), BF16),
        pltpu.VMEM((2, ROWS, FF), BF16),
        pltpu.VMEM((2 * ROWS, 2 * ROWS), F32),
        pltpu.VMEM((2 * ROWS, 2 * ROWS), F32),
        pltpu.VMEM((2 * ROWS, 2 * ROWS), BF16),
        pltpu.VMEM((2 * ROWS, 2 * ROWS), BF16),
        dma((9,)), dma((5,)), dma((2,)), dma((2,)),
        dma((STEPS - 1, 2)), dma((STEPS - 1, 2)), dma((STEPS - 1, 2)), dma((STEPS - 1, 2)),
        dma((2 * STAGES - 1,)), dma((2,)), dma, dma, dma, pltpu.SemaphoreType.REGULAR,
    ]

    def device_fn(x_init, h_init, w_in, w_out, w_qkv, w_o, w_up, w_down, ada_mod, alpha_coef, beta_coef):
        call = pl.pallas_call(
            kernel,
            name="dit_steps",
            out_shape=(jax.ShapeDtypeStruct((2, LAT, ROWS), F32), jax.ShapeDtypeStruct((2, ROWS, DIM), BF16)),
            in_specs=[hbm] * 9 + [smem] * 2,
            out_specs=(vmem, hbm),
            scratch_shapes=scratch,
            compiler_params=pltpu.CompilerParams(collective_id=0, has_side_effects=True, vmem_limit_bytes=60 * 1024 * 1024),
        )
        x_final, h_final = call(x_init.swapaxes(1, 2), h_init, w_in, w_out.T, w_qkv.reshape(DIM, 3 * DIM), w_o.reshape(DIM, DIM),
                                w_up.reshape(DIM, FF), w_down.reshape(FF, DIM), ada_mod.swapaxes(1, 2), alpha_coef, beta_coef)
        return x_final.swapaxes(1, 2), h_final[None]

    weight_spec = P("stage", None, None)
    return jax.shard_map(
        device_fn,
        mesh=mesh,
        in_specs=(P("data", "seq", None), P(None, "data", "seq", None), P(), P(), weight_spec, P("stage", None, None, None), weight_spec, weight_spec, P(None, "stage", None, None), P(), P()),
        out_specs=(P("data", "seq", None), P("stage", "data", "seq", None)),
        check_vma=False,
    )
```

```python
import functools

import jax
import jax.numpy as jnp
from jax import lax
from jax.experimental import pallas as pl
from jax.experimental.pallas import tpu as pltpu
from jax.sharding import PartitionSpec as P

LN_EPS = 1e-6
MESH = pl.DeviceIdType.MESH
BF16 = jnp.bfloat16
F32 = jnp.float32

STEPS = 4
STAGES = 4
DIM = 768
FF = 3072
HEADS = 12
HD = 64
ROWS = 128
LAT = 48
EXP2_SCALE = HD ** -0.5 * 1.4426950408889634
GELU_C0 = 0.7978845608028654
GELU_C1 = GELU_C0 * 0.044715


def layer_norm(hidden):
    mean_val = jnp.mean(hidden, axis=-1, keepdims=True)
    centered = hidden - mean_val
    variance = jnp.mean(centered * centered, axis=-1, keepdims=True)
    return centered * lax.rsqrt(variance + LN_EPS)


def gelu(val):
    half = 0.5 * val
    return half + half * jnp.tanh(val * (GELU_C0 + GELU_C1 * (val * val)))


def mm(lhs, rhs):
    return jnp.dot(lhs, rhs, preferred_element_type=F32)


def interleave(*streams):
    order = []
    for idx, pieces in enumerate(streams):
        for pos in range(len(pieces)):
            order.append(((pos + 0.5) / len(pieces), idx, pos))
    for _, idx, pos in sorted(order):
        streams[idx][pos]()


def kernel(x_hbm, h_hbm, win_hbm, wout_hbm, wqkv_hbm, wo_hbm, wup_hbm, wdown_hbm, mod_hbm, alpha_ref, beta_ref,
           xo_ref, ho_ref,
           wqkv, wo, wup, wdown, win, wout, mod, xraw, xsend, hsend, hin, outb, xbt, xbt_out, xs, xfin_out, xfin,
           hres, unorm, qs, ks, vt, attn, act, s_a, s_b, p_a, p_b,
           w_sem, small_sem, init_send, init_recv, st_send, st_recv, x_send, x_recv, xf_send, xf_recv, ho_send, ho_recv, go_sem):
    y = lax.axis_index("seq")
    s = lax.axis_index("stage")
    z = lax.axis_index("data")
    oy = 1 - y
    is_first = s == 0
    is_last = s == STAGES - 1
    is_waiter = s == STAGES - 2
    uses_x = jnp.logical_or(is_first, is_last)
    h_idx = jnp.maximum(s - 1, 0)

    def local(src, dst, sem):
        return pltpu.make_async_copy(src, dst, sem)

    def remote(src, dst, ssem, rsem, yy, ss):
        return pltpu.make_async_remote_copy(src_ref=src, dst_ref=dst, send_sem=ssem, recv_sem=rsem,
                                            device_id=(z, yy, ss), device_id_type=MESH)

    cp_h = local(h_hbm.at[h_idx, y], hin.at[0, 1], small_sem.at[0])
    cp_x = local(x_hbm.at[y], xraw.at[1], small_sem.at[1])
    cp_mod = local(mod_hbm, mod, small_sem.at[2])
    cp_win = local(win_hbm, win, small_sem.at[3])
    cp_wout = local(wout_hbm, wout, small_sem.at[4])
    cp_wqkv = [local(wqkv_hbm.at[:, pl.ds(j * DIM, DIM)], wqkv.at[j], w_sem.at[j]) for j in range(3)]
    cp_rest = [local(wo_hbm, wo, w_sem.at[3])]
    cp_rest += [local(wup_hbm.at[:, pl.ds(j * DIM, DIM)], wup.at[j], w_sem.at[4 + j]) for j in range(4)]
    cp_rest += [local(wdown_hbm, wdown, w_sem.at[8])]
    cp_hs = local(h_hbm.at[h_idx, oy], hsend, small_sem.at[5])
    cp_xs = local(x_hbm.at[oy], xsend, small_sem.at[6])
    rc_h = remote(hsend, hin.at[0, 0], init_send.at[0], init_recv.at[0], oy, s)
    rc_x = remote(xsend, xraw.at[0], init_send.at[1], init_recv.at[1], oy, s)

    @pl.when(jnp.logical_not(is_first))
    def _():
        cp_hs.start()
        cp_h.start()

    cp_xs.start()
    cp_x.start()
    cp_mod.start()
    cp_win.start()
    cp_wout.start()
    for j in (1, 2, 0):
        cp_wqkv[j].start()

    barrier = pltpu.get_barrier_semaphore()
    for dy in range(2):
        for ds in range(STAGES):
            if dy == 0 and ds == 0:
                continue
            pl.semaphore_signal(barrier, inc=1, device_id=(z, (y + dy) % 2, (s + ds) % STAGES), device_id_type=MESH)
    cp_xs.wait()

    @pl.when(jnp.logical_not(is_first))
    def _():
        cp_hs.wait()

    pl.semaphore_wait(barrier, 2 * STAGES - 1)

    @pl.when(uses_x)
    def _():
        rc_x.start()

    @pl.when(jnp.logical_not(jnp.logical_or(is_first, is_waiter)))
    def _():
        rc_h.start()

    for cp in cp_rest:
        cp.start()

    @pl.when(is_last)
    def _():
        rc_h.wait_send()
        pl.semaphore_signal(go_sem, inc=1, device_id=(z, y, s - 1), device_id_type=MESH)

    @pl.when(is_waiter)
    def _():
        pl.semaphore_wait(go_sem, 1)
        rc_h.start()

    cp_x.wait()
    cp_mod.wait()
    cp_win.wait()
    cp_wout.wait()

    @pl.when(jnp.logical_not(is_first))
    def _():
        cp_h.wait()

    @pl.when(uses_x)
    def _():
        xs[1] = xraw[1]
        xbt[0, 1] = xraw[1].astype(BF16)

    for cp in cp_wqkv:
        cp.wait()

    def stage_copy(k, c):
        return remote(outb.at[k, c], hin.at[k + 1, c], st_send.at[k, c], st_recv.at[k, c], y, s + 1)

    def x_copy(k, c):
        return remote(xbt_out.at[k, c], xbt.at[k + 1, c], x_send.at[k, c], x_recv.at[k, c], y, 0)

    lane = lax.broadcasted_iota(jnp.int32, (ROWS, 128), 1)
    PAIRS = HEADS // 2
    LNB = 32

    def embed(k, c):
        @pl.when(is_first)
        def _():
            xb = xbt[k, c].astype(F32).T.astype(BF16)
            hin[k, c] = mm(xb, win[...]).astype(BF16)

    def ln1_pieces(k, c):
        def piece(r):
            def run():
                rows = pl.ds(r, LNB)
                h0 = hin[k, c, rows].astype(F32)
                unorm[c, rows] = (layer_norm(h0) * (1.0 + mod[k, 1]) + mod[k, 0]).astype(BF16)
            return run
        return [piece(r) for r in range(0, ROWS, LNB)]

    def q_pieces(c):
        def piece(n):
            def run():
                qs[c, :, n:n + 256] = mm(unorm[c], wqkv[0, :, n:n + 256]).astype(BF16)
            return run
        return [piece(n) for n in range(0, DIM, 256)]

    def k_pieces(c):
        def piece(n):
            def run():
                ks[c, :, n:n + 256] = mm(unorm[c], wqkv[1, :, n:n + 256]).astype(BF16)
            return run
        return [piece(n) for n in range(0, DIM, 256)]

    def v_pieces(c):
        def piece(n):
            def run():
                val = mm(unorm[c], wqkv[2, :, n:n + 256])
                vt[c, n:n + 256, :] = val.T.astype(BF16)
            return run
        return [piece(n) for n in range(0, DIM, 256)]

    def attn_pieces(c):
        s_scr, p_scr = (s_a, s_b), (p_a, p_b)

        def scores(p):
            cols = slice(p * 128, (p + 1) * 128)
            q2 = qs[c, :, cols]
            zero = jnp.zeros_like(q2)
            qq = jnp.concatenate([jnp.where(lane < HD, q2, zero), jnp.where(lane < HD, zero, q2)], axis=0)
            k2 = jnp.concatenate([ks[0, :, cols], ks[1, :, cols]], axis=0)
            s_scr[p % 2][...] = lax.dot_general(k2, qq, (((1,), (1,)), ((), ())), preferred_element_type=F32)

        def softmax(p, half):
            cols = slice(half * ROWS, (half + 1) * ROWS)
            st = s_scr[p % 2][:, cols]
            mx = jnp.max(st, axis=0, keepdims=True)
            ex = jnp.exp2((st - mx) * EXP2_SCALE)
            inv = 1.0 / jnp.sum(ex, axis=0, keepdims=True)
            p_scr[p % 2][:, cols] = (ex * inv).astype(BF16)

        def values(p):
            cols = slice(p * 128, (p + 1) * 128)
            v2 = jnp.concatenate([vt[0, cols, :], vt[1, cols, :]], axis=1)
            ot = mm(v2, p_scr[p % 2][...])
            o2 = jnp.concatenate([ot[:HD, :ROWS], ot[HD:, ROWS:]], axis=0)
            attn[c, :, cols] = o2.T.astype(BF16)

        pieces = [functools.partial(scores, 0)]
        for p in range(PAIRS):
            if p + 1 < PAIRS:
                pieces.append(functools.partial(scores, p + 1))
            pieces.append(functools.partial(softmax, p, 0))
            pieces.append(functools.partial(softmax, p, 1))
            pieces.append(functools.partial(values, p))
        return pieces

    def wo_pieces(c):
        def piece(n):
            def run():
                hres[c, :, n:n + 256] = mm(attn[c], wo[:, n:n + 256])
            return run
        return [piece(n) for n in range(0, DIM, 256)]

    def ln2_pieces(k, c):
        def piece(r):
            def run():
                rows = pl.ds(r, LNB)
                h1 = hin[k, c, rows].astype(F32) + mod[k, 2] * hres[c, rows]
                hres[c, rows] = h1
                unorm[c, rows] = (layer_norm(h1) * (1.0 + mod[k, 4]) + mod[k, 3]).astype(BF16)
            return run
        return [piece(r) for r in range(0, ROWS, LNB)]

    def up_pieces(c):
        def piece(n):
            def run():
                j, m = divmod(n, DIM)
                act[c, :, n:n + 256] = gelu(mm(unorm[c], wup[j, :, m:m + 256])).astype(BF16)
            return run
        return [piece(n) for n in range(0, FF, 256)]

    def down_pieces(k, c):
        def store(n, res):
            out = hres[c, :, n:n + 256] + mod[k, 5][:, n:n + 256] * res
            outb[k, c, :, n:n + 256] = out.astype(BF16)

        def full(n):
            def run():
                store(n, mm(act[c], wdown[:, n:n + 256]))
            return run

        def halves(n):
            def run():
                lo = mm(act[c, :, :FF // 2], wdown[:FF // 2, n:n + 256])
                hi = mm(act[c, :, FF // 2:], wdown[FF // 2:, n:n + 256])
                store(n, lo + hi)
            return run
        return [full(0), full(256), halves(512)]

    def finish(k, c):
        @pl.when(jnp.logical_and(k < STEPS - 1, jnp.logical_not(is_last)))
        def _():
            stage_copy(k, c).start()

        if c == 0:
            @pl.when(k == STEPS - 1)
            def _():
                remote(outb.at[k, c], ho_ref.at[y], ho_send, ho_recv, oy, s).start()
        else:
            @pl.when(k == STEPS - 1)
            def _():
                ho_ref[y] = outb[k, c]

        @pl.when(is_last)
        def _():
            eps = lax.dot_general(wout[...], outb[k, c], (((1,), (1,)), ((), ())), preferred_element_type=F32)
            xn = alpha_ref[k] * xs[c] + beta_ref[k] * eps
            xs[c] = xn

            @pl.when(k < STEPS - 1)
            def _():
                xbt_out[k, c] = xn.astype(BF16)
                x_copy(k, c).start()

            @pl.when(k == STEPS - 1)
            def _():
                xfin_out[c] = xn
                if c == 0:
                    for t in range(STAGES):
                        remote(xfin_out.at[c], xfin.at[y], xf_send.at[t], xf_recv.at[y], oy, t).start()
                else:
                    for t in range(STAGES - 1):
                        remote(xfin_out.at[c], xfin.at[y], xf_send.at[STAGES + t], xf_recv.at[y], y, t).start()
                    xfin[y] = xn

    def step(k, _):
        kprev = jnp.maximum(k - 1, 0)
        ca = jnp.where(k == 0, 1, 0)
        cb = 1 - ca

        @pl.when(jnp.logical_and(k > 0, jnp.logical_not(is_first)))
        def _():
            stage_copy(kprev, ca).wait_recv()

        @pl.when(jnp.logical_and(k > 0, is_first))
        def _():
            x_copy(kprev, ca).wait_recv()

        embed(k, ca)
        interleave(ln1_pieces(k, ca))
        interleave(k_pieces(ca) + v_pieces(ca))

        @pl.when(jnp.logical_and(k > 0, jnp.logical_not(is_first)))
        def _():
            stage_copy(kprev, cb).wait_recv()

        @pl.when(jnp.logical_and(k > 0, is_first))
        def _():
            x_copy(kprev, cb).wait_recv()

        @pl.when(k == 0)
        def _():
            @pl.when(jnp.logical_not(is_first))
            def _():
                rc_h.wait_recv()

            @pl.when(uses_x)
            def _():
                rc_x.wait_recv()
                xs[0] = xraw[0]
                xbt[0, 0] = xraw[0].astype(BF16)

            for cp in cp_rest:
                cp.wait()

        embed(k, cb)
        interleave(q_pieces(ca), ln1_pieces(k, cb))
        interleave(k_pieces(cb))
        interleave(q_pieces(cb))
        interleave(v_pieces(cb))
        interleave(attn_pieces(0))
        att1 = attn_pieces(1)
        interleave(wo_pieces(0) + ln2_pieces(k, 0), att1[:8])
        interleave(up_pieces(0))
        interleave(down_pieces(k, 0), att1[8:])
        finish(k, 0)
        interleave(wo_pieces(1))
        interleave(ln2_pieces(k, 1))
        interleave(up_pieces(1))
        interleave(down_pieces(k, 1))
        finish(k, 1)
        return 0

    lax.fori_loop(0, STEPS, step, 0)

    remote(xfin_out.at[0], xfin.at[oy], xf_send.at[0], xf_recv.at[oy], oy, s).wait_recv()

    @pl.when(jnp.logical_not(is_last))
    def _():
        remote(xfin_out.at[0], xfin.at[y], xf_send.at[0], xf_recv.at[y], y, s).wait_recv()

    for b in range(2):
        xo_ref[b] = xfin[b]

    @pl.when(is_last)
    def _():
        for t in range(STAGES):
            remote(xfin_out.at[0], xfin.at[y], xf_send.at[t], xf_recv.at[y], oy, t).wait_send()
        for t in range(STAGES - 1):
            remote(xfin_out.at[1], xfin.at[y], xf_send.at[STAGES + t], xf_recv.at[y], y, t).wait_send()
        for k in range(STEPS - 1):
            for c in range(2):
                x_copy(k, c).wait_send()

    @pl.when(jnp.logical_not(is_last))
    def _():
        for k in range(STEPS - 1):
            for c in range(2):
                stage_copy(k, c).wait_send()

    @pl.when(jnp.logical_not(jnp.logical_or(is_first, is_last)))
    def _():
        rc_h.wait_send()

    @pl.when(uses_x)
    def _():
        rc_x.wait_send()

    last = remote(outb.at[STEPS - 1, 0], ho_ref.at[oy], ho_send, ho_recv, oy, s)
    last.wait_send()
    last.wait_recv()


def writer(x_ref, h_ref, xo_ref, ho_ref, sems):
    copies = [pltpu.make_async_copy(x_ref, xo_ref, sems.at[0]), pltpu.make_async_copy(h_ref, ho_ref, sems.at[1])]
    for copy in copies:
        copy.start()
    for copy in copies:
        copy.wait()


def solution(mesh):
    hbm = pl.BlockSpec(memory_space=pltpu.HBM)
    smem = pl.BlockSpec(memory_space=pltpu.SMEM)
    vmem = pl.BlockSpec(memory_space=pltpu.VMEM)
    dma = pltpu.SemaphoreType.DMA
    scratch = [
        pltpu.VMEM((3, DIM, DIM), BF16),
        pltpu.VMEM((DIM, DIM), BF16),
        pltpu.VMEM((4, DIM, DIM), BF16),
        pltpu.VMEM((FF, DIM), BF16),
        pltpu.VMEM((LAT, DIM), BF16),
        pltpu.VMEM((LAT, DIM), BF16),
        pltpu.VMEM((STEPS, 6, 1, DIM), F32),
        pltpu.VMEM((2, LAT, ROWS), F32),
        pltpu.VMEM((LAT, ROWS), F32),
        pltpu.VMEM((ROWS, DIM), BF16),
        pltpu.VMEM((STEPS, 2, ROWS, DIM), BF16),
        pltpu.VMEM((STEPS, 2, ROWS, DIM), BF16),
        pltpu.VMEM((STEPS, 2, LAT, ROWS), BF16),
        pltpu.VMEM((STEPS, 2, LAT, ROWS), BF16),
        pltpu.VMEM((2, LAT, ROWS), F32),
        pltpu.VMEM((2, LAT, ROWS), F32),
        pltpu.VMEM((2, LAT, ROWS), F32),
        pltpu.VMEM((2, ROWS, DIM), F32),
        pltpu.VMEM((2, ROWS, DIM), BF16),
        pltpu.VMEM((2, ROWS, DIM), BF16),
        pltpu.VMEM((2, ROWS, DIM), BF16),
        pltpu.VMEM((2, DIM, ROWS), BF16),
        pltpu.VMEM((2, ROWS, DIM), BF16),
        pltpu.VMEM((2, ROWS, FF), BF16),
        pltpu.VMEM((2 * ROWS, 2 * ROWS), F32),
        pltpu.VMEM((2 * ROWS, 2 * ROWS), F32),
        pltpu.VMEM((2 * ROWS, 2 * ROWS), BF16),
        pltpu.VMEM((2 * ROWS, 2 * ROWS), BF16),
        dma((9,)), dma((7,)), dma((2,)), dma((2,)),
        dma((STEPS - 1, 2)), dma((STEPS - 1, 2)), dma((STEPS - 1, 2)), dma((STEPS - 1, 2)),
        dma((2 * STAGES - 1,)), dma((2,)), dma, dma, pltpu.SemaphoreType.REGULAR,
    ]

    def device_fn(x_init, h_init, w_in, w_out, w_qkv, w_o, w_up, w_down, ada_mod, alpha_coef, beta_coef):
        call = pl.pallas_call(
            kernel,
            name="dit_steps",
            out_shape=(pltpu.VMEM((2, LAT, ROWS), F32), pltpu.VMEM((2, ROWS, DIM), BF16)),
            in_specs=[hbm] * 9 + [smem] * 2,
            out_specs=(vmem, vmem),
            scratch_shapes=scratch,
            compiler_params=pltpu.CompilerParams(collective_id=0, has_side_effects=True, vmem_limit_bytes=58 * 1024 * 1024),
        )
        x_final, h_final = call(x_init.swapaxes(1, 2), h_init, w_in, w_out.T, w_qkv.reshape(DIM, 3 * DIM), w_o.reshape(DIM, DIM),
                                w_up.reshape(DIM, FF), w_down.reshape(FF, DIM), ada_mod.swapaxes(1, 2), alpha_coef, beta_coef)
        x_final, h_final = pl.pallas_call(
            writer,
            name="write_out",
            out_shape=(jax.ShapeDtypeStruct(x_final.shape, F32), jax.ShapeDtypeStruct(h_final.shape, BF16)),
            in_specs=[vmem] * 2,
            out_specs=(hbm, hbm),
            scratch_shapes=[dma((2,))],
        )(pltpu.with_memory_space_constraint(x_final, pltpu.VMEM), pltpu.with_memory_space_constraint(h_final, pltpu.VMEM))
        return x_final.swapaxes(1, 2), h_final[None]

    weight_spec = P("stage", None, None)
    return jax.shard_map(
        device_fn,
        mesh=mesh,
        in_specs=(P("data", "seq", None), P(None, "data", "seq", None), P(), P(), weight_spec, P("stage", None, None, None), weight_spec, weight_spec, P(None, "stage", None, None), P(), P()),
        out_specs=(P("data", "seq", None), P("stage", "data", "seq", None)),
        check_vma=False,
    )
```

```python
import functools

import jax
import jax.numpy as jnp
from jax import lax
from jax.experimental import pallas as pl
from jax.experimental.pallas import tpu as pltpu
from jax.sharding import PartitionSpec as P

LN_EPS = 1e-6
MESH = pl.DeviceIdType.MESH
BF16 = jnp.bfloat16
F32 = jnp.float32

STEPS = 4
STAGES = 4
DIM = 768
FF = 3072
HEADS = 12
HD = 64
ROWS = 128
LAT = 48
EXP2_SCALE = HD ** -0.5 * 1.4426950408889634
GELU_C0 = 0.7978845608028654
GELU_C1 = GELU_C0 * 0.044715


def layer_norm(hidden):
    mean_val = jnp.mean(hidden, axis=-1, keepdims=True)
    centered = hidden - mean_val
    variance = jnp.mean(centered * centered, axis=-1, keepdims=True)
    return centered * lax.rsqrt(variance + LN_EPS)


def gelu(val):
    half = 0.5 * val
    return half + half * jnp.tanh(val * (GELU_C0 + GELU_C1 * (val * val)))


def mm(lhs, rhs):
    return jnp.dot(lhs, rhs, preferred_element_type=F32)


def interleave(*streams):
    order = []
    for idx, pieces in enumerate(streams):
        for pos in range(len(pieces)):
            order.append(((pos + 0.5) / len(pieces), idx, pos))
    for _, idx, pos in sorted(order):
        streams[idx][pos]()


def kernel(x_hbm, h_hbm, win_hbm, wout_hbm, wqkv_hbm, wo_hbm, wup_hbm, wdown_hbm, mod_hbm, alpha_ref, beta_ref,
           xo_ref, ho_ref,
           wqkv, wo, wup, wdown, win, wout, mod, xraw, xsend, hsend, hin, outb, xbt, xbt_out, xs, xfin_out, xfin,
           hres, unorm, qs, ks, vt, attn, act, s_scr, p_scr,
           w_sem, small_sem, init_send, init_recv, st_send, st_recv, x_send, x_recv, xf_send, xf_recv, ho_send, ho_recv, go_sem):
    y = lax.axis_index("seq")
    s = lax.axis_index("stage")
    z = lax.axis_index("data")
    oy = 1 - y
    is_first = s == 0
    is_last = s == STAGES - 1
    is_waiter = s == STAGES - 2
    uses_x = jnp.logical_or(is_first, is_last)
    h_idx = jnp.maximum(s - 1, 0)

    def local(src, dst, sem):
        return pltpu.make_async_copy(src, dst, sem)

    def remote(src, dst, ssem, rsem, yy, ss):
        return pltpu.make_async_remote_copy(src_ref=src, dst_ref=dst, send_sem=ssem, recv_sem=rsem,
                                            device_id=(z, yy, ss), device_id_type=MESH)

    cp_h = local(h_hbm.at[h_idx, y], hin.at[0, 1], small_sem.at[0])
    cp_x = local(x_hbm.at[y], xraw.at[1], small_sem.at[1])
    cp_mod = local(mod_hbm, mod, small_sem.at[2])
    cp_win = local(win_hbm, win, small_sem.at[3])
    cp_wout = local(wout_hbm, wout, small_sem.at[4])
    cp_wqkv = [local(wqkv_hbm.at[:, pl.ds(j * DIM, DIM)], wqkv.at[j], w_sem.at[j]) for j in range(3)]
    cp_rest = [local(wo_hbm, wo, w_sem.at[3])]
    cp_rest += [local(wup_hbm.at[:, pl.ds(j * DIM, DIM)], wup.at[j], w_sem.at[4 + j]) for j in range(4)]
    cp_rest += [local(wdown_hbm, wdown, w_sem.at[8])]
    cp_hs = local(h_hbm.at[h_idx, oy], hsend, small_sem.at[5])
    cp_xs = local(x_hbm.at[oy], xsend, small_sem.at[6])
    rc_h = remote(hsend, hin.at[0, 0], init_send.at[0], init_recv.at[0], oy, s)
    rc_x = remote(xsend, xraw.at[0], init_send.at[1], init_recv.at[1], oy, s)

    @pl.when(jnp.logical_not(is_first))
    def _():
        cp_hs.start()
        cp_h.start()

    cp_xs.start()
    cp_x.start()
    cp_mod.start()
    cp_win.start()
    cp_wout.start()
    for j in (1, 2, 0):
        cp_wqkv[j].start()

    barrier = pltpu.get_barrier_semaphore()
    for dy in range(2):
        for ds in range(STAGES):
            if dy == 0 and ds == 0:
                continue
            pl.semaphore_signal(barrier, inc=1, device_id=(z, (y + dy) % 2, (s + ds) % STAGES), device_id_type=MESH)
    cp_xs.wait()

    @pl.when(jnp.logical_not(is_first))
    def _():
        cp_hs.wait()

    pl.semaphore_wait(barrier, 2 * STAGES - 1)

    @pl.when(uses_x)
    def _():
        rc_x.start()

    @pl.when(jnp.logical_not(jnp.logical_or(is_first, is_waiter)))
    def _():
        rc_h.start()

    for cp in cp_rest:
        cp.start()

    @pl.when(is_last)
    def _():
        rc_h.wait_send()
        pl.semaphore_signal(go_sem, inc=1, device_id=(z, y, s - 1), device_id_type=MESH)

    @pl.when(is_waiter)
    def _():
        pl.semaphore_wait(go_sem, 1)
        rc_h.start()

    cp_x.wait()
    cp_mod.wait()
    cp_win.wait()
    cp_wout.wait()

    @pl.when(jnp.logical_not(is_first))
    def _():
        cp_h.wait()

    @pl.when(uses_x)
    def _():
        xs[1] = xraw[1]
        xbt[0, 1] = xraw[1].astype(BF16)

    for cp in cp_wqkv:
        cp.wait()

    def stage_copy(k, c):
        return remote(outb.at[k, c], hin.at[k + 1, c], st_send.at[k, c], st_recv.at[k, c], y, s + 1)

    def x_copy(k, c):
        return remote(xbt_out.at[k, c], xbt.at[k + 1, c], x_send.at[k, c], x_recv.at[k, c], y, 0)

    lane = lax.broadcasted_iota(jnp.int32, (ROWS, 128), 1)
    PAIRS = HEADS // 2
    LNB = 32

    def embed(k, c):
        @pl.when(is_first)
        def _():
            xb = xbt[k, c].astype(F32).T.astype(BF16)
            hin[k, c] = mm(xb, win[...]).astype(BF16)

    def ln1_pieces(k, c):
        def piece(r):
            def run():
                rows = pl.ds(r, LNB)
                h0 = hin[k, c, rows].astype(F32)
                unorm[c, rows] = (layer_norm(h0) * (1.0 + mod[k, 1]) + mod[k, 0]).astype(BF16)
            return run
        return [piece(r) for r in range(0, ROWS, LNB)]

    def q_pieces(c):
        def piece(n):
            def run():
                qs[c, :, n:n + 256] = mm(unorm[c], wqkv[0, :, n:n + 256]).astype(BF16)
            return run
        return [piece(n) for n in range(0, DIM, 256)]

    def k_pieces(c):
        def piece(n):
            def run():
                ks[c, :, n:n + 256] = mm(unorm[c], wqkv[1, :, n:n + 256]).astype(BF16)
            return run
        return [piece(n) for n in range(0, DIM, 256)]

    def v_pieces(c):
        def piece(n):
            def run():
                val = mm(unorm[c], wqkv[2, :, n:n + 256])
                vt[c, n:n + 256, :] = val.T.astype(BF16)
            return run
        return [piece(n) for n in range(0, DIM, 256)]

    def attn_units(c):
        mxs, invs = {}, {}

        def scores(p):
            cols = slice(p * 128, (p + 1) * 128)
            q2 = qs[c, :, cols]
            zero = jnp.zeros_like(q2)
            qq = jnp.concatenate([jnp.where(lane < HD, q2, zero), jnp.where(lane < HD, zero, q2)], axis=0)
            k2 = jnp.concatenate([ks[0, :, cols], ks[1, :, cols]], axis=0)
            st = lax.dot_general(k2, qq, (((1,), (1,)), ((), ())), preferred_element_type=F32)
            s_scr[c, p] = st
            mxs[p] = jnp.max(st, axis=0, keepdims=True)

        def exps(p, half):
            cols = slice(half * ROWS, (half + 1) * ROWS)
            ex = jnp.exp2((s_scr[c, p, :, cols] - mxs[p][:, cols]) * EXP2_SCALE)
            inv = 1.0 / jnp.sum(ex, axis=0, keepdims=True)
            p_scr[c, p, :, cols] = (ex * inv).astype(BF16)

        def values(p):
            cols = slice(p * 128, (p + 1) * 128)
            v2 = jnp.concatenate([vt[0, cols, :], vt[1, cols, :]], axis=1)
            ot = mm(v2, p_scr[c, p])
            o2 = jnp.concatenate([ot[:HD, :ROWS], ot[HD:, ROWS:]], axis=0)
            attn[c, :, cols] = o2.T.astype(BF16)

        sc = [functools.partial(scores, p) for p in range(PAIRS)]
        ev = []
        for p in range(PAIRS):
            ev.append(functools.partial(exps, p, 0))
            ev.append(functools.partial(exps, p, 1))
            if p:
                ev.append(functools.partial(values, p - 1))
        ev.append(functools.partial(values, PAIRS - 1))
        return sc, ev

    def wo_pieces(c):
        def piece(n):
            def run():
                hres[c, :, n:n + 256] = mm(attn[c], wo[:, n:n + 256])
            return run
        return [piece(n) for n in range(0, DIM, 256)]

    def ln2_pieces(k, c):
        def piece(r):
            def run():
                rows = pl.ds(r, LNB)
                h1 = hin[k, c, rows].astype(F32) + mod[k, 2] * hres[c, rows]
                hres[c, rows] = h1
                unorm[c, rows] = (layer_norm(h1) * (1.0 + mod[k, 4]) + mod[k, 3]).astype(BF16)
            return run
        return [piece(r) for r in range(0, ROWS, LNB)]

    def up_pieces(c):
        def piece(n):
            def run():
                j, m = divmod(n, DIM)
                act[c, :, n:n + 256] = gelu(mm(unorm[c], wup[j, :, m:m + 256])).astype(BF16)
            return run
        return [piece(n) for n in range(0, FF, 256)]

    def down_pieces(k, c):
        def store(n, res):
            out = hres[c, :, n:n + 256] + mod[k, 5][:, n:n + 256] * res
            outb[k, c, :, n:n + 256] = out.astype(BF16)

        def full(n):
            def run():
                store(n, mm(act[c], wdown[:, n:n + 256]))
            return run

        def halves(n):
            def run():
                lo = mm(act[c, :, :FF // 2], wdown[:FF // 2, n:n + 256])
                hi = mm(act[c, :, FF // 2:], wdown[FF // 2:, n:n + 256])
                store(n, lo + hi)
            return run
        return [full(0), full(256), halves(512)]

    def finish(k, c):
        @pl.when(jnp.logical_and(k < STEPS - 1, jnp.logical_not(is_last)))
        def _():
            stage_copy(k, c).start()

        if c == 0:
            @pl.when(k == STEPS - 1)
            def _():
                remote(outb.at[k, c], ho_ref.at[y], ho_send, ho_recv, oy, s).start()
        else:
            @pl.when(k == STEPS - 1)
            def _():
                ho_ref[y] = outb[k, c]

        @pl.when(is_last)
        def _():
            eps = lax.dot_general(wout[...], outb[k, c], (((1,), (1,)), ((), ())), preferred_element_type=F32)
            xn = alpha_ref[k] * xs[c] + beta_ref[k] * eps
            xs[c] = xn

            @pl.when(k < STEPS - 1)
            def _():
                xbt_out[k, c] = xn.astype(BF16)
                x_copy(k, c).start()

            @pl.when(k == STEPS - 1)
            def _():
                xfin_out[c] = xn
                if c == 0:
                    for t in range(STAGES):
                        remote(xfin_out.at[c], xfin.at[y], xf_send.at[t], xf_recv.at[y], oy, t).start()
                else:
                    for t in range(STAGES - 1):
                        remote(xfin_out.at[c], xfin.at[y], xf_send.at[STAGES + t], xf_recv.at[y], y, t).start()
                    xfin[y] = xn

    def step(k, _):
        kprev = jnp.maximum(k - 1, 0)
        ca = jnp.where(k == 0, 1, 0)
        cb = 1 - ca

        @pl.when(jnp.logical_and(k > 0, jnp.logical_not(is_first)))
        def _():
            stage_copy(kprev, ca).wait_recv()

        @pl.when(jnp.logical_and(k > 0, is_first))
        def _():
            x_copy(kprev, ca).wait_recv()

        embed(k, ca)
        interleave(ln1_pieces(k, ca))
        interleave(k_pieces(ca) + v_pieces(ca))

        @pl.when(jnp.logical_and(k > 0, jnp.logical_not(is_first)))
        def _():
            stage_copy(kprev, cb).wait_recv()

        @pl.when(jnp.logical_and(k > 0, is_first))
        def _():
            x_copy(kprev, cb).wait_recv()

        @pl.when(k == 0)
        def _():
            @pl.when(jnp.logical_not(is_first))
            def _():
                rc_h.wait_recv()

            @pl.when(uses_x)
            def _():
                rc_x.wait_recv()
                xs[0] = xraw[0]
                xbt[0, 0] = xraw[0].astype(BF16)

            for cp in cp_rest:
                cp.wait()

        embed(k, cb)
        interleave(q_pieces(ca), ln1_pieces(k, cb))
        interleave(k_pieces(cb))
        interleave(q_pieces(cb))
        sc0, ev0 = attn_units(0)
        sc1, ev1 = attn_units(1)
        interleave(sc0[:2])
        interleave(v_pieces(cb) + sc0[2:] + sc1, ev0)
        interleave(wo_pieces(0), ev1[:3])
        interleave(ln2_pieces(k, 0), ev1[3:5])
        interleave(up_pieces(0), ev1[5:10])
        down0 = down_pieces(k, 0)
        interleave(down0[:2], ev1[10:] + wo_pieces(1))
        interleave(down0[2:], ln2_pieces(k, 1))
        finish(k, 0)
        interleave(up_pieces(1))
        interleave(down_pieces(k, 1))
        finish(k, 1)
        return 0

    lax.fori_loop(0, STEPS, step, 0)

    remote(xfin_out.at[0], xfin.at[oy], xf_send.at[0], xf_recv.at[oy], oy, s).wait_recv()

    @pl.when(jnp.logical_not(is_last))
    def _():
        remote(xfin_out.at[0], xfin.at[y], xf_send.at[0], xf_recv.at[y], y, s).wait_recv()

    for b in range(2):
        xo_ref[b] = xfin[b]

    @pl.when(is_last)
    def _():
        for t in range(STAGES):
            remote(xfin_out.at[0], xfin.at[y], xf_send.at[t], xf_recv.at[y], oy, t).wait_send()
        for t in range(STAGES - 1):
            remote(xfin_out.at[1], xfin.at[y], xf_send.at[STAGES + t], xf_recv.at[y], y, t).wait_send()
        for k in range(STEPS - 1):
            for c in range(2):
                x_copy(k, c).wait_send()

    @pl.when(jnp.logical_not(is_last))
    def _():
        for k in range(STEPS - 1):
            for c in range(2):
                stage_copy(k, c).wait_send()

    @pl.when(jnp.logical_not(jnp.logical_or(is_first, is_last)))
    def _():
        rc_h.wait_send()

    @pl.when(uses_x)
    def _():
        rc_x.wait_send()

    last = remote(outb.at[STEPS - 1, 0], ho_ref.at[oy], ho_send, ho_recv, oy, s)
    last.wait_send()
    last.wait_recv()


def writer(x_ref, h_ref, xo_ref, ho_ref, sems):
    copies = [pltpu.make_async_copy(x_ref, xo_ref, sems.at[0]), pltpu.make_async_copy(h_ref, ho_ref, sems.at[1])]
    for copy in copies:
        copy.start()
    for copy in copies:
        copy.wait()


def solution(mesh):
    hbm = pl.BlockSpec(memory_space=pltpu.HBM)
    smem = pl.BlockSpec(memory_space=pltpu.SMEM)
    vmem = pl.BlockSpec(memory_space=pltpu.VMEM)
    dma = pltpu.SemaphoreType.DMA
    scratch = [
        pltpu.VMEM((3, DIM, DIM), BF16),
        pltpu.VMEM((DIM, DIM), BF16),
        pltpu.VMEM((4, DIM, DIM), BF16),
        pltpu.VMEM((FF, DIM), BF16),
        pltpu.VMEM((LAT, DIM), BF16),
        pltpu.VMEM((LAT, DIM), BF16),
        pltpu.VMEM((STEPS, 6, 1, DIM), F32),
        pltpu.VMEM((2, LAT, ROWS), F32),
        pltpu.VMEM((LAT, ROWS), F32),
        pltpu.VMEM((ROWS, DIM), BF16),
        pltpu.VMEM((STEPS, 2, ROWS, DIM), BF16),
        pltpu.VMEM((STEPS, 2, ROWS, DIM), BF16),
        pltpu.VMEM((STEPS, 2, LAT, ROWS), BF16),
        pltpu.VMEM((STEPS, 2, LAT, ROWS), BF16),
        pltpu.VMEM((2, LAT, ROWS), F32),
        pltpu.VMEM((2, LAT, ROWS), F32),
        pltpu.VMEM((2, LAT, ROWS), F32),
        pltpu.VMEM((2, ROWS, DIM), F32),
        pltpu.VMEM((2, ROWS, DIM), BF16),
        pltpu.VMEM((2, ROWS, DIM), BF16),
        pltpu.VMEM((2, ROWS, DIM), BF16),
        pltpu.VMEM((2, DIM, ROWS), BF16),
        pltpu.VMEM((2, ROWS, DIM), BF16),
        pltpu.VMEM((2, ROWS, FF), BF16),
        pltpu.VMEM((2, HEADS // 2, 2 * ROWS, 2 * ROWS), F32),
        pltpu.VMEM((2, HEADS // 2, 2 * ROWS, 2 * ROWS), BF16),
        dma((9,)), dma((7,)), dma((2,)), dma((2,)),
        dma((STEPS - 1, 2)), dma((STEPS - 1, 2)), dma((STEPS - 1, 2)), dma((STEPS - 1, 2)),
        dma((2 * STAGES - 1,)), dma((2,)), dma, dma, pltpu.SemaphoreType.REGULAR,
    ]

    def device_fn(x_init, h_init, w_in, w_out, w_qkv, w_o, w_up, w_down, ada_mod, alpha_coef, beta_coef):
        call = pl.pallas_call(
            kernel,
            name="dit_steps",
            out_shape=(pltpu.VMEM((2, LAT, ROWS), F32), pltpu.VMEM((2, ROWS, DIM), BF16)),
            in_specs=[hbm] * 9 + [smem] * 2,
            out_specs=(vmem, vmem),
            scratch_shapes=scratch,
            compiler_params=pltpu.CompilerParams(collective_id=0, has_side_effects=True, vmem_limit_bytes=58 * 1024 * 1024),
        )
        x_final, h_final = call(x_init.swapaxes(1, 2), h_init, w_in, w_out.T, w_qkv.reshape(DIM, 3 * DIM), w_o.reshape(DIM, DIM),
                                w_up.reshape(DIM, FF), w_down.reshape(FF, DIM), ada_mod.swapaxes(1, 2), alpha_coef, beta_coef)
        x_final, h_final = pl.pallas_call(
            writer,
            name="write_out",
            out_shape=(jax.ShapeDtypeStruct(x_final.shape, F32), jax.ShapeDtypeStruct(h_final.shape, BF16)),
            in_specs=[vmem] * 2,
            out_specs=(hbm, hbm),
            scratch_shapes=[dma((2,))],
        )(pltpu.with_memory_space_constraint(x_final, pltpu.VMEM), pltpu.with_memory_space_constraint(h_final, pltpu.VMEM))
        return x_final.swapaxes(1, 2), h_final[None]

    weight_spec = P("stage", None, None)
    return jax.shard_map(
        device_fn,
        mesh=mesh,
        in_specs=(P("data", "seq", None), P(None, "data", "seq", None), P(), P(), weight_spec, P("stage", None, None, None), weight_spec, weight_spec, P(None, "stage", None, None), P(), P()),
        out_specs=(P("data", "seq", None), P("stage", "data", "seq", None)),
        check_vma=False,
    )
```

```python
import functools

import jax
import jax.numpy as jnp
from jax import lax
from jax.experimental import pallas as pl
from jax.experimental.pallas import tpu as pltpu
from jax.sharding import PartitionSpec as P

LN_EPS = 1e-6
MESH = pl.DeviceIdType.MESH
BF16 = jnp.bfloat16
F32 = jnp.float32

STEPS = 4
STAGES = 4
DIM = 768
FF = 3072
HEADS = 12
HD = 64
ROWS = 128
LAT = 48
EXP2_SCALE = HD ** -0.5 * 1.4426950408889634
GELU_C0 = 0.7978845608028654
GELU_C1 = GELU_C0 * 0.044715


def layer_norm(hidden):
    mean_val = jnp.mean(hidden, axis=-1, keepdims=True)
    centered = hidden - mean_val
    variance = jnp.mean(centered * centered, axis=-1, keepdims=True)
    return centered * lax.rsqrt(variance + LN_EPS)


def gelu(val):
    half = 0.5 * val
    return half + half * jnp.tanh(val * (GELU_C0 + GELU_C1 * (val * val)))


def mm(lhs, rhs):
    return jnp.dot(lhs, rhs, preferred_element_type=F32)


def interleave(*streams):
    order = []
    for idx, pieces in enumerate(streams):
        for pos in range(len(pieces)):
            order.append(((pos + 0.5) / len(pieces), idx, pos))
    for _, idx, pos in sorted(order):
        streams[idx][pos]()


def kernel(x_hbm, h_hbm, win_hbm, wout_hbm, wqkv_hbm, wo_hbm, wup_hbm, wdown_hbm, mod_hbm, alpha_ref, beta_ref,
           xo_ref, ho_ref,
           wqkv, wo, wup, wdown, win, wout, mod, xraw, xsend, hsend, hin, outb, xbt, xbt_out, xs, xfin_out, xfin,
           hres, unorm, qs, ks, vt, attn, act, s_scr, p_scr,
           w_sem, small_sem, init_send, init_recv, st_send, st_recv, x_send, x_recv, xf_send, xf_recv, ho_send, ho_recv, go_sem):
    y = lax.axis_index("seq")
    s = lax.axis_index("stage")
    z = lax.axis_index("data")
    oy = 1 - y
    is_first = s == 0
    is_last = s == STAGES - 1
    is_waiter = s == STAGES - 2
    uses_x = jnp.logical_or(is_first, is_last)
    h_idx = jnp.maximum(s - 1, 0)

    def local(src, dst, sem):
        return pltpu.make_async_copy(src, dst, sem)

    def remote(src, dst, ssem, rsem, yy, ss):
        return pltpu.make_async_remote_copy(src_ref=src, dst_ref=dst, send_sem=ssem, recv_sem=rsem,
                                            device_id=(z, yy, ss), device_id_type=MESH)

    cp_h = local(h_hbm.at[h_idx, y], hin.at[0, 1], small_sem.at[0])
    cp_x = local(x_hbm.at[y], xraw.at[1], small_sem.at[1])
    cp_mod = local(mod_hbm, mod, small_sem.at[2])
    cp_win = local(win_hbm, win, small_sem.at[3])
    cp_wout = local(wout_hbm, wout, small_sem.at[4])
    cp_wqkv = [local(wqkv_hbm.at[:, pl.ds(j * DIM, DIM)], wqkv.at[j], w_sem.at[j]) for j in range(3)]
    cp_rest = [local(wo_hbm, wo, w_sem.at[3])]
    cp_rest += [local(wup_hbm.at[:, pl.ds(j * DIM, DIM)], wup.at[j], w_sem.at[4 + j]) for j in range(4)]
    cp_rest += [local(wdown_hbm, wdown, w_sem.at[8])]
    cp_hs = local(h_hbm.at[h_idx, oy], hsend, small_sem.at[5])
    cp_xs = local(x_hbm.at[oy], xsend, small_sem.at[6])
    rc_h = remote(hsend, hin.at[0, 0], init_send.at[0], init_recv.at[0], oy, s)
    rc_x = remote(xsend, xraw.at[0], init_send.at[1], init_recv.at[1], oy, s)

    @pl.when(jnp.logical_not(is_first))
    def _():
        cp_hs.start()
        cp_h.start()

    cp_xs.start()
    cp_x.start()
    cp_mod.start()
    cp_win.start()
    cp_wout.start()
    for j in (1, 2, 0):
        cp_wqkv[j].start()

    barrier = pltpu.get_barrier_semaphore()
    for dy in range(2):
        for ds in range(STAGES):
            if dy == 0 and ds == 0:
                continue
            pl.semaphore_signal(barrier, inc=1, device_id=(z, (y + dy) % 2, (s + ds) % STAGES), device_id_type=MESH)
    cp_xs.wait()

    @pl.when(jnp.logical_not(is_first))
    def _():
        cp_hs.wait()

    pl.semaphore_wait(barrier, 2 * STAGES - 1)

    @pl.when(uses_x)
    def _():
        rc_x.start()

    @pl.when(jnp.logical_not(jnp.logical_or(is_first, is_waiter)))
    def _():
        rc_h.start()

    for cp in cp_rest:
        cp.start()

    @pl.when(is_last)
    def _():
        rc_h.wait_send()
        pl.semaphore_signal(go_sem, inc=1, device_id=(z, y, s - 1), device_id_type=MESH)

    @pl.when(is_waiter)
    def _():
        pl.semaphore_wait(go_sem, 1)
        rc_h.start()

    cp_x.wait()
    cp_mod.wait()
    cp_win.wait()
    cp_wout.wait()

    @pl.when(jnp.logical_not(is_first))
    def _():
        cp_h.wait()

    @pl.when(uses_x)
    def _():
        xs[1] = xraw[1]
        xbt[0, 1] = xraw[1].astype(BF16)

    for cp in cp_wqkv:
        cp.wait()

    def stage_copy(k, c):
        return remote(outb.at[k, c], hin.at[k + 1, c], st_send.at[k, c], st_recv.at[k, c], y, s + 1)

    def x_copy(k, c):
        return remote(xbt_out.at[k, c], xbt.at[k + 1, c], x_send.at[k, c], x_recv.at[k, c], y, 0)

    lane = lax.broadcasted_iota(jnp.int32, (ROWS, 128), 1)
    PAIRS = HEADS // 2
    LNB = 32

    def embed(k, c):
        @pl.when(is_first)
        def _():
            xb = xbt[k, c].astype(F32).T.astype(BF16)
            hin[k, c] = mm(xb, win[...]).astype(BF16)

    def ln1_pieces(k, c):
        def piece(r):
            def run():
                rows = pl.ds(r, LNB)
                h0 = hin[k, c, rows].astype(F32)
                unorm[c, rows] = (layer_norm(h0) * (1.0 + mod[k, 1]) + mod[k, 0]).astype(BF16)
            return run
        return [piece(r) for r in range(0, ROWS, LNB)]

    def q_pieces(c):
        def piece(n):
            def run():
                qs[c, :, n:n + 256] = mm(unorm[c], wqkv[0, :, n:n + 256]).astype(BF16)
            return run
        return [piece(n) for n in range(0, DIM, 256)]

    def k_pieces(c):
        def piece(n):
            def run():
                ks[c, :, n:n + 256] = mm(unorm[c], wqkv[1, :, n:n + 256]).astype(BF16)
            return run
        return [piece(n) for n in range(0, DIM, 256)]

    def v_pieces(c):
        def piece(n):
            def run():
                val = mm(unorm[c], wqkv[2, :, n:n + 256])
                vt[c, n:n + 256, :] = val.T.astype(BF16)
            return run
        return [piece(n) for n in range(0, DIM, 256)]

    def attn_units(c):
        mxs, invs = {}, {}

        def scores(p):
            cols = slice(p * 128, (p + 1) * 128)
            q2 = qs[c, :, cols]
            zero = jnp.zeros_like(q2)
            qq = jnp.concatenate([jnp.where(lane < HD, q2, zero), jnp.where(lane < HD, zero, q2)], axis=0)
            k2 = jnp.concatenate([ks[0, :, cols], ks[1, :, cols]], axis=0)
            st = lax.dot_general(k2, qq, (((1,), (1,)), ((), ())), preferred_element_type=F32)
            s_scr[c, p] = st
            if c == 0:
                mxs[p] = jnp.max(st, axis=0, keepdims=True)

        def exps(p, half):
            cols = slice(half * ROWS, (half + 1) * ROWS)
            st = s_scr[c, p, :, cols]
            mx = mxs[p][:, cols] if p in mxs else jnp.max(st, axis=0, keepdims=True)
            ex = jnp.exp2((st - mx) * EXP2_SCALE)
            inv = 1.0 / jnp.sum(ex, axis=0, keepdims=True)
            p_scr[c, p, :, cols] = (ex * inv).astype(BF16)

        def values(p):
            cols = slice(p * 128, (p + 1) * 128)
            v2 = jnp.concatenate([vt[0, cols, :], vt[1, cols, :]], axis=1)
            ot = mm(v2, p_scr[c, p])
            o2 = jnp.concatenate([ot[:HD, :ROWS], ot[HD:, ROWS:]], axis=0)
            attn[c, :, cols] = o2.T.astype(BF16)

        sc = [functools.partial(scores, p) for p in range(PAIRS)]
        ex = [functools.partial(exps, p, half) for p in range(PAIRS) for half in range(2)]
        va = [functools.partial(values, p) for p in range(PAIRS)]
        return sc, ex, va

    def wo_pieces(c):
        def piece(n):
            def run():
                hres[c, :, n:n + 256] = mm(attn[c], wo[:, n:n + 256])
            return run
        return [piece(n) for n in range(0, DIM, 256)]

    def ln2_pieces(k, c):
        def piece(r):
            def run():
                rows = pl.ds(r, LNB)
                h1 = hin[k, c, rows].astype(F32) + mod[k, 2] * hres[c, rows]
                hres[c, rows] = h1
                unorm[c, rows] = (layer_norm(h1) * (1.0 + mod[k, 4]) + mod[k, 3]).astype(BF16)
            return run
        return [piece(r) for r in range(0, ROWS, LNB)]

    def up_pieces(c):
        def piece(n):
            def run():
                j, m = divmod(n, DIM)
                act[c, :, n:n + 256] = gelu(mm(unorm[c], wup[j, :, m:m + 256])).astype(BF16)
            return run
        return [piece(n) for n in range(0, FF, 256)]

    def down_pieces(k, c):
        def store(n, res):
            out = hres[c, :, n:n + 256] + mod[k, 5][:, n:n + 256] * res
            outb[k, c, :, n:n + 256] = out.astype(BF16)

        def full(n):
            def run():
                store(n, mm(act[c], wdown[:, n:n + 256]))
            return run

        def halves(n):
            def run():
                lo = mm(act[c, :, :FF // 2], wdown[:FF // 2, n:n + 256])
                hi = mm(act[c, :, FF // 2:], wdown[FF // 2:, n:n + 256])
                store(n, lo + hi)
            return run
        return [full(0), full(256), halves(512)]

    def finish(k, c):
        @pl.when(jnp.logical_and(k < STEPS - 1, jnp.logical_not(is_last)))
        def _():
            stage_copy(k, c).start()

        if c == 0:
            @pl.when(k == STEPS - 1)
            def _():
                remote(outb.at[k, c], ho_ref.at[y], ho_send, ho_recv, oy, s).start()
        else:
            @pl.when(k == STEPS - 1)
            def _():
                ho_ref[y] = outb[k, c]

        @pl.when(is_last)
        def _():
            eps = lax.dot_general(wout[...], outb[k, c], (((1,), (1,)), ((), ())), preferred_element_type=F32)
            xn = alpha_ref[k] * xs[c] + beta_ref[k] * eps
            xs[c] = xn

            @pl.when(k < STEPS - 1)
            def _():
                xbt_out[k, c] = xn.astype(BF16)
                x_copy(k, c).start()

            @pl.when(k == STEPS - 1)
            def _():
                xfin_out[c] = xn
                if c == 0:
                    for t in range(STAGES):
                        remote(xfin_out.at[c], xfin.at[y], xf_send.at[t], xf_recv.at[y], oy, t).start()
                else:
                    for t in range(STAGES - 1):
                        remote(xfin_out.at[c], xfin.at[y], xf_send.at[STAGES + t], xf_recv.at[y], y, t).start()
                    xfin[y] = xn

    def step(k, _):
        kprev = jnp.maximum(k - 1, 0)
        ca = jnp.where(k == 0, 1, 0)
        cb = 1 - ca

        @pl.when(jnp.logical_and(k > 0, jnp.logical_not(is_first)))
        def _():
            stage_copy(kprev, ca).wait_recv()

        @pl.when(jnp.logical_and(k > 0, is_first))
        def _():
            x_copy(kprev, ca).wait_recv()

        spare = k // 64

        def hold_scores(n):
            s_scr[1, PAIRS + spare, 0:16, 0:128] = act[0, 0:16, n * 256:n * 256 + 128].astype(F32)

        embed(k, ca)
        interleave(ln1_pieces(k, ca))
        interleave(k_pieces(ca) + v_pieces(ca))

        @pl.when(jnp.logical_and(k > 0, jnp.logical_not(is_first)))
        def _():
            stage_copy(kprev, cb).wait_recv()

        @pl.when(jnp.logical_and(k > 0, is_first))
        def _():
            x_copy(kprev, cb).wait_recv()

        @pl.when(k == 0)
        def _():
            @pl.when(jnp.logical_not(is_first))
            def _():
                rc_h.wait_recv()

            @pl.when(uses_x)
            def _():
                rc_x.wait_recv()
                xs[0] = xraw[0]
                xbt[0, 0] = xraw[0].astype(BF16)

            for cp in cp_rest:
                cp.wait()

        embed(k, cb)
        interleave(q_pieces(ca), ln1_pieces(k, cb))
        interleave(k_pieces(cb))
        interleave(q_pieces(cb))
        sc0, ex0, va0 = attn_units(0)
        sc1, ex1, va1 = attn_units(1)
        vb = v_pieces(cb)
        interleave(sc0[:2] + [vb[0]] + sc0[2:4] + [vb[1]] + sc0[4:] + [vb[2]], ex0[:6])
        interleave([piece for pair in zip(sc1, va0) for piece in pair], ex0[6:])
        interleave(wo_pieces(0))
        interleave(ln2_pieces(k, 0))
        up0 = up_pieces(0)
        down0 = down_pieces(k, 0)
        for p in range(3):
            interleave(up0[3 * p:3 * p + 3])
            hold_scores(3 * p + 2)
            interleave(ex1[2 * p:2 * p + 2])
        interleave(up0[9:])
        hold_scores(11)
        interleave(down0[:2], ex1[6:])
        interleave(va1 + wo_pieces(1))
        interleave(down0[2:], ln2_pieces(k, 1))
        finish(k, 0)
        interleave(up_pieces(1))
        interleave(down_pieces(k, 1))
        finish(k, 1)
        return 0

    lax.fori_loop(0, STEPS, step, 0)

    remote(xfin_out.at[0], xfin.at[oy], xf_send.at[0], xf_recv.at[oy], oy, s).wait_recv()

    @pl.when(jnp.logical_not(is_last))
    def _():
        remote(xfin_out.at[0], xfin.at[y], xf_send.at[0], xf_recv.at[y], y, s).wait_recv()

    for b in range(2):
        xo_ref[b] = xfin[b]

    @pl.when(is_last)
    def _():
        for t in range(STAGES):
            remote(xfin_out.at[0], xfin.at[y], xf_send.at[t], xf_recv.at[y], oy, t).wait_send()
        for t in range(STAGES - 1):
            remote(xfin_out.at[1], xfin.at[y], xf_send.at[STAGES + t], xf_recv.at[y], y, t).wait_send()
        for k in range(STEPS - 1):
            for c in range(2):
                x_copy(k, c).wait_send()

    @pl.when(jnp.logical_not(is_last))
    def _():
        for k in range(STEPS - 1):
            for c in range(2):
                stage_copy(k, c).wait_send()

    @pl.when(jnp.logical_not(jnp.logical_or(is_first, is_last)))
    def _():
        rc_h.wait_send()

    @pl.when(uses_x)
    def _():
        rc_x.wait_send()

    last = remote(outb.at[STEPS - 1, 0], ho_ref.at[oy], ho_send, ho_recv, oy, s)
    last.wait_send()
    last.wait_recv()


def writer(x_ref, h_ref, xo_ref, ho_ref, sems):
    copies = [pltpu.make_async_copy(x_ref, xo_ref, sems.at[0]), pltpu.make_async_copy(h_ref, ho_ref, sems.at[1])]
    for copy in copies:
        copy.start()
    for copy in copies:
        copy.wait()


def solution(mesh):
    hbm = pl.BlockSpec(memory_space=pltpu.HBM)
    smem = pl.BlockSpec(memory_space=pltpu.SMEM)
    vmem = pl.BlockSpec(memory_space=pltpu.VMEM)
    dma = pltpu.SemaphoreType.DMA
    scratch = [
        pltpu.VMEM((3, DIM, DIM), BF16),
        pltpu.VMEM((DIM, DIM), BF16),
        pltpu.VMEM((4, DIM, DIM), BF16),
        pltpu.VMEM((FF, DIM), BF16),
        pltpu.VMEM((LAT, DIM), BF16),
        pltpu.VMEM((LAT, DIM), BF16),
        pltpu.VMEM((STEPS, 6, 1, DIM), F32),
        pltpu.VMEM((2, LAT, ROWS), F32),
        pltpu.VMEM((LAT, ROWS), F32),
        pltpu.VMEM((ROWS, DIM), BF16),
        pltpu.VMEM((STEPS, 2, ROWS, DIM), BF16),
        pltpu.VMEM((STEPS, 2, ROWS, DIM), BF16),
        pltpu.VMEM((STEPS, 2, LAT, ROWS), BF16),
        pltpu.VMEM((STEPS, 2, LAT, ROWS), BF16),
        pltpu.VMEM((2, LAT, ROWS), F32),
        pltpu.VMEM((2, LAT, ROWS), F32),
        pltpu.VMEM((2, LAT, ROWS), F32),
        pltpu.VMEM((2, ROWS, DIM), F32),
        pltpu.VMEM((2, ROWS, DIM), BF16),
        pltpu.VMEM((2, ROWS, DIM), BF16),
        pltpu.VMEM((2, ROWS, DIM), BF16),
        pltpu.VMEM((2, DIM, ROWS), BF16),
        pltpu.VMEM((2, ROWS, DIM), BF16),
        pltpu.VMEM((2, ROWS, FF), BF16),
        pltpu.VMEM((2, HEADS // 2 + 1, 2 * ROWS, 2 * ROWS), F32),
        pltpu.VMEM((2, HEADS // 2, 2 * ROWS, 2 * ROWS), BF16),
        dma((9,)), dma((7,)), dma((2,)), dma((2,)),
        dma((STEPS - 1, 2)), dma((STEPS - 1, 2)), dma((STEPS - 1, 2)), dma((STEPS - 1, 2)),
        dma((2 * STAGES - 1,)), dma((2,)), dma, dma, pltpu.SemaphoreType.REGULAR,
    ]

    def device_fn(x_init, h_init, w_in, w_out, w_qkv, w_o, w_up, w_down, ada_mod, alpha_coef, beta_coef):
        call = pl.pallas_call(
            kernel,
            name="dit_steps",
            out_shape=(pltpu.VMEM((2, LAT, ROWS), F32), pltpu.VMEM((2, ROWS, DIM), BF16)),
            in_specs=[hbm] * 9 + [smem] * 2,
            out_specs=(vmem, vmem),
            scratch_shapes=scratch,
            compiler_params=pltpu.CompilerParams(collective_id=0, has_side_effects=True, vmem_limit_bytes=58 * 1024 * 1024),
        )
        x_final, h_final = call(x_init.swapaxes(1, 2), h_init, w_in, w_out.T, w_qkv.reshape(DIM, 3 * DIM), w_o.reshape(DIM, DIM),
                                w_up.reshape(DIM, FF), w_down.reshape(FF, DIM), ada_mod.swapaxes(1, 2), alpha_coef, beta_coef)
        x_final, h_final = pl.pallas_call(
            writer,
            name="write_out",
            out_shape=(jax.ShapeDtypeStruct(x_final.shape, F32), jax.ShapeDtypeStruct(h_final.shape, BF16)),
            in_specs=[vmem] * 2,
            out_specs=(hbm, hbm),
            scratch_shapes=[dma((2,))],
        )(pltpu.with_memory_space_constraint(x_final, pltpu.VMEM), pltpu.with_memory_space_constraint(h_final, pltpu.VMEM))
        return x_final.swapaxes(1, 2), h_final[None]

    weight_spec = P("stage", None, None)
    return jax.shard_map(
        device_fn,
        mesh=mesh,
        in_specs=(P("data", "seq", None), P(None, "data", "seq", None), P(), P(), weight_spec, P("stage", None, None, None), weight_spec, weight_spec, P(None, "stage", None, None), P(), P()),
        out_specs=(P("data", "seq", None), P("stage", "data", "seq", None)),
        check_vma=False,
    )
```

```python
import functools

import jax
import jax.numpy as jnp
from jax import lax
from jax.experimental import pallas as pl
from jax.experimental.pallas import tpu as pltpu
from jax.sharding import PartitionSpec as P

LN_EPS = 1e-6
MESH = pl.DeviceIdType.MESH
BF16 = jnp.bfloat16
F32 = jnp.float32

STEPS = 4
STAGES = 4
DIM = 768
FF = 3072
HEADS = 12
HD = 64
ROWS = 128
LAT = 48
EXP2_SCALE = HD ** -0.5 * 1.4426950408889634
GELU_C0 = 0.7978845608028654
GELU_C1 = GELU_C0 * 0.044715


def layer_norm(hidden):
    mean_val = jnp.mean(hidden, axis=-1, keepdims=True)
    centered = hidden - mean_val
    variance = jnp.mean(centered * centered, axis=-1, keepdims=True)
    return centered * lax.rsqrt(variance + LN_EPS)


def gelu(val):
    half = 0.5 * val
    return half + half * jnp.tanh(val * (GELU_C0 + GELU_C1 * (val * val)))


def mm(lhs, rhs):
    return jnp.dot(lhs, rhs, preferred_element_type=F32)


def interleave(*streams):
    order = []
    for idx, pieces in enumerate(streams):
        for pos in range(len(pieces)):
            order.append(((pos + 0.5) / len(pieces), idx, pos))
    for _, idx, pos in sorted(order):
        streams[idx][pos]()


def kernel(x_hbm, h_hbm, win_hbm, wout_hbm, wqkv_hbm, wo_hbm, wup_hbm, wdown_hbm, mod_hbm, alpha_ref, beta_ref,
           xo_ref, ho_ref,
           wqkv, wo, wup, wdown, win, wout, mod, xraw, xsend, hsend, hin, outb, xbt, xbt_out, xs, xfin_out, xfin,
           hres, unorm, qs, ks, vt, attn, act, s_scr, p_scr,
           w_sem, small_sem, init_send, init_recv, st_send, st_recv, x_send, x_recv, xf_send, xf_recv, ho_send, ho_recv, go_sem):
    y = lax.axis_index("seq")
    s = lax.axis_index("stage")
    z = lax.axis_index("data")
    oy = 1 - y
    is_first = s == 0
    is_last = s == STAGES - 1
    is_waiter = s == STAGES - 2
    uses_x = jnp.logical_or(is_first, is_last)
    h_idx = jnp.maximum(s - 1, 0)

    def local(src, dst, sem):
        return pltpu.make_async_copy(src, dst, sem)

    def remote(src, dst, ssem, rsem, yy, ss):
        return pltpu.make_async_remote_copy(src_ref=src, dst_ref=dst, send_sem=ssem, recv_sem=rsem,
                                            device_id=(z, yy, ss), device_id_type=MESH)

    cp_h = local(h_hbm.at[h_idx, y], hin.at[0, 1], small_sem.at[0])
    cp_x = local(x_hbm.at[y], xraw.at[1], small_sem.at[1])
    cp_mod = local(mod_hbm, mod, small_sem.at[2])
    cp_win = local(win_hbm, win, small_sem.at[3])
    cp_wout = local(wout_hbm, wout, small_sem.at[4])
    cp_wqkv = [local(wqkv_hbm.at[:, pl.ds(j * DIM, DIM)], wqkv.at[j], w_sem.at[j]) for j in range(3)]
    cp_rest = [local(wo_hbm, wo, w_sem.at[3])]
    cp_rest += [local(wup_hbm.at[:, pl.ds(j * DIM, DIM)], wup.at[j], w_sem.at[4 + j]) for j in range(4)]
    cp_rest += [local(wdown_hbm, wdown, w_sem.at[8])]
    cp_hs = local(h_hbm.at[h_idx, oy], hsend, small_sem.at[5])
    cp_xs = local(x_hbm.at[oy], xsend, small_sem.at[6])
    rc_h = remote(hsend, hin.at[0, 0], init_send.at[0], init_recv.at[0], oy, s)
    rc_x = remote(xsend, xraw.at[0], init_send.at[1], init_recv.at[1], oy, s)

    @pl.when(jnp.logical_not(is_first))
    def _():
        cp_hs.start()
        cp_h.start()

    cp_xs.start()
    cp_x.start()
    cp_mod.start()
    cp_win.start()
    cp_wout.start()
    for j in (1, 2, 0):
        cp_wqkv[j].start()

    for cp in cp_rest:
        cp.start()

    barrier = pltpu.get_barrier_semaphore()
    for dy in range(2):
        for ds in range(STAGES):
            if dy == 0 and ds == 0:
                continue
            pl.semaphore_signal(barrier, inc=1, device_id=(z, (y + dy) % 2, (s + ds) % STAGES), device_id_type=MESH)
    cp_xs.wait()

    @pl.when(jnp.logical_not(is_first))
    def _():
        cp_hs.wait()

    pl.semaphore_wait(barrier, 2 * STAGES - 1)

    @pl.when(uses_x)
    def _():
        rc_x.start()

    @pl.when(jnp.logical_not(jnp.logical_or(is_first, is_waiter)))
    def _():
        rc_h.start()

    @pl.when(is_last)
    def _():
        rc_h.wait_send()
        pl.semaphore_signal(go_sem, inc=1, device_id=(z, y, s - 1), device_id_type=MESH)

    @pl.when(is_waiter)
    def _():
        pl.semaphore_wait(go_sem, 1)
        rc_h.start()

    cp_x.wait()
    cp_mod.wait()
    cp_win.wait()
    cp_wout.wait()

    @pl.when(jnp.logical_not(is_first))
    def _():
        cp_h.wait()

    @pl.when(uses_x)
    def _():
        xs[1] = xraw[1]
        xbt[0, 1] = xraw[1].astype(BF16)

    for cp in cp_wqkv:
        cp.wait()

    def stage_copy(k, c):
        return remote(outb.at[k, c], hin.at[k + 1, c], st_send.at[k, c], st_recv.at[k, c], y, s + 1)

    def x_copy(k, c):
        return remote(xbt_out.at[k, c], xbt.at[k + 1, c], x_send.at[k, c], x_recv.at[k, c], y, 0)

    lane = lax.broadcasted_iota(jnp.int32, (ROWS, 128), 1)
    PAIRS = HEADS // 2
    LNB = 32

    def embed(k, c):
        @pl.when(is_first)
        def _():
            xb = xbt[k, c].astype(F32).T.astype(BF16)
            hin[k, c] = mm(xb, win[...]).astype(BF16)

    def ln1_pieces(k, c):
        def piece(r):
            def run():
                rows = pl.ds(r, LNB)
                h0 = hin[k, c, rows].astype(F32)
                unorm[c, rows] = (layer_norm(h0) * (1.0 + mod[k, 1]) + mod[k, 0]).astype(BF16)
            return run
        return [piece(r) for r in range(0, ROWS, LNB)]

    def q_pieces(c):
        def piece(n):
            def run():
                val = mm(unorm[c], wqkv[0, :, n:n + 256])
                for p in range(2):
                    part = val[:, p * 128:(p + 1) * 128]
                    qs[c, n // 128 + p, :ROWS] = jnp.where(lane < HD, part, 0.0).astype(BF16)
                    qs[c, n // 128 + p, ROWS:] = jnp.where(lane < HD, 0.0, part).astype(BF16)
            return run
        return [piece(n) for n in range(0, DIM, 256)]

    def k_pieces(c):
        def piece(n):
            def run():
                ks[c, :, n:n + 256] = mm(unorm[c], wqkv[1, :, n:n + 256]).astype(BF16)
            return run
        return [piece(n) for n in range(0, DIM, 256)]

    def v_pieces(c):
        def piece(n):
            def run():
                val = mm(unorm[c], wqkv[2, :, n:n + 256])
                vt[c, n:n + 256, :] = val.T.astype(BF16)
            return run
        return [piece(n) for n in range(0, DIM, 256)]

    def attn_units(c):
        mxs, invs = {}, {}

        def scores(p):
            cols = slice(p * 128, (p + 1) * 128)
            k2 = jnp.concatenate([ks[0, :, cols], ks[1, :, cols]], axis=0)
            st = lax.dot_general(k2, qs[c, p], (((1,), (1,)), ((), ())), preferred_element_type=F32)
            s_scr[c, p] = st
            mxs[p] = jnp.max(st, axis=0, keepdims=True)

        def exps(p, half):
            cols = slice(half * ROWS, (half + 1) * ROWS)
            ex = jnp.exp2((s_scr[c, p, :, cols] - mxs[p][:, cols]) * EXP2_SCALE)
            inv = 1.0 / jnp.sum(ex, axis=0, keepdims=True)
            p_scr[c, p, :, cols] = (ex * inv).astype(BF16)

        def values(p):
            cols = slice(p * 128, (p + 1) * 128)
            v2 = jnp.concatenate([vt[0, cols, :], vt[1, cols, :]], axis=1)
            ot = mm(v2, p_scr[c, p])
            o2 = jnp.concatenate([ot[:HD, :ROWS], ot[HD:, ROWS:]], axis=0)
            attn[c, :, cols] = o2.T.astype(BF16)

        sc = [functools.partial(scores, p) for p in range(PAIRS)]
        ev = []
        for p in range(PAIRS):
            ev.append(functools.partial(exps, p, 0))
            ev.append(functools.partial(exps, p, 1))
            if p:
                ev.append(functools.partial(values, p - 1))
        ev.append(functools.partial(values, PAIRS - 1))
        return sc, ev

    def wo_pieces(c):
        def piece(n):
            def run():
                hres[c, :, n:n + 256] = mm(attn[c], wo[:, n:n + 256])
            return run
        return [piece(n) for n in range(0, DIM, 256)]

    def ln2_pieces(k, c):
        def piece(r):
            def run():
                rows = pl.ds(r, LNB)
                h1 = hin[k, c, rows].astype(F32) + mod[k, 2] * hres[c, rows]
                hres[c, rows] = h1
                unorm[c, rows] = (layer_norm(h1) * (1.0 + mod[k, 4]) + mod[k, 3]).astype(BF16)
            return run
        return [piece(r) for r in range(0, ROWS, LNB)]

    def up_pieces(c):
        def piece(n):
            def run():
                j, m = divmod(n, DIM)
                act[c, :, n:n + 256] = gelu(mm(unorm[c], wup[j, :, m:m + 256])).astype(BF16)
            return run
        return [piece(n) for n in range(0, FF, 256)]

    def down_pieces(k, c):
        def store(n, res):
            out = hres[c, :, n:n + 256] + mod[k, 5][:, n:n + 256] * res
            outb[k, c, :, n:n + 256] = out.astype(BF16)

        def full(n):
            def run():
                store(n, mm(act[c], wdown[:, n:n + 256]))
            return run

        def halves(n):
            def run():
                lo = mm(act[c, :, :FF // 2], wdown[:FF // 2, n:n + 256])
                hi = mm(act[c, :, FF // 2:], wdown[FF // 2:, n:n + 256])
                store(n, lo + hi)
            return run
        return [full(0), full(256), halves(512)]

    def finish(k, c):
        @pl.when(jnp.logical_and(k < STEPS - 1, jnp.logical_not(is_last)))
        def _():
            stage_copy(k, c).start()

        if c == 0:
            @pl.when(k == STEPS - 1)
            def _():
                remote(outb.at[k, c], ho_ref.at[y], ho_send, ho_recv, oy, s).start()
        else:
            @pl.when(k == STEPS - 1)
            def _():
                ho_ref[y] = outb[k, c]

        @pl.when(is_last)
        def _():
            eps = lax.dot_general(wout[...], outb[k, c], (((1,), (1,)), ((), ())), preferred_element_type=F32)
            xn = alpha_ref[k] * xs[c] + beta_ref[k] * eps
            xs[c] = xn

            @pl.when(k < STEPS - 1)
            def _():
                xbt_out[k, c] = xn.astype(BF16)
                x_copy(k, c).start()

            @pl.when(k == STEPS - 1)
            def _():
                xfin_out[c] = xn
                if c == 0:
                    for t in range(STAGES):
                        remote(xfin_out.at[c], xfin.at[y], xf_send.at[t], xf_recv.at[y], oy, t).start()
                else:
                    for t in range(STAGES - 1):
                        remote(xfin_out.at[c], xfin.at[y], xf_send.at[STAGES + t], xf_recv.at[y], y, t).start()
                    xfin[y] = xn

    def step(k, _):
        kprev = jnp.maximum(k - 1, 0)
        ca = jnp.where(k == 0, 1, 0)
        cb = 1 - ca

        @pl.when(jnp.logical_and(k > 0, jnp.logical_not(is_first)))
        def _():
            stage_copy(kprev, ca).wait_recv()

        @pl.when(jnp.logical_and(k > 0, is_first))
        def _():
            x_copy(kprev, ca).wait_recv()

        embed(k, ca)
        interleave(ln1_pieces(k, ca))
        interleave(k_pieces(ca) + v_pieces(ca))

        @pl.when(jnp.logical_and(k > 0, jnp.logical_not(is_first)))
        def _():
            stage_copy(kprev, cb).wait_recv()

        @pl.when(jnp.logical_and(k > 0, is_first))
        def _():
            x_copy(kprev, cb).wait_recv()

        @pl.when(k == 0)
        def _():
            @pl.when(jnp.logical_not(is_first))
            def _():
                rc_h.wait_recv()

            @pl.when(uses_x)
            def _():
                rc_x.wait_recv()
                xs[0] = xraw[0]
                xbt[0, 0] = xraw[0].astype(BF16)

            for cp in cp_rest:
                cp.wait()

        embed(k, cb)
        interleave(q_pieces(ca), ln1_pieces(k, cb))
        interleave(k_pieces(cb))
        interleave(q_pieces(cb))
        sc0, ev0 = attn_units(0)
        sc1, ev1 = attn_units(1)
        interleave(sc0[:2])
        interleave(v_pieces(cb) + sc0[2:] + sc1, ev0)
        interleave(wo_pieces(0), ev1[:3])
        interleave(ln2_pieces(k, 0), ev1[3:5])
        interleave(up_pieces(0), ev1[5:10])
        down0 = down_pieces(k, 0)
        interleave(down0[:2], ev1[10:] + wo_pieces(1))
        interleave(down0[2:], ln2_pieces(k, 1))
        finish(k, 0)
        interleave(up_pieces(1))
        interleave(down_pieces(k, 1))
        finish(k, 1)
        return 0

    lax.fori_loop(0, STEPS, step, 0)

    remote(xfin_out.at[0], xfin.at[oy], xf_send.at[0], xf_recv.at[oy], oy, s).wait_recv()

    @pl.when(jnp.logical_not(is_last))
    def _():
        remote(xfin_out.at[0], xfin.at[y], xf_send.at[0], xf_recv.at[y], y, s).wait_recv()

    for b in range(2):
        xo_ref[b] = xfin[b]

    @pl.when(is_last)
    def _():
        for t in range(STAGES):
            remote(xfin_out.at[0], xfin.at[y], xf_send.at[t], xf_recv.at[y], oy, t).wait_send()
        for t in range(STAGES - 1):
            remote(xfin_out.at[1], xfin.at[y], xf_send.at[STAGES + t], xf_recv.at[y], y, t).wait_send()
        for k in range(STEPS - 1):
            for c in range(2):
                x_copy(k, c).wait_send()

    @pl.when(jnp.logical_not(is_last))
    def _():
        for k in range(STEPS - 1):
            for c in range(2):
                stage_copy(k, c).wait_send()

    @pl.when(jnp.logical_not(jnp.logical_or(is_first, is_last)))
    def _():
        rc_h.wait_send()

    @pl.when(uses_x)
    def _():
        rc_x.wait_send()

    last = remote(outb.at[STEPS - 1, 0], ho_ref.at[oy], ho_send, ho_recv, oy, s)
    last.wait_send()
    last.wait_recv()


def writer(x_ref, h_ref, xo_ref, ho_ref, sems):
    copies = [pltpu.make_async_copy(x_ref, xo_ref, sems.at[0]), pltpu.make_async_copy(h_ref, ho_ref, sems.at[1])]
    for copy in copies:
        copy.start()
    for copy in copies:
        copy.wait()


def solution(mesh):
    hbm = pl.BlockSpec(memory_space=pltpu.HBM)
    smem = pl.BlockSpec(memory_space=pltpu.SMEM)
    vmem = pl.BlockSpec(memory_space=pltpu.VMEM)
    dma = pltpu.SemaphoreType.DMA
    scratch = [
        pltpu.VMEM((3, DIM, DIM), BF16),
        pltpu.VMEM((DIM, DIM), BF16),
        pltpu.VMEM((4, DIM, DIM), BF16),
        pltpu.VMEM((FF, DIM), BF16),
        pltpu.VMEM((LAT, DIM), BF16),
        pltpu.VMEM((LAT, DIM), BF16),
        pltpu.VMEM((STEPS, 6, 1, DIM), F32),
        pltpu.VMEM((2, LAT, ROWS), F32),
        pltpu.VMEM((LAT, ROWS), F32),
        pltpu.VMEM((ROWS, DIM), BF16),
        pltpu.VMEM((STEPS, 2, ROWS, DIM), BF16),
        pltpu.VMEM((STEPS, 2, ROWS, DIM), BF16),
        pltpu.VMEM((STEPS, 2, LAT, ROWS), BF16),
        pltpu.VMEM((STEPS, 2, LAT, ROWS), BF16),
        pltpu.VMEM((2, LAT, ROWS), F32),
        pltpu.VMEM((2, LAT, ROWS), F32),
        pltpu.VMEM((2, LAT, ROWS), F32),
        pltpu.VMEM((2, ROWS, DIM), F32),
        pltpu.VMEM((2, ROWS, DIM), BF16),
        pltpu.VMEM((2, HEADS // 2, 2 * ROWS, 128), BF16),
        pltpu.VMEM((2, ROWS, DIM), BF16),
        pltpu.VMEM((2, DIM, ROWS), BF16),
        pltpu.VMEM((2, ROWS, DIM), BF16),
        pltpu.VMEM((2, ROWS, FF), BF16),
        pltpu.VMEM((2, HEADS // 2, 2 * ROWS, 2 * ROWS), F32),
        pltpu.VMEM((2, HEADS // 2, 2 * ROWS, 2 * ROWS), BF16),
        dma((9,)), dma((7,)), dma((2,)), dma((2,)),
        dma((STEPS - 1, 2)), dma((STEPS - 1, 2)), dma((STEPS - 1, 2)), dma((STEPS - 1, 2)),
        dma((2 * STAGES - 1,)), dma((2,)), dma, dma, pltpu.SemaphoreType.REGULAR,
    ]

    def device_fn(x_init, h_init, w_in, w_out, w_qkv, w_o, w_up, w_down, ada_mod, alpha_coef, beta_coef):
        call = pl.pallas_call(
            kernel,
            name="dit_steps",
            out_shape=(pltpu.VMEM((2, LAT, ROWS), F32), pltpu.VMEM((2, ROWS, DIM), BF16)),
            in_specs=[hbm] * 9 + [smem] * 2,
            out_specs=(vmem, vmem),
            scratch_shapes=scratch,
            compiler_params=pltpu.CompilerParams(collective_id=0, has_side_effects=True, vmem_limit_bytes=58 * 1024 * 1024),
        )
        x_final, h_final = call(x_init.swapaxes(1, 2), h_init, w_in, w_out.T, w_qkv.reshape(DIM, 3 * DIM), w_o.reshape(DIM, DIM),
                                w_up.reshape(DIM, FF), w_down.reshape(FF, DIM), ada_mod.swapaxes(1, 2), alpha_coef, beta_coef)
        x_final, h_final = pl.pallas_call(
            writer,
            name="write_out",
            out_shape=(jax.ShapeDtypeStruct(x_final.shape, F32), jax.ShapeDtypeStruct(h_final.shape, BF16)),
            in_specs=[vmem] * 2,
            out_specs=(hbm, hbm),
            scratch_shapes=[dma((2,))],
        )(pltpu.with_memory_space_constraint(x_final, pltpu.VMEM), pltpu.with_memory_space_constraint(h_final, pltpu.VMEM))
        return x_final.swapaxes(1, 2), h_final[None]

    weight_spec = P("stage", None, None)
    return jax.shard_map(
        device_fn,
        mesh=mesh,
        in_specs=(P("data", "seq", None), P(None, "data", "seq", None), P(), P(), weight_spec, P("stage", None, None, None), weight_spec, weight_spec, P(None, "stage", None, None), P(), P()),
        out_specs=(P("data", "seq", None), P("stage", "data", "seq", None)),
        check_vma=False,
    )
```

```python
import functools

import jax
import jax.numpy as jnp
from jax import lax
from jax.experimental import pallas as pl
from jax.experimental.pallas import tpu as pltpu
from jax.sharding import PartitionSpec as P

LN_EPS = 1e-6
MESH = pl.DeviceIdType.MESH
BF16 = jnp.bfloat16
F32 = jnp.float32

STEPS = 4
STAGES = 4
DIM = 768
FF = 3072
HEADS = 12
HD = 64
ROWS = 128
LAT = 48
EXP2_SCALE = HD ** -0.5 * 1.4426950408889634
GELU_C0 = 0.7978845608028654
GELU_C1 = GELU_C0 * 0.044715


def layer_norm(hidden):
    mean_val = jnp.mean(hidden, axis=-1, keepdims=True)
    centered = hidden - mean_val
    variance = jnp.mean(centered * centered, axis=-1, keepdims=True)
    return centered * lax.rsqrt(variance + LN_EPS)


def gelu(val):
    half = 0.5 * val
    return half + half * jnp.tanh(val * (GELU_C0 + GELU_C1 * (val * val)))


def mm(lhs, rhs):
    return jnp.dot(lhs, rhs, preferred_element_type=F32)


def interleave(*streams):
    order = []
    for idx, pieces in enumerate(streams):
        for pos in range(len(pieces)):
            order.append(((pos + 0.5) / len(pieces), idx, pos))
    for _, idx, pos in sorted(order):
        streams[idx][pos]()


def kernel(x_hbm, h_hbm, win_hbm, wout_hbm, wqkv_hbm, wo_hbm, wup_hbm, wdown_hbm, mod_hbm, alpha_ref, beta_ref,
           xo_ref, ho_ref,
           wqkv, wo, wup, wdown, win, wout, mod, xraw, xsend, hsend, hin, outb, xbt, xbt_out, xs, xfin_out, xfin,
           hres, unorm, qs, ks, vt, attn, act, s_scr, p_scr,
           w_sem, small_sem, init_send, init_recv, st_send, st_recv, x_send, x_recv, xf_send, xf_recv, ho_send, ho_recv, go_sem):
    y = lax.axis_index("seq")
    s = lax.axis_index("stage")
    z = lax.axis_index("data")
    oy = 1 - y
    is_first = s == 0
    is_last = s == STAGES - 1
    is_waiter = s == STAGES - 2
    uses_x = jnp.logical_or(is_first, is_last)
    h_idx = jnp.maximum(s - 1, 0)

    def local(src, dst, sem):
        return pltpu.make_async_copy(src, dst, sem)

    def remote(src, dst, ssem, rsem, yy, ss):
        return pltpu.make_async_remote_copy(src_ref=src, dst_ref=dst, send_sem=ssem, recv_sem=rsem,
                                            device_id=(z, yy, ss), device_id_type=MESH)

    cp_h = local(h_hbm.at[h_idx, y], hin.at[0, 1], small_sem.at[0])
    cp_x = local(x_hbm.at[y], xraw.at[1], small_sem.at[1])
    cp_mod = local(mod_hbm, mod, small_sem.at[2])
    cp_win = local(win_hbm, win, small_sem.at[3])
    cp_wout = local(wout_hbm, wout, small_sem.at[4])
    cp_wqkv = [local(wqkv_hbm.at[:, pl.ds(j * DIM, DIM)], wqkv.at[j], w_sem.at[j]) for j in range(3)]
    cp_rest = [local(wo_hbm, wo, w_sem.at[3])]
    cp_rest += [local(wup_hbm.at[:, pl.ds(j * DIM, DIM)], wup.at[j], w_sem.at[4 + j]) for j in range(4)]
    cp_rest += [local(wdown_hbm, wdown, w_sem.at[8])]
    cp_hs = local(h_hbm.at[h_idx, oy], hsend, small_sem.at[5])
    cp_xs = local(x_hbm.at[oy], xsend, small_sem.at[6])
    rc_h = remote(hsend, hin.at[0, 0], init_send.at[0], init_recv.at[0], oy, s)
    rc_x = remote(xsend, xraw.at[0], init_send.at[1], init_recv.at[1], oy, s)

    @pl.when(jnp.logical_not(is_first))
    def _():
        cp_hs.start()
        cp_h.start()

    cp_xs.start()
    cp_x.start()
    cp_mod.start()
    cp_win.start()
    cp_wout.start()
    for j in (1, 2, 0):
        cp_wqkv[j].start()

    barrier = pltpu.get_barrier_semaphore()
    for dy in range(2):
        for ds in range(STAGES):
            if dy == 0 and ds == 0:
                continue
            pl.semaphore_signal(barrier, inc=1, device_id=(z, (y + dy) % 2, (s + ds) % STAGES), device_id_type=MESH)
    cp_xs.wait()

    @pl.when(jnp.logical_not(is_first))
    def _():
        cp_hs.wait()

    pl.semaphore_wait(barrier, 2 * STAGES - 1)

    @pl.when(uses_x)
    def _():
        rc_x.start()

    @pl.when(jnp.logical_not(jnp.logical_or(is_first, is_waiter)))
    def _():
        rc_h.start()

    for cp in cp_rest:
        cp.start()

    @pl.when(is_last)
    def _():
        rc_h.wait_send()
        pl.semaphore_signal(go_sem, inc=1, device_id=(z, y, s - 1), device_id_type=MESH)

    @pl.when(is_waiter)
    def _():
        pl.semaphore_wait(go_sem, 1)
        rc_h.start()

    cp_x.wait()
    cp_mod.wait()
    cp_win.wait()
    cp_wout.wait()

    @pl.when(jnp.logical_not(is_first))
    def _():
        cp_h.wait()

    @pl.when(uses_x)
    def _():
        xs[1] = xraw[1]
        xbt[0, 1] = xraw[1].astype(BF16)

    for cp in cp_wqkv:
        cp.wait()

    def stage_copy(k, c):
        return remote(outb.at[k, c], hin.at[k + 1, c], st_send.at[k, c], st_recv.at[k, c], y, s + 1)

    def x_copy(k, c):
        return remote(xbt_out.at[k, c], xbt.at[k + 1, c], x_send.at[k, c], x_recv.at[k, c], y, 0)

    lane = lax.broadcasted_iota(jnp.int32, (ROWS, 128), 1)
    PAIRS = HEADS // 2
    LNB = 32

    def embed(k, c):
        @pl.when(is_first)
        def _():
            xb = xbt[k, c].astype(F32).T.astype(BF16)
            hin[k, c] = mm(xb, win[...]).astype(BF16)

    def ln1_pieces(k, c):
        def piece(r):
            def run():
                rows = pl.ds(r, LNB)
                h0 = hin[k, c, rows].astype(F32)
                unorm[c, rows] = (layer_norm(h0) * (1.0 + mod[k, 1]) + mod[k, 0]).astype(BF16)
            return run
        return [piece(r) for r in range(0, ROWS, LNB)]

    def q_pieces(c):
        def piece(n):
            def run():
                val = mm(unorm[c], wqkv[0, :, n:n + 256])
                for p in range(2):
                    part = val[:, p * 128:(p + 1) * 128]
                    qs[c, n // 128 + p, :ROWS] = jnp.where(lane < HD, part, 0.0).astype(BF16)
                    qs[c, n // 128 + p, ROWS:] = jnp.where(lane < HD, 0.0, part).astype(BF16)
            return run
        return [piece(n) for n in range(0, DIM, 256)]

    def k_pieces(c):
        def piece(n):
            def run():
                ks[c, :, n:n + 256] = mm(unorm[c], wqkv[1, :, n:n + 256]).astype(BF16)
            return run
        return [piece(n) for n in range(0, DIM, 256)]

    def v_pieces(c):
        def piece(n):
            def run():
                val = mm(unorm[c], wqkv[2, :, n:n + 256])
                vt[c, n:n + 256, :] = val.T.astype(BF16)
            return run
        return [piece(n) for n in range(0, DIM, 256)]

    def attn_units(c):
        mxs, invs = {}, {}

        def scores(p):
            cols = slice(p * 128, (p + 1) * 128)
            k2 = jnp.concatenate([ks[0, :, cols], ks[1, :, cols]], axis=0)
            st = lax.dot_general(k2, qs[c, p], (((1,), (1,)), ((), ())), preferred_element_type=F32)
            s_scr[c, p] = st
            mxs[p] = jnp.max(st, axis=0, keepdims=True)

        def exps(p, half):
            cols = slice(half * ROWS, (half + 1) * ROWS)
            ex = jnp.exp2((s_scr[c, p, :, cols] - mxs[p][:, cols]) * EXP2_SCALE)
            inv = 1.0 / jnp.sum(ex, axis=0, keepdims=True)
            p_scr[c, p, :, cols] = (ex * inv).astype(BF16)

        def values(p):
            cols = slice(p * 128, (p + 1) * 128)
            v2 = jnp.concatenate([vt[0, cols, :], vt[1, cols, :]], axis=1)
            ot = mm(v2, p_scr[c, p])
            o2 = jnp.concatenate([ot[:HD, :ROWS], ot[HD:, ROWS:]], axis=0)
            attn[c, :, cols] = o2.T.astype(BF16)

        sc = [functools.partial(scores, p) for p in range(PAIRS)]
        ev = []
        for p in range(PAIRS):
            ev.append(functools.partial(exps, p, 0))
            ev.append(functools.partial(exps, p, 1))
            if p:
                ev.append(functools.partial(values, p - 1))
        ev.append(functools.partial(values, PAIRS - 1))
        return sc, ev

    def wo_pieces(c):
        def piece(n):
            def run():
                hres[c, :, n:n + 256] = mm(attn[c], wo[:, n:n + 256])
            return run
        return [piece(n) for n in range(0, DIM, 256)]

    def ln2_pieces(k, c):
        def piece(r):
            def run():
                rows = pl.ds(r, LNB)
                h1 = hin[k, c, rows].astype(F32) + mod[k, 2] * hres[c, rows]
                hres[c, rows] = h1
                unorm[c, rows] = (layer_norm(h1) * (1.0 + mod[k, 4]) + mod[k, 3]).astype(BF16)
            return run
        return [piece(r) for r in range(0, ROWS, LNB)]

    def up_pieces(c):
        def piece(n):
            def run():
                j, m = divmod(n, DIM)
                act[c, :, n:n + 256] = gelu(mm(unorm[c], wup[j, :, m:m + 256])).astype(BF16)
            return run
        return [piece(n) for n in range(0, FF, 256)]

    def down_pieces(k, c):
        def store(n, res):
            out = hres[c, :, n:n + 256] + mod[k, 5][:, n:n + 256] * res
            outb[k, c, :, n:n + 256] = out.astype(BF16)

        def full(n):
            def run():
                store(n, mm(act[c], wdown[:, n:n + 256]))
            return run

        def halves(n):
            def run():
                lo = mm(act[c, :, :FF // 2], wdown[:FF // 2, n:n + 256])
                hi = mm(act[c, :, FF // 2:], wdown[FF // 2:, n:n + 256])
                store(n, lo + hi)
            return run
        return [full(0), full(256), halves(512)]

    def finish(k, c):
        @pl.when(jnp.logical_and(k < STEPS - 1, jnp.logical_not(is_last)))
        def _():
            stage_copy(k, c).start()

        if c == 0:
            @pl.when(k == STEPS - 1)
            def _():
                remote(outb.at[k, c], ho_ref.at[y], ho_send, ho_recv, oy, s).start()
        else:
            @pl.when(k == STEPS - 1)
            def _():
                ho_ref[y] = outb[k, c]

        @pl.when(is_last)
        def _():
            eps = lax.dot_general(wout[...], outb[k, c], (((1,), (1,)), ((), ())), preferred_element_type=F32)
            xn = alpha_ref[k] * xs[c] + beta_ref[k] * eps
            xs[c] = xn

            @pl.when(k < STEPS - 1)
            def _():
                xbt_out[k, c] = xn.astype(BF16)
                x_copy(k, c).start()

            @pl.when(k == STEPS - 1)
            def _():
                xfin_out[c] = xn
                if c == 0:
                    for t in range(STAGES):
                        remote(xfin_out.at[c], xfin.at[y], xf_send.at[t], xf_recv.at[y], oy, t).start()
                else:
                    for t in range(STAGES - 1):
                        remote(xfin_out.at[c], xfin.at[y], xf_send.at[STAGES + t], xf_recv.at[y], y, t).start()
                    xfin[y] = xn

    def step(k, _):
        kprev = jnp.maximum(k - 1, 0)
        ca = jnp.where(k == 0, 1, 0)
        cb = 1 - ca

        @pl.when(jnp.logical_and(k > 0, jnp.logical_not(is_first)))
        def _():
            stage_copy(kprev, ca).wait_recv()

        @pl.when(jnp.logical_and(k > 0, is_first))
        def _():
            x_copy(kprev, ca).wait_recv()

        embed(k, ca)
        interleave(ln1_pieces(k, ca))
        interleave(k_pieces(ca) + v_pieces(ca))

        @pl.when(jnp.logical_and(k > 0, jnp.logical_not(is_first)))
        def _():
            stage_copy(kprev, cb).wait_recv()

        @pl.when(jnp.logical_and(k > 0, is_first))
        def _():
            x_copy(kprev, cb).wait_recv()

        @pl.when(k == 0)
        def _():
            @pl.when(jnp.logical_not(is_first))
            def _():
                rc_h.wait_recv()

            @pl.when(uses_x)
            def _():
                rc_x.wait_recv()
                xs[0] = xraw[0]
                xbt[0, 0] = xraw[0].astype(BF16)

            for cp in cp_rest:
                cp.wait()

        embed(k, cb)
        interleave(q_pieces(ca), ln1_pieces(k, cb))
        interleave(k_pieces(cb))
        interleave(q_pieces(cb))
        sc0, ev0 = attn_units(0)
        sc1, ev1 = attn_units(1)
        interleave(sc0[:2])
        interleave(v_pieces(cb) + sc0[2:] + sc1, ev0)
        interleave(wo_pieces(0), ev1[:3])
        interleave(ln2_pieces(k, 0), ev1[3:5])
        interleave(up_pieces(0), ev1[5:10])
        down0 = down_pieces(k, 0)
        interleave(down0[:2], ev1[10:] + wo_pieces(1))
        interleave(down0[2:], ln2_pieces(k, 1))
        finish(k, 0)
        interleave(up_pieces(1))
        interleave(down_pieces(k, 1))
        finish(k, 1)
        return 0

    lax.fori_loop(0, STEPS, step, 0)

    remote(xfin_out.at[0], xfin.at[oy], xf_send.at[0], xf_recv.at[oy], oy, s).wait_recv()

    @pl.when(jnp.logical_not(is_last))
    def _():
        remote(xfin_out.at[0], xfin.at[y], xf_send.at[0], xf_recv.at[y], y, s).wait_recv()

    for b in range(2):
        xo_ref[b] = xfin[b]

    @pl.when(is_last)
    def _():
        for t in range(STAGES):
            remote(xfin_out.at[0], xfin.at[y], xf_send.at[t], xf_recv.at[y], oy, t).wait_send()
        for t in range(STAGES - 1):
            remote(xfin_out.at[1], xfin.at[y], xf_send.at[STAGES + t], xf_recv.at[y], y, t).wait_send()
        for k in range(STEPS - 1):
            for c in range(2):
                x_copy(k, c).wait_send()

    @pl.when(jnp.logical_not(is_last))
    def _():
        for k in range(STEPS - 1):
            for c in range(2):
                stage_copy(k, c).wait_send()

    @pl.when(jnp.logical_not(jnp.logical_or(is_first, is_last)))
    def _():
        rc_h.wait_send()

    @pl.when(uses_x)
    def _():
        rc_x.wait_send()

    last = remote(outb.at[STEPS - 1, 0], ho_ref.at[oy], ho_send, ho_recv, oy, s)
    last.wait_send()
    last.wait_recv()


def writer(x_ref, h_ref, xo_ref, ho_ref, sems):
    copies = [pltpu.make_async_copy(x_ref, xo_ref, sems.at[0]), pltpu.make_async_copy(h_ref, ho_ref, sems.at[1])]
    for copy in copies:
        copy.start()
    for copy in copies:
        copy.wait()


def solution(mesh):
    hbm = pl.BlockSpec(memory_space=pltpu.HBM)
    smem = pl.BlockSpec(memory_space=pltpu.SMEM)
    vmem = pl.BlockSpec(memory_space=pltpu.VMEM)
    dma = pltpu.SemaphoreType.DMA
    scratch = [
        pltpu.VMEM((3, DIM, DIM), BF16),
        pltpu.VMEM((DIM, DIM), BF16),
        pltpu.VMEM((4, DIM, DIM), BF16),
        pltpu.VMEM((FF, DIM), BF16),
        pltpu.VMEM((LAT, DIM), BF16),
        pltpu.VMEM((LAT, DIM), BF16),
        pltpu.VMEM((STEPS, 6, 1, DIM), F32),
        pltpu.VMEM((2, LAT, ROWS), F32),
        pltpu.VMEM((LAT, ROWS), F32),
        pltpu.VMEM((ROWS, DIM), BF16),
        pltpu.VMEM((STEPS, 2, ROWS, DIM), BF16),
        pltpu.VMEM((STEPS, 2, ROWS, DIM), BF16),
        pltpu.VMEM((STEPS, 2, LAT, ROWS), BF16),
        pltpu.VMEM((STEPS, 2, LAT, ROWS), BF16),
        pltpu.VMEM((2, LAT, ROWS), F32),
        pltpu.VMEM((2, LAT, ROWS), F32),
        pltpu.VMEM((2, LAT, ROWS), F32),
        pltpu.VMEM((2, ROWS, DIM), F32),
        pltpu.VMEM((2, ROWS, DIM), BF16),
        pltpu.VMEM((2, HEADS // 2, 2 * ROWS, 128), BF16),
        pltpu.VMEM((2, ROWS, DIM), BF16),
        pltpu.VMEM((2, DIM, ROWS), BF16),
        pltpu.VMEM((2, ROWS, DIM), BF16),
        pltpu.VMEM((2, ROWS, FF), BF16),
        pltpu.VMEM((2, HEADS // 2, 2 * ROWS, 2 * ROWS), F32),
        pltpu.VMEM((2, HEADS // 2, 2 * ROWS, 2 * ROWS), BF16),
        dma((9,)), dma((7,)), dma((2,)), dma((2,)),
        dma((STEPS - 1, 2)), dma((STEPS - 1, 2)), dma((STEPS - 1, 2)), dma((STEPS - 1, 2)),
        dma((2 * STAGES - 1,)), dma((2,)), dma, dma, pltpu.SemaphoreType.REGULAR,
    ]

    def device_fn(x_init, h_init, w_in, w_out, w_qkv, w_o, w_up, w_down, ada_mod, alpha_coef, beta_coef):
        call = pl.pallas_call(
            kernel,
            name="dit_steps",
            out_shape=(pltpu.VMEM((2, LAT, ROWS), F32), pltpu.VMEM((2, ROWS, DIM), BF16)),
            in_specs=[hbm] * 9 + [smem] * 2,
            out_specs=(vmem, vmem),
            scratch_shapes=scratch,
            compiler_params=pltpu.CompilerParams(collective_id=0, has_side_effects=True, vmem_limit_bytes=58 * 1024 * 1024),
        )
        x_final, h_final = call(x_init.swapaxes(1, 2), h_init, w_in, w_out.T, w_qkv.reshape(DIM, 3 * DIM), w_o.reshape(DIM, DIM),
                                w_up.reshape(DIM, FF), w_down.reshape(FF, DIM), ada_mod.swapaxes(1, 2), alpha_coef, beta_coef)
        x_final, h_final = pl.pallas_call(
            writer,
            name="write_out",
            out_shape=(jax.ShapeDtypeStruct(x_final.shape, F32), jax.ShapeDtypeStruct(h_final.shape, BF16)),
            in_specs=[vmem] * 2,
            out_specs=(hbm, hbm),
            scratch_shapes=[dma((2,))],
        )(pltpu.with_memory_space_constraint(x_final, pltpu.VMEM), pltpu.with_memory_space_constraint(h_final, pltpu.VMEM))
        return x_final.swapaxes(1, 2), h_final[None]

    weight_spec = P("stage", None, None)
    return jax.shard_map(
        device_fn,
        mesh=mesh,
        in_specs=(P("data", "seq", None), P(None, "data", "seq", None), P(), P(), weight_spec, P("stage", None, None, None), weight_spec, weight_spec, P(None, "stage", None, None), P(), P()),
        out_specs=(P("data", "seq", None), P("stage", "data", "seq", None)),
        check_vma=False,
    )
```

```python
import functools

import jax
import jax.numpy as jnp
from jax import lax
from jax.experimental import pallas as pl
from jax.experimental.pallas import tpu as pltpu
from jax.sharding import PartitionSpec as P

LN_EPS = 1e-6
MESH = pl.DeviceIdType.MESH
BF16 = jnp.bfloat16
F32 = jnp.float32

STEPS = 4
STAGES = 4
DIM = 768
FF = 3072
HEADS = 12
HD = 64
ROWS = 128
LAT = 48
EXP2_SCALE = HD ** -0.5 * 1.4426950408889634
GELU_C0 = 0.7978845608028654
GELU_C1 = GELU_C0 * 0.044715


def layer_norm(hidden):
    mean_val = jnp.mean(hidden, axis=-1, keepdims=True)
    centered = hidden - mean_val
    variance = jnp.mean(centered * centered, axis=-1, keepdims=True)
    return centered * lax.rsqrt(variance + LN_EPS)


def gelu(val):
    half = 0.5 * val
    return half + half * jnp.tanh(val * (GELU_C0 + GELU_C1 * (val * val)))


def mm(lhs, rhs):
    return jnp.dot(lhs, rhs, preferred_element_type=F32)


def interleave(*streams):
    order = []
    for idx, pieces in enumerate(streams):
        for pos in range(len(pieces)):
            order.append(((pos + 0.5) / len(pieces), idx, pos))
    for _, idx, pos in sorted(order):
        streams[idx][pos]()


def kernel(x_hbm, h_hbm, win_hbm, wout_hbm, wqkv_hbm, wo_hbm, wup_hbm, wdown_hbm, mod_hbm, alpha_ref, beta_ref,
           xo_ref, ho_ref,
           wqkv, wo, wup, wdown, win, wout, mod, xraw, xsend, hsend, hin, outb, xbt, xbt_out, xs, xfin_out, xfin,
           hres, unorm, qs, ks, vt, attn, act, s_scr, p_scr,
           w_sem, small_sem, init_send, init_recv, st_send, st_recv, x_send, x_recv, xf_send, xf_recv, ho_send, ho_recv, go_sem):
    y = lax.axis_index("seq")
    s = lax.axis_index("stage")
    z = lax.axis_index("data")
    oy = 1 - y
    is_first = s == 0
    is_last = s == STAGES - 1
    is_waiter = s == STAGES - 2
    uses_x = jnp.logical_or(is_first, is_last)
    h_idx = jnp.maximum(s - 1, 0)

    def local(src, dst, sem):
        return pltpu.make_async_copy(src, dst, sem)

    def remote(src, dst, ssem, rsem, yy, ss):
        return pltpu.make_async_remote_copy(src_ref=src, dst_ref=dst, send_sem=ssem, recv_sem=rsem,
                                            device_id=(z, yy, ss), device_id_type=MESH)

    cp_h = local(h_hbm.at[h_idx, y], hin.at[0, 1], small_sem.at[0])
    cp_x = local(x_hbm.at[y], xraw.at[1], small_sem.at[1])
    cp_mod = local(mod_hbm, mod, small_sem.at[2])
    cp_win = local(win_hbm, win, small_sem.at[3])
    cp_wout = local(wout_hbm, wout, small_sem.at[4])
    cp_wqkv = [local(wqkv_hbm.at[:, pl.ds(j * DIM, DIM)], wqkv.at[j], w_sem.at[j]) for j in range(3)]
    cp_rest = [local(wo_hbm, wo, w_sem.at[3])]
    cp_rest += [local(wup_hbm.at[:, pl.ds(j * DIM, DIM)], wup.at[j], w_sem.at[4 + j]) for j in range(4)]
    cp_rest += [local(wdown_hbm, wdown, w_sem.at[8])]
    cp_hs = local(h_hbm.at[h_idx, oy], hsend, small_sem.at[5])
    cp_xs = local(x_hbm.at[oy], xsend, small_sem.at[6])
    rc_h = remote(hsend, hin.at[0, 0], init_send.at[0], init_recv.at[0], oy, s)
    rc_x = remote(xsend, xraw.at[0], init_send.at[1], init_recv.at[1], oy, s)

    @pl.when(jnp.logical_not(is_first))
    def _():
        cp_hs.start()
        cp_h.start()

    cp_xs.start()
    cp_x.start()
    cp_mod.start()
    cp_win.start()
    cp_wout.start()

    barrier = pltpu.get_barrier_semaphore()
    for dy in range(2):
        for ds in range(STAGES):
            if dy == 0 and ds == 0:
                continue
            pl.semaphore_signal(barrier, inc=1, device_id=(z, (y + dy) % 2, (s + ds) % STAGES), device_id_type=MESH)
    cp_xs.wait()

    @pl.when(jnp.logical_not(is_first))
    def _():
        cp_hs.wait()

    pl.semaphore_wait(barrier, 2 * STAGES - 1)

    @pl.when(uses_x)
    def _():
        rc_x.start()

    @pl.when(jnp.logical_not(jnp.logical_or(is_first, is_waiter)))
    def _():
        rc_h.start()

    for j in (1, 2, 0):
        cp_wqkv[j].start()

    @pl.when(is_waiter)
    def _():
        pl.semaphore_wait(go_sem, 1)
        rc_h.start()

    for cp in cp_rest:
        cp.start()

    @pl.when(is_last)
    def _():
        rc_h.wait_send()
        pl.semaphore_signal(go_sem, inc=1, device_id=(z, y, s - 1), device_id_type=MESH)

    cp_x.wait()
    cp_mod.wait()
    cp_win.wait()
    cp_wout.wait()

    @pl.when(jnp.logical_not(is_first))
    def _():
        cp_h.wait()

    @pl.when(uses_x)
    def _():
        xs[1] = xraw[1]
        xbt[0, 1] = xraw[1].astype(BF16)

    for cp in cp_wqkv:
        cp.wait()

    def stage_copy(k, c):
        return remote(outb.at[k, c], hin.at[k + 1, c], st_send.at[k, c], st_recv.at[k, c], y, s + 1)

    def x_copy(k, c):
        return remote(xbt_out.at[k, c], xbt.at[k + 1, c], x_send.at[k, c], x_recv.at[k, c], y, 0)

    lane = lax.broadcasted_iota(jnp.int32, (ROWS, 128), 1)
    PAIRS = HEADS // 2
    LNB = 32

    def embed(k, c):
        @pl.when(is_first)
        def _():
            xb = xbt[k, c].astype(F32).T.astype(BF16)
            hin[k, c] = mm(xb, win[...]).astype(BF16)

    def ln1_pieces(k, c):
        def piece(r):
            def run():
                rows = pl.ds(r, LNB)
                h0 = hin[k, c, rows].astype(F32)
                unorm[c, rows] = (layer_norm(h0) * (1.0 + mod[k, 1]) + mod[k, 0]).astype(BF16)
            return run
        return [piece(r) for r in range(0, ROWS, LNB)]

    def q_pieces(c):
        def piece(n):
            def run():
                val = mm(unorm[c], wqkv[0, :, n:n + 256])
                for p in range(2):
                    part = val[:, p * 128:(p + 1) * 128]
                    qs[c, n // 128 + p, :ROWS] = jnp.where(lane < HD, part, 0.0).astype(BF16)
                    qs[c, n // 128 + p, ROWS:] = jnp.where(lane < HD, 0.0, part).astype(BF16)
            return run
        return [piece(n) for n in range(0, DIM, 256)]

    def k_pieces(c):
        def piece(n):
            def run():
                ks[c, :, n:n + 256] = mm(unorm[c], wqkv[1, :, n:n + 256]).astype(BF16)
            return run
        return [piece(n) for n in range(0, DIM, 256)]

    def v_pieces(c):
        def piece(n):
            def run():
                val = mm(unorm[c], wqkv[2, :, n:n + 256])
                vt[c, n:n + 256, :] = val.T.astype(BF16)
            return run
        return [piece(n) for n in range(0, DIM, 256)]

    def attn_units(c):
        mxs, invs = {}, {}

        def scores(p):
            cols = slice(p * 128, (p + 1) * 128)
            k2 = jnp.concatenate([ks[0, :, cols], ks[1, :, cols]], axis=0)
            st = lax.dot_general(k2, qs[c, p], (((1,), (1,)), ((), ())), preferred_element_type=F32)
            s_scr[c, p] = st
            mxs[p] = jnp.max(st, axis=0, keepdims=True)

        def exps(p, half):
            cols = slice(half * ROWS, (half + 1) * ROWS)
            ex = jnp.exp2((s_scr[c, p, :, cols] - mxs[p][:, cols]) * EXP2_SCALE)
            inv = 1.0 / jnp.sum(ex, axis=0, keepdims=True)
            p_scr[c, p, :, cols] = (ex * inv).astype(BF16)

        def values(p):
            cols = slice(p * 128, (p + 1) * 128)
            v2 = jnp.concatenate([vt[0, cols, :], vt[1, cols, :]], axis=1)
            ot = mm(v2, p_scr[c, p])
            o2 = jnp.concatenate([ot[:HD, :ROWS], ot[HD:, ROWS:]], axis=0)
            attn[c, :, cols] = o2.T.astype(BF16)

        sc = [functools.partial(scores, p) for p in range(PAIRS)]
        ev = []
        for p in range(PAIRS):
            ev.append(functools.partial(exps, p, 0))
            ev.append(functools.partial(exps, p, 1))
            if p:
                ev.append(functools.partial(values, p - 1))
        ev.append(functools.partial(values, PAIRS - 1))
        return sc, ev

    def wo_pieces(c):
        def piece(n):
            def run():
                hres[c, :, n:n + 256] = mm(attn[c], wo[:, n:n + 256])
            return run
        return [piece(n) for n in range(0, DIM, 256)]

    def ln2_pieces(k, c):
        def piece(r):
            def run():
                rows = pl.ds(r, LNB)
                h1 = hin[k, c, rows].astype(F32) + mod[k, 2] * hres[c, rows]
                hres[c, rows] = h1
                unorm[c, rows] = (layer_norm(h1) * (1.0 + mod[k, 4]) + mod[k, 3]).astype(BF16)
            return run
        return [piece(r) for r in range(0, ROWS, LNB)]

    def up_pieces(c):
        def piece(n):
            def run():
                j, m = divmod(n, DIM)
                act[c, :, n:n + 256] = gelu(mm(unorm[c], wup[j, :, m:m + 256])).astype(BF16)
            return run
        return [piece(n) for n in range(0, FF, 256)]

    def down_pieces(k, c):
        def store(n, res):
            out = hres[c, :, n:n + 256] + mod[k, 5][:, n:n + 256] * res
            outb[k, c, :, n:n + 256] = out.astype(BF16)

        def full(n):
            def run():
                store(n, mm(act[c], wdown[:, n:n + 256]))
            return run

        def halves(n):
            def run():
                lo = mm(act[c, :, :FF // 2], wdown[:FF // 2, n:n + 256])
                hi = mm(act[c, :, FF // 2:], wdown[FF // 2:, n:n + 256])
                store(n, lo + hi)
            return run
        return [full(0), full(256), halves(512)]

    def finish(k, c):
        @pl.when(jnp.logical_and(k < STEPS - 1, jnp.logical_not(is_last)))
        def _():
            stage_copy(k, c).start()

        if c == 0:
            @pl.when(k == STEPS - 1)
            def _():
                remote(outb.at[k, c], ho_ref.at[y], ho_send, ho_recv, oy, s).start()
        else:
            @pl.when(k == STEPS - 1)
            def _():
                ho_ref[y] = outb[k, c]

        @pl.when(is_last)
        def _():
            eps = lax.dot_general(wout[...], outb[k, c], (((1,), (1,)), ((), ())), preferred_element_type=F32)
            xn = alpha_ref[k] * xs[c] + beta_ref[k] * eps
            xs[c] = xn

            @pl.when(k < STEPS - 1)
            def _():
                xbt_out[k, c] = xn.astype(BF16)
                x_copy(k, c).start()

            @pl.when(k == STEPS - 1)
            def _():
                xfin_out[c] = xn
                if c == 0:
                    for t in range(STAGES):
                        remote(xfin_out.at[c], xfin.at[y], xf_send.at[t], xf_recv.at[y], oy, t).start()
                else:
                    for t in range(STAGES - 1):
                        remote(xfin_out.at[c], xfin.at[y], xf_send.at[STAGES + t], xf_recv.at[y], y, t).start()
                    xfin[y] = xn

    def step(k, _):
        kprev = jnp.maximum(k - 1, 0)
        ca = jnp.where(k == 0, 1, 0)
        cb = 1 - ca

        @pl.when(jnp.logical_and(k > 0, jnp.logical_not(is_first)))
        def _():
            stage_copy(kprev, ca).wait_recv()

        @pl.when(jnp.logical_and(k > 0, is_first))
        def _():
            x_copy(kprev, ca).wait_recv()

        embed(k, ca)
        interleave(ln1_pieces(k, ca))
        interleave(k_pieces(ca) + v_pieces(ca))

        @pl.when(jnp.logical_and(k > 0, jnp.logical_not(is_first)))
        def _():
            stage_copy(kprev, cb).wait_recv()

        @pl.when(jnp.logical_and(k > 0, is_first))
        def _():
            x_copy(kprev, cb).wait_recv()

        @pl.when(k == 0)
        def _():
            @pl.when(jnp.logical_not(is_first))
            def _():
                rc_h.wait_recv()

            @pl.when(uses_x)
            def _():
                rc_x.wait_recv()
                xs[0] = xraw[0]
                xbt[0, 0] = xraw[0].astype(BF16)

            for cp in cp_rest:
                cp.wait()

        embed(k, cb)
        interleave(q_pieces(ca), ln1_pieces(k, cb))
        interleave(k_pieces(cb))
        interleave(q_pieces(cb))
        sc0, ev0 = attn_units(0)
        sc1, ev1 = attn_units(1)
        interleave(sc0[:2])
        interleave(v_pieces(cb) + sc0[2:] + sc1, ev0)
        interleave(wo_pieces(0), ev1[:3])
        interleave(ln2_pieces(k, 0), ev1[3:5])
        interleave(up_pieces(0), ev1[5:10])
        down0 = down_pieces(k, 0)
        interleave(down0[:2], ev1[10:] + wo_pieces(1))
        interleave(down0[2:], ln2_pieces(k, 1))
        finish(k, 0)
        interleave(up_pieces(1))
        interleave(down_pieces(k, 1))
        finish(k, 1)
        return 0

    lax.fori_loop(0, STEPS, step, 0)

    remote(xfin_out.at[0], xfin.at[oy], xf_send.at[0], xf_recv.at[oy], oy, s).wait_recv()

    @pl.when(jnp.logical_not(is_last))
    def _():
        remote(xfin_out.at[0], xfin.at[y], xf_send.at[0], xf_recv.at[y], y, s).wait_recv()

    for b in range(2):
        xo_ref[b] = xfin[b]

    @pl.when(is_last)
    def _():
        for t in range(STAGES):
            remote(xfin_out.at[0], xfin.at[y], xf_send.at[t], xf_recv.at[y], oy, t).wait_send()
        for t in range(STAGES - 1):
            remote(xfin_out.at[1], xfin.at[y], xf_send.at[STAGES + t], xf_recv.at[y], y, t).wait_send()
        for k in range(STEPS - 1):
            for c in range(2):
                x_copy(k, c).wait_send()

    @pl.when(jnp.logical_not(is_last))
    def _():
        for k in range(STEPS - 1):
            for c in range(2):
                stage_copy(k, c).wait_send()

    @pl.when(jnp.logical_not(jnp.logical_or(is_first, is_last)))
    def _():
        rc_h.wait_send()

    @pl.when(uses_x)
    def _():
        rc_x.wait_send()

    last = remote(outb.at[STEPS - 1, 0], ho_ref.at[oy], ho_send, ho_recv, oy, s)
    last.wait_send()
    last.wait_recv()


def writer(x_ref, h_ref, xo_ref, ho_ref, sems):
    copies = [pltpu.make_async_copy(x_ref, xo_ref, sems.at[0]), pltpu.make_async_copy(h_ref, ho_ref, sems.at[1])]
    for copy in copies:
        copy.start()
    for copy in copies:
        copy.wait()


def solution(mesh):
    hbm = pl.BlockSpec(memory_space=pltpu.HBM)
    smem = pl.BlockSpec(memory_space=pltpu.SMEM)
    vmem = pl.BlockSpec(memory_space=pltpu.VMEM)
    dma = pltpu.SemaphoreType.DMA
    scratch = [
        pltpu.VMEM((3, DIM, DIM), BF16),
        pltpu.VMEM((DIM, DIM), BF16),
        pltpu.VMEM((4, DIM, DIM), BF16),
        pltpu.VMEM((FF, DIM), BF16),
        pltpu.VMEM((LAT, DIM), BF16),
        pltpu.VMEM((LAT, DIM), BF16),
        pltpu.VMEM((STEPS, 6, 1, DIM), F32),
        pltpu.VMEM((2, LAT, ROWS), F32),
        pltpu.VMEM((LAT, ROWS), F32),
        pltpu.VMEM((ROWS, DIM), BF16),
        pltpu.VMEM((STEPS, 2, ROWS, DIM), BF16),
        pltpu.VMEM((STEPS, 2, ROWS, DIM), BF16),
        pltpu.VMEM((STEPS, 2, LAT, ROWS), BF16),
        pltpu.VMEM((STEPS, 2, LAT, ROWS), BF16),
        pltpu.VMEM((2, LAT, ROWS), F32),
        pltpu.VMEM((2, LAT, ROWS), F32),
        pltpu.VMEM((2, LAT, ROWS), F32),
        pltpu.VMEM((2, ROWS, DIM), F32),
        pltpu.VMEM((2, ROWS, DIM), BF16),
        pltpu.VMEM((2, HEADS // 2, 2 * ROWS, 128), BF16),
        pltpu.VMEM((2, ROWS, DIM), BF16),
        pltpu.VMEM((2, DIM, ROWS), BF16),
        pltpu.VMEM((2, ROWS, DIM), BF16),
        pltpu.VMEM((2, ROWS, FF), BF16),
        pltpu.VMEM((2, HEADS // 2, 2 * ROWS, 2 * ROWS), F32),
        pltpu.VMEM((2, HEADS // 2, 2 * ROWS, 2 * ROWS), BF16),
        dma((9,)), dma((7,)), dma((2,)), dma((2,)),
        dma((STEPS - 1, 2)), dma((STEPS - 1, 2)), dma((STEPS - 1, 2)), dma((STEPS - 1, 2)),
        dma((2 * STAGES - 1,)), dma((2,)), dma, dma, pltpu.SemaphoreType.REGULAR,
    ]

    def device_fn(x_init, h_init, w_in, w_out, w_qkv, w_o, w_up, w_down, ada_mod, alpha_coef, beta_coef):
        call = pl.pallas_call(
            kernel,
            name="dit_steps",
            out_shape=(pltpu.VMEM((2, LAT, ROWS), F32), pltpu.VMEM((2, ROWS, DIM), BF16)),
            in_specs=[hbm] * 9 + [smem] * 2,
            out_specs=(vmem, vmem),
            scratch_shapes=scratch,
            compiler_params=pltpu.CompilerParams(collective_id=0, has_side_effects=True, vmem_limit_bytes=58 * 1024 * 1024),
        )
        x_final, h_final = call(x_init.swapaxes(1, 2), h_init, w_in, w_out.T, w_qkv.reshape(DIM, 3 * DIM), w_o.reshape(DIM, DIM),
                                w_up.reshape(DIM, FF), w_down.reshape(FF, DIM), ada_mod.swapaxes(1, 2), alpha_coef, beta_coef)
        x_final, h_final = pl.pallas_call(
            writer,
            name="write_out",
            out_shape=(jax.ShapeDtypeStruct(x_final.shape, F32), jax.ShapeDtypeStruct(h_final.shape, BF16)),
            in_specs=[vmem] * 2,
            out_specs=(hbm, hbm),
            scratch_shapes=[dma((2,))],
        )(pltpu.with_memory_space_constraint(x_final, pltpu.VMEM), pltpu.with_memory_space_constraint(h_final, pltpu.VMEM))
        return x_final.swapaxes(1, 2), h_final[None]

    weight_spec = P("stage", None, None)
    return jax.shard_map(
        device_fn,
        mesh=mesh,
        in_specs=(P("data", "seq", None), P(None, "data", "seq", None), P(), P(), weight_spec, P("stage", None, None, None), weight_spec, weight_spec, P(None, "stage", None, None), P(), P()),
        out_specs=(P("data", "seq", None), P("stage", "data", "seq", None)),
        check_vma=False,
    )
```

```python
import functools

import jax
import jax.numpy as jnp
from jax import lax
from jax.experimental import pallas as pl
from jax.experimental.pallas import tpu as pltpu
from jax.sharding import PartitionSpec as P

LN_EPS = 1e-6
MESH = pl.DeviceIdType.MESH
BF16 = jnp.bfloat16
F32 = jnp.float32

STEPS = 4
STAGES = 4
DIM = 768
FF = 3072
HEADS = 12
HD = 64
ROWS = 128
LAT = 48
EXP2_SCALE = HD ** -0.5 * 1.4426950408889634
GELU_C0 = 0.7978845608028654
GELU_C1 = GELU_C0 * 0.044715


def layer_norm(hidden):
    mean_val = jnp.mean(hidden, axis=-1, keepdims=True)
    centered = hidden - mean_val
    variance = jnp.mean(centered * centered, axis=-1, keepdims=True)
    return centered * lax.rsqrt(variance + LN_EPS)


def gelu(val):
    half = 0.5 * val
    return half + half * jnp.tanh(val * (GELU_C0 + GELU_C1 * (val * val)))


def mm(lhs, rhs):
    return jnp.dot(lhs, rhs, preferred_element_type=F32)


def interleave(*streams):
    order = []
    for idx, pieces in enumerate(streams):
        for pos in range(len(pieces)):
            order.append(((pos + 0.5) / len(pieces), idx, pos))
    for _, idx, pos in sorted(order):
        streams[idx][pos]()


def kernel(x_hbm, h_hbm, win_hbm, wout_hbm, wqkv_hbm, wo_hbm, wup_hbm, wdown_hbm, mod_hbm, alpha_ref, beta_ref,
           xo_ref, ho_ref,
           wqkv, wo, wup, wdown, win, wout, mod, xraw, xsend, hsend, hin, outb, xbt, xbt_out, xs, xfin_out, xfin,
           hres, unorm, qs, ks, vt, attn, act, s_scr, p_scr,
           w_sem, small_sem, init_send, init_recv, st_send, st_recv, x_send, x_recv, xf_send, xf_recv, ho_send, ho_recv, go_sem):
    y = lax.axis_index("seq")
    s = lax.axis_index("stage")
    z = lax.axis_index("data")
    oy = 1 - y
    is_first = s == 0
    is_last = s == STAGES - 1
    is_waiter = s == STAGES - 2
    uses_x = jnp.logical_or(is_first, is_last)
    h_idx = jnp.maximum(s - 1, 0)

    def local(src, dst, sem):
        return pltpu.make_async_copy(src, dst, sem)

    def remote(src, dst, ssem, rsem, yy, ss):
        return pltpu.make_async_remote_copy(src_ref=src, dst_ref=dst, send_sem=ssem, recv_sem=rsem,
                                            device_id=(z, yy, ss), device_id_type=MESH)

    cp_h = local(h_hbm.at[h_idx, y], hin.at[0, 1], small_sem.at[0])
    cp_x = local(x_hbm.at[y], xraw.at[1], small_sem.at[1])
    cp_mod = local(mod_hbm, mod, small_sem.at[2])
    cp_win = local(win_hbm, win, small_sem.at[3])
    cp_wout = local(wout_hbm, wout, small_sem.at[4])
    cp_wqkv = [local(wqkv_hbm.at[:, pl.ds(j * DIM, DIM)], wqkv.at[j], w_sem.at[j]) for j in range(3)]
    cp_rest = [local(wo_hbm, wo, w_sem.at[3])]
    cp_rest += [local(wup_hbm.at[:, pl.ds(j * DIM, DIM)], wup.at[j], w_sem.at[4 + j]) for j in range(4)]
    cp_rest += [local(wdown_hbm, wdown, w_sem.at[8])]
    cp_hs = local(h_hbm.at[h_idx, oy], hsend, small_sem.at[5])
    cp_xs = local(x_hbm.at[oy], xsend, small_sem.at[6])
    rc_h = remote(hsend, hin.at[0, 0], init_send.at[0], init_recv.at[0], oy, s)
    rc_x = remote(xsend, xraw.at[0], init_send.at[1], init_recv.at[1], oy, s)

    @pl.when(jnp.logical_not(is_first))
    def _():
        cp_hs.start()
        cp_h.start()

    cp_xs.start()
    cp_x.start()
    cp_mod.start()
    cp_win.start()
    cp_wout.start()
    for j in (1, 2, 0):
        cp_wqkv[j].start()

    barrier = pltpu.get_barrier_semaphore()
    for dy in range(2):
        for ds in range(STAGES):
            if dy == 0 and ds == 0:
                continue
            pl.semaphore_signal(barrier, inc=1, device_id=(z, (y + dy) % 2, (s + ds) % STAGES), device_id_type=MESH)
    cp_xs.wait()

    @pl.when(jnp.logical_not(is_first))
    def _():
        cp_hs.wait()

    pl.semaphore_wait(barrier, 2 * STAGES - 1)

    @pl.when(uses_x)
    def _():
        rc_x.start()

    @pl.when(jnp.logical_not(jnp.logical_or(is_first, is_waiter)))
    def _():
        rc_h.start()

    for cp in cp_rest:
        cp.start()

    @pl.when(is_last)
    def _():
        rc_h.wait_send()
        pl.semaphore_signal(go_sem, inc=1, device_id=(z, y, s - 1), device_id_type=MESH)

    @pl.when(is_waiter)
    def _():
        pl.semaphore_wait(go_sem, 1)
        rc_h.start()

    cp_x.wait()
    cp_mod.wait()
    cp_win.wait()
    cp_wout.wait()

    @pl.when(jnp.logical_not(is_first))
    def _():
        cp_h.wait()

    @pl.when(uses_x)
    def _():
        xs[1] = xraw[1]
        xbt[0, 1] = xraw[1].astype(BF16)

    for cp in cp_wqkv:
        cp.wait()

    def stage_copy(k, c):
        return remote(outb.at[k, c], hin.at[k + 1, c], st_send.at[k, c], st_recv.at[k, c], y, s + 1)

    def x_copy(k, c):
        return remote(xbt_out.at[k, c], xbt.at[k + 1, c], x_send.at[k, c], x_recv.at[k, c], y, 0)

    lane = lax.broadcasted_iota(jnp.int32, (ROWS, 128), 1)
    PAIRS = HEADS // 2
    LNB = 32

    def embed(k, c):
        @pl.when(is_first)
        def _():
            xb = xbt[k, c].astype(F32).T.astype(BF16)
            hin[k, c] = mm(xb, win[...]).astype(BF16)

    def ln1_pieces(k, c):
        def piece(r):
            def run():
                rows = pl.ds(r, LNB)
                h0 = hin[k, c, rows].astype(F32)
                unorm[c, rows] = (layer_norm(h0) * (1.0 + mod[k, 1]) + mod[k, 0]).astype(BF16)
            return run
        return [piece(r) for r in range(0, ROWS, LNB)]

    def q_pieces(c):
        def piece(n):
            def run():
                val = mm(unorm[c], wqkv[0, :, n:n + 256])
                for p in range(2):
                    part = val[:, p * 128:(p + 1) * 128]
                    qs[c, n // 128 + p, :ROWS] = jnp.where(lane < HD, part, 0.0).astype(BF16)
                    qs[c, n // 128 + p, ROWS:] = jnp.where(lane < HD, 0.0, part).astype(BF16)
            return run
        return [piece(n) for n in range(0, DIM, 256)]

    def k_pieces(c):
        def piece(n):
            def run():
                ks[c, :, n:n + 256] = mm(unorm[c], wqkv[1, :, n:n + 256]).astype(BF16)
            return run
        return [piece(n) for n in range(0, DIM, 256)]

    def v_pieces(c):
        def piece(n):
            def run():
                val = mm(unorm[c], wqkv[2, :, n:n + 256])
                vt[c, n:n + 256, :] = val.T.astype(BF16)
            return run
        return [piece(n) for n in range(0, DIM, 256)]

    def attn_units(c):
        mxs, invs = {}, {}

        def scores(p):
            cols = slice(p * 128, (p + 1) * 128)
            k2 = jnp.concatenate([ks[0, :, cols], ks[1, :, cols]], axis=0)
            st = lax.dot_general(k2, qs[c, p], (((1,), (1,)), ((), ())), preferred_element_type=F32)
            s_scr[c, p] = st
            mxs[p] = jnp.max(st, axis=0, keepdims=True)

        def exps(p, half):
            cols = slice(half * ROWS, (half + 1) * ROWS)
            ex = jnp.exp2((s_scr[c, p, :, cols] - mxs[p][:, cols]) * EXP2_SCALE)
            inv = 1.0 / jnp.sum(ex, axis=0, keepdims=True)
            p_scr[c, p, :, cols] = (ex * inv).astype(BF16)

        def values(p):
            cols = slice(p * 128, (p + 1) * 128)
            v2 = jnp.concatenate([vt[0, cols, :], vt[1, cols, :]], axis=1)
            ot = mm(v2, p_scr[c, p])
            o2 = jnp.concatenate([ot[:HD, :ROWS], ot[HD:, ROWS:]], axis=0)
            attn[c, :, cols] = o2.T.astype(BF16)

        sc = [functools.partial(scores, p) for p in range(PAIRS)]
        ev = []
        for p in range(PAIRS):
            ev.append(functools.partial(exps, p, 0))
            ev.append(functools.partial(exps, p, 1))
            if p:
                ev.append(functools.partial(values, p - 1))
        ev.append(functools.partial(values, PAIRS - 1))
        return sc, ev

    def wo_pieces(c):
        def piece(n):
            def run():
                hres[c, :, n:n + 256] = mm(attn[c], wo[:, n:n + 256])
            return run
        return [piece(n) for n in range(0, DIM, 256)]

    def ln2_pieces(k, c):
        def piece(r):
            def run():
                rows = pl.ds(r, LNB)
                h1 = hin[k, c, rows].astype(F32) + mod[k, 2] * hres[c, rows]
                hres[c, rows] = h1
                unorm[c, rows] = (layer_norm(h1) * (1.0 + mod[k, 4]) + mod[k, 3]).astype(BF16)
            return run
        return [piece(r) for r in range(0, ROWS, LNB)]

    def up_pieces(c):
        def piece(n):
            def run():
                j, m = divmod(n, DIM)
                act[c, :, n:n + 256] = gelu(mm(unorm[c], wup[j, :, m:m + 256])).astype(BF16)
            return run
        return [piece(n) for n in range(0, FF, 256)]

    def down_pieces(k, c):
        def store(n, res):
            out = hres[c, :, n:n + 256] + mod[k, 5][:, n:n + 256] * res
            outb[k, c, :, n:n + 256] = out.astype(BF16)

        def full(n):
            def run():
                store(n, mm(act[c], wdown[:, n:n + 256]))
            return run

        def halves(n):
            def run():
                lo = mm(act[c, :, :FF // 2], wdown[:FF // 2, n:n + 256])
                hi = mm(act[c, :, FF // 2:], wdown[FF // 2:, n:n + 256])
                store(n, lo + hi)
            return run
        return [full(0), full(256), halves(512)]

    def finish(k, c):
        k = jnp.int32(k)
        @pl.when(jnp.logical_and(k < STEPS - 1, jnp.logical_not(is_last)))
        def _():
            stage_copy(k, c).start()

        if c == 0:
            @pl.when(k == STEPS - 1)
            def _():
                remote(outb.at[k, c], ho_ref.at[y], ho_send, ho_recv, oy, s).start()
        else:
            @pl.when(k == STEPS - 1)
            def _():
                ho_ref[y] = outb[k, c]

        @pl.when(is_last)
        def _():
            eps = lax.dot_general(wout[...], outb[k, c], (((1,), (1,)), ((), ())), preferred_element_type=F32)
            xn = alpha_ref[k] * xs[c] + beta_ref[k] * eps
            xs[c] = xn

            @pl.when(k < STEPS - 1)
            def _():
                xbt_out[k, c] = xn.astype(BF16)
                x_copy(k, c).start()

            @pl.when(k == STEPS - 1)
            def _():
                xfin_out[c] = xn
                if c == 0:
                    for t in range(STAGES):
                        remote(xfin_out.at[c], xfin.at[y], xf_send.at[t], xf_recv.at[y], oy, t).start()
                else:
                    for t in range(STAGES - 1):
                        remote(xfin_out.at[c], xfin.at[y], xf_send.at[STAGES + t], xf_recv.at[y], y, t).start()
                    xfin[y] = xn

    def chunk_input(k, c):
        @pl.when(jnp.logical_not(is_first))
        def _():
            stage_copy(k - 1, c).wait_recv()

        @pl.when(is_first)
        def _():
            x_copy(k - 1, c).wait_recv()

        embed(k, c)

    def block(k, head, waits):
        sc0, ev0 = attn_units(0)
        sc1, ev1 = attn_units(1)
        waits[0]()
        interleave(sc0[:2])
        interleave(head + sc0[2:] + sc1, ev0)
        waits[1]()
        interleave(wo_pieces(0), ev1[:3])
        interleave(ln2_pieces(k, 0), ev1[3:5])
        waits[2]()
        interleave(up_pieces(0), ev1[5:10])
        waits[3]()
        down0 = down_pieces(k, 0)
        interleave(down0[:2], ev1[10:] + wo_pieces(1))
        interleave(down0[2:], ln2_pieces(k, 1))
        finish(k, 0)
        interleave(up_pieces(1))
        interleave(down_pieces(k, 1))
        finish(k, 1)

    embed(0, 1)
    interleave(ln1_pieces(0, 1))
    interleave(k_pieces(1) + v_pieces(1) + q_pieces(1))

    @pl.when(jnp.logical_not(is_first))
    def _():
        rc_h.wait_recv()

    @pl.when(uses_x)
    def _():
        rc_x.wait_recv()
        xs[0] = xraw[0]
        xbt[0, 0] = xraw[0].astype(BF16)

    embed(0, 0)
    interleave(ln1_pieces(0, 0))
    interleave(k_pieces(0) + q_pieces(0))
    block(0, v_pieces(0), [lambda: None, cp_rest[0].wait, lambda: [cp.wait() for cp in cp_rest[1:5]], cp_rest[5].wait])

    def step(k, _):
        chunk_input(k, 0)
        interleave(ln1_pieces(k, 0))
        interleave(k_pieces(0) + v_pieces(0))
        chunk_input(k, 1)
        interleave(q_pieces(0), ln1_pieces(k, 1))
        interleave(k_pieces(1))
        interleave(q_pieces(1))
        block(k, v_pieces(1), [lambda: None] * 4)
        return 0

    lax.fori_loop(1, STEPS, step, 0)

    remote(xfin_out.at[0], xfin.at[oy], xf_send.at[0], xf_recv.at[oy], oy, s).wait_recv()

    @pl.when(jnp.logical_not(is_last))
    def _():
        remote(xfin_out.at[0], xfin.at[y], xf_send.at[0], xf_recv.at[y], y, s).wait_recv()

    for b in range(2):
        xo_ref[b] = xfin[b]

    @pl.when(is_last)
    def _():
        for t in range(STAGES):
            remote(xfin_out.at[0], xfin.at[y], xf_send.at[t], xf_recv.at[y], oy, t).wait_send()
        for t in range(STAGES - 1):
            remote(xfin_out.at[1], xfin.at[y], xf_send.at[STAGES + t], xf_recv.at[y], y, t).wait_send()
        for k in range(STEPS - 1):
            for c in range(2):
                x_copy(k, c).wait_send()

    @pl.when(jnp.logical_not(is_last))
    def _():
        for k in range(STEPS - 1):
            for c in range(2):
                stage_copy(k, c).wait_send()

    @pl.when(jnp.logical_not(jnp.logical_or(is_first, is_last)))
    def _():
        rc_h.wait_send()

    @pl.when(uses_x)
    def _():
        rc_x.wait_send()

    last = remote(outb.at[STEPS - 1, 0], ho_ref.at[oy], ho_send, ho_recv, oy, s)
    last.wait_send()
    last.wait_recv()


def writer(x_ref, h_ref, xo_ref, ho_ref, sems):
    copies = [pltpu.make_async_copy(x_ref, xo_ref, sems.at[0]), pltpu.make_async_copy(h_ref, ho_ref, sems.at[1])]
    for copy in copies:
        copy.start()
    for copy in copies:
        copy.wait()


def solution(mesh):
    hbm = pl.BlockSpec(memory_space=pltpu.HBM)
    smem = pl.BlockSpec(memory_space=pltpu.SMEM)
    vmem = pl.BlockSpec(memory_space=pltpu.VMEM)
    dma = pltpu.SemaphoreType.DMA
    scratch = [
        pltpu.VMEM((3, DIM, DIM), BF16),
        pltpu.VMEM((DIM, DIM), BF16),
        pltpu.VMEM((4, DIM, DIM), BF16),
        pltpu.VMEM((FF, DIM), BF16),
        pltpu.VMEM((LAT, DIM), BF16),
        pltpu.VMEM((LAT, DIM), BF16),
        pltpu.VMEM((STEPS, 6, 1, DIM), F32),
        pltpu.VMEM((2, LAT, ROWS), F32),
        pltpu.VMEM((LAT, ROWS), F32),
        pltpu.VMEM((ROWS, DIM), BF16),
        pltpu.VMEM((STEPS, 2, ROWS, DIM), BF16),
        pltpu.VMEM((STEPS, 2, ROWS, DIM), BF16),
        pltpu.VMEM((STEPS, 2, LAT, ROWS), BF16),
        pltpu.VMEM((STEPS, 2, LAT, ROWS), BF16),
        pltpu.VMEM((2, LAT, ROWS), F32),
        pltpu.VMEM((2, LAT, ROWS), F32),
        pltpu.VMEM((2, LAT, ROWS), F32),
        pltpu.VMEM((2, ROWS, DIM), F32),
        pltpu.VMEM((2, ROWS, DIM), BF16),
        pltpu.VMEM((2, HEADS // 2, 2 * ROWS, 128), BF16),
        pltpu.VMEM((2, ROWS, DIM), BF16),
        pltpu.VMEM((2, DIM, ROWS), BF16),
        pltpu.VMEM((2, ROWS, DIM), BF16),
        pltpu.VMEM((2, ROWS, FF), BF16),
        pltpu.VMEM((2, HEADS // 2, 2 * ROWS, 2 * ROWS), F32),
        pltpu.VMEM((2, HEADS // 2, 2 * ROWS, 2 * ROWS), BF16),
        dma((9,)), dma((7,)), dma((2,)), dma((2,)),
        dma((STEPS - 1, 2)), dma((STEPS - 1, 2)), dma((STEPS - 1, 2)), dma((STEPS - 1, 2)),
        dma((2 * STAGES - 1,)), dma((2,)), dma, dma, pltpu.SemaphoreType.REGULAR,
    ]

    def device_fn(x_init, h_init, w_in, w_out, w_qkv, w_o, w_up, w_down, ada_mod, alpha_coef, beta_coef):
        call = pl.pallas_call(
            kernel,
            name="dit_steps",
            out_shape=(pltpu.VMEM((2, LAT, ROWS), F32), pltpu.VMEM((2, ROWS, DIM), BF16)),
            in_specs=[hbm] * 9 + [smem] * 2,
            out_specs=(vmem, vmem),
            scratch_shapes=scratch,
            compiler_params=pltpu.CompilerParams(collective_id=0, has_side_effects=True, vmem_limit_bytes=58 * 1024 * 1024),
        )
        x_final, h_final = call(x_init.swapaxes(1, 2), h_init, w_in, w_out.T, w_qkv.reshape(DIM, 3 * DIM), w_o.reshape(DIM, DIM),
                                w_up.reshape(DIM, FF), w_down.reshape(FF, DIM), ada_mod.swapaxes(1, 2), alpha_coef, beta_coef)
        x_final, h_final = pl.pallas_call(
            writer,
            name="write_out",
            out_shape=(jax.ShapeDtypeStruct(x_final.shape, F32), jax.ShapeDtypeStruct(h_final.shape, BF16)),
            in_specs=[vmem] * 2,
            out_specs=(hbm, hbm),
            scratch_shapes=[dma((2,))],
        )(pltpu.with_memory_space_constraint(x_final, pltpu.VMEM), pltpu.with_memory_space_constraint(h_final, pltpu.VMEM))
        return x_final.swapaxes(1, 2), h_final[None]

    weight_spec = P("stage", None, None)
    return jax.shard_map(
        device_fn,
        mesh=mesh,
        in_specs=(P("data", "seq", None), P(None, "data", "seq", None), P(), P(), weight_spec, P("stage", None, None, None), weight_spec, weight_spec, P(None, "stage", None, None), P(), P()),
        out_specs=(P("data", "seq", None), P("stage", "data", "seq", None)),
        check_vma=False,
    )
```

```python
import functools

import jax
import jax.numpy as jnp
from jax import lax
from jax.experimental import pallas as pl
from jax.experimental.pallas import tpu as pltpu
from jax.sharding import PartitionSpec as P

LN_EPS = 1e-6
MESH = pl.DeviceIdType.MESH
BF16 = jnp.bfloat16
F32 = jnp.float32

STEPS = 4
STAGES = 4
DIM = 768
FF = 3072
HEADS = 12
HD = 64
ROWS = 128
LAT = 48
EXP2_SCALE = HD ** -0.5 * 1.4426950408889634
GELU_C0 = 0.7978845608028654
GELU_C1 = GELU_C0 * 0.044715


def layer_norm(hidden):
    mean_val = jnp.mean(hidden, axis=-1, keepdims=True)
    centered = hidden - mean_val
    variance = jnp.mean(centered * centered, axis=-1, keepdims=True)
    return centered * lax.rsqrt(variance + LN_EPS)


def gelu(val):
    half = 0.5 * val
    return half + half * jnp.tanh(val * (GELU_C0 + GELU_C1 * (val * val)))


def mm(lhs, rhs):
    return jnp.dot(lhs, rhs, preferred_element_type=F32)


def interleave(*streams):
    order = []
    for idx, pieces in enumerate(streams):
        for pos in range(len(pieces)):
            order.append(((pos + 0.5) / len(pieces), idx, pos))
    for _, idx, pos in sorted(order):
        streams[idx][pos]()


def kernel(x_hbm, h_hbm, win_hbm, wout_hbm, wqkv_hbm, wo_hbm, wup_hbm, wdown_hbm, mod_hbm, alpha_ref, beta_ref,
           xo_ref, ho_ref,
           wqkv, wo, wup, wdown, win, wout, mod, xraw, xsend, hsend, hin, outb, xbt, xbt_out, xs, xfin_out, xfin,
           hres, unorm, qs, ks, vt, attn, act, s_scr, p_scr,
           w_sem, small_sem, init_send, init_recv, st_send, st_recv, x_send, x_recv, xf_send, xf_recv, ho_send, ho_recv, go_sem):
    y = lax.axis_index("seq")
    s = lax.axis_index("stage")
    z = lax.axis_index("data")
    oy = 1 - y
    is_first = s == 0
    is_last = s == STAGES - 1
    is_waiter = s == STAGES - 2
    uses_x = jnp.logical_or(is_first, is_last)
    h_idx = jnp.maximum(s - 1, 0)

    def local(src, dst, sem):
        return pltpu.make_async_copy(src, dst, sem)

    def remote(src, dst, ssem, rsem, yy, ss):
        return pltpu.make_async_remote_copy(src_ref=src, dst_ref=dst, send_sem=ssem, recv_sem=rsem,
                                            device_id=(z, yy, ss), device_id_type=MESH)

    cp_h = local(h_hbm.at[h_idx, y], hin.at[0, 1], small_sem.at[0])
    cp_x = local(x_hbm.at[y], xraw.at[1], small_sem.at[1])
    cp_mod = local(mod_hbm, mod, small_sem.at[2])
    cp_win = local(win_hbm, win, small_sem.at[3])
    cp_wout = local(wout_hbm, wout, small_sem.at[4])
    cp_wqkv = [local(wqkv_hbm.at[:, pl.ds(j * DIM, DIM)], wqkv.at[j], w_sem.at[j]) for j in range(3)]
    cp_rest = [local(wo_hbm, wo, w_sem.at[3])]
    cp_rest += [local(wup_hbm.at[:, pl.ds(j * DIM, DIM)], wup.at[j], w_sem.at[4 + j]) for j in range(4)]
    cp_rest += [local(wdown_hbm, wdown, w_sem.at[8])]
    cp_hs = local(h_hbm.at[h_idx, oy], hsend, small_sem.at[5])
    cp_xs = local(x_hbm.at[oy], xsend, small_sem.at[6])
    rc_h = remote(hsend, hin.at[0, 0], init_send.at[0], init_recv.at[0], oy, s)
    rc_x = remote(xsend, xraw.at[0], init_send.at[1], init_recv.at[1], oy, s)

    @pl.when(jnp.logical_not(is_first))
    def _():
        cp_hs.start()
        cp_h.start()

    cp_xs.start()
    cp_x.start()
    cp_mod.start()
    cp_win.start()
    cp_wout.start()
    for j in (1, 2, 0):
        cp_wqkv[j].start()

    barrier = pltpu.get_barrier_semaphore()
    for dy in range(2):
        for ds in range(STAGES):
            if dy == 0 and ds == 0:
                continue
            pl.semaphore_signal(barrier, inc=1, device_id=(z, (y + dy) % 2, (s + ds) % STAGES), device_id_type=MESH)
    cp_xs.wait()

    @pl.when(jnp.logical_not(is_first))
    def _():
        cp_hs.wait()

    pl.semaphore_wait(barrier, 2 * STAGES - 1)

    @pl.when(uses_x)
    def _():
        rc_x.start()

    @pl.when(jnp.logical_not(jnp.logical_or(is_first, is_waiter)))
    def _():
        rc_h.start()

    for cp in cp_rest:
        cp.start()

    @pl.when(is_last)
    def _():
        rc_h.wait_send()
        pl.semaphore_signal(go_sem, inc=1, device_id=(z, y, s - 1), device_id_type=MESH)

    @pl.when(is_waiter)
    def _():
        pl.semaphore_wait(go_sem, 1)
        rc_h.start()

    cp_x.wait()
    cp_mod.wait()
    cp_win.wait()
    cp_wout.wait()

    @pl.when(jnp.logical_not(is_first))
    def _():
        cp_h.wait()

    @pl.when(uses_x)
    def _():
        xs[1] = xraw[1]
        xbt[0, 1] = xraw[1].astype(BF16)

    for cp in cp_wqkv:
        cp.wait()

    def stage_copy(k, c):
        return remote(outb.at[k, c], hin.at[k + 1, c], st_send.at[k, c], st_recv.at[k, c], y, s + 1)

    def x_copy(k, c):
        return remote(xbt_out.at[k, c], xbt.at[k + 1, c], x_send.at[k, c], x_recv.at[k, c], y, 0)

    lane = lax.broadcasted_iota(jnp.int32, (ROWS, 128), 1)
    PAIRS = HEADS // 2
    LNB = 32

    def embed(k, c):
        @pl.when(is_first)
        def _():
            xb = xbt[k, c].astype(F32).T.astype(BF16)
            hin[k, c] = mm(xb, win[...]).astype(BF16)

    def ln1_pieces(k, c):
        def piece(r):
            def run():
                rows = pl.ds(r, LNB)
                h0 = hin[k, c, rows].astype(F32)
                unorm[c, rows] = (layer_norm(h0) * (1.0 + mod[k, 1]) + mod[k, 0]).astype(BF16)
            return run
        return [piece(r) for r in range(0, ROWS, LNB)]

    def q_pieces(c):
        def piece(n):
            def run():
                val = mm(unorm[c], wqkv[0, :, n:n + 256])
                for p in range(2):
                    part = val[:, p * 128:(p + 1) * 128]
                    qs[c, n // 128 + p, :ROWS] = jnp.where(lane < HD, part, 0.0).astype(BF16)
                    qs[c, n // 128 + p, ROWS:] = jnp.where(lane < HD, 0.0, part).astype(BF16)
            return run
        return [piece(n) for n in range(0, DIM, 256)]

    def k_pieces(c):
        def piece(n):
            def run():
                ks[c, :, n:n + 256] = mm(unorm[c], wqkv[1, :, n:n + 256]).astype(BF16)
            return run
        return [piece(n) for n in range(0, DIM, 256)]

    def v_pieces(c):
        def piece(n):
            def run():
                val = mm(unorm[c], wqkv[2, :, n:n + 256])
                vt[c, n:n + 256, :] = val.T.astype(BF16)
            return run
        return [piece(n) for n in range(0, DIM, 256)]

    def attn_units(c):
        mxs, invs = {}, {}

        def scores(p):
            cols = slice(p * 128, (p + 1) * 128)
            k2 = jnp.concatenate([ks[0, :, cols], ks[1, :, cols]], axis=0)
            st = lax.dot_general(k2, qs[c, p], (((1,), (1,)), ((), ())), preferred_element_type=F32)
            s_scr[c, p] = st
            mxs[p] = jnp.max(st, axis=0, keepdims=True)

        def exps(p, half):
            cols = slice(half * ROWS, (half + 1) * ROWS)
            ex = jnp.exp2((s_scr[c, p, :, cols] - mxs[p][:, cols]) * EXP2_SCALE)
            inv = 1.0 / jnp.sum(ex, axis=0, keepdims=True)
            p_scr[c, p, :, cols] = (ex * inv).astype(BF16)

        def values(p):
            cols = slice(p * 128, (p + 1) * 128)
            v2 = jnp.concatenate([vt[0, cols, :], vt[1, cols, :]], axis=1)
            ot = mm(v2, p_scr[c, p])
            o2 = jnp.concatenate([ot[:HD, :ROWS], ot[HD:, ROWS:]], axis=0)
            attn[c, :, cols] = o2.T.astype(BF16)

        sc = [functools.partial(scores, p) for p in range(PAIRS)]
        ev = []
        for p in range(PAIRS):
            ev.append(functools.partial(exps, p, 0))
            ev.append(functools.partial(exps, p, 1))
            if p:
                ev.append(functools.partial(values, p - 1))
        ev.append(functools.partial(values, PAIRS - 1))
        return sc, ev

    def wo_pieces(c):
        def piece(n):
            def run():
                hres[c, :, n:n + 256] = mm(attn[c], wo[:, n:n + 256])
            return run
        return [piece(n) for n in range(0, DIM, 256)]

    def ln2_pieces(k, c):
        def piece(r):
            def run():
                rows = pl.ds(r, LNB)
                h1 = hin[k, c, rows].astype(F32) + mod[k, 2] * hres[c, rows]
                hres[c, rows] = h1
                unorm[c, rows] = (layer_norm(h1) * (1.0 + mod[k, 4]) + mod[k, 3]).astype(BF16)
            return run
        return [piece(r) for r in range(0, ROWS, LNB)]

    def up_pieces(c):
        def piece(n):
            def run():
                j, m = divmod(n, DIM)
                act[c, :, n:n + 256] = gelu(mm(unorm[c], wup[j, :, m:m + 256])).astype(BF16)
            return run
        return [piece(n) for n in range(0, FF, 256)]

    def down_pieces(k, c):
        def store(n, res):
            out = hres[c, :, n:n + 256] + mod[k, 5][:, n:n + 256] * res
            outb[k, c, :, n:n + 256] = out.astype(BF16)

        def full(n):
            def run():
                store(n, mm(act[c], wdown[:, n:n + 256]))
            return run

        def halves(n):
            def run():
                lo = mm(act[c, :, :FF // 2], wdown[:FF // 2, n:n + 256])
                hi = mm(act[c, :, FF // 2:], wdown[FF // 2:, n:n + 256])
                store(n, lo + hi)
            return run
        return [full(0), full(256), halves(512)]

    def finish(k, c):
        last = isinstance(k, int) and k == STEPS - 1
        if last:
            if c == 0:
                remote(outb.at[k, c], ho_ref.at[y], ho_send, ho_recv, oy, s).start()
            else:
                ho_ref[y] = outb[k, c]
        else:
            @pl.when(jnp.logical_not(is_last))
            def _():
                stage_copy(k, c).start()

        @pl.when(is_last)
        def _():
            eps = lax.dot_general(wout[...], outb[k, c], (((1,), (1,)), ((), ())), preferred_element_type=F32)
            xn = alpha_ref[k] * xs[c] + beta_ref[k] * eps
            if not last:
                xs[c] = xn
                xbt_out[k, c] = xn.astype(BF16)
                x_copy(k, c).start()
            else:
                xfin_out[c] = xn
                if c == 0:
                    for t in range(STAGES):
                        remote(xfin_out.at[c], xfin.at[y], xf_send.at[t], xf_recv.at[y], oy, t).start()
                else:
                    for t in range(STAGES - 1):
                        remote(xfin_out.at[c], xfin.at[y], xf_send.at[STAGES + t], xf_recv.at[y], y, t).start()
                    xfin[y] = xn

    def chunk_input(k, c):
        @pl.when(jnp.logical_not(is_first))
        def _():
            stage_copy(k - 1, c).wait_recv()

        @pl.when(is_first)
        def _():
            x_copy(k - 1, c).wait_recv()

        embed(k, c)

    def block(k, head, waits):
        sc0, ev0 = attn_units(0)
        sc1, ev1 = attn_units(1)
        waits[0]()
        interleave(sc0[:2])
        interleave(head + sc0[2:] + sc1, ev0)
        waits[1]()
        interleave(wo_pieces(0), ev1[:3])
        interleave(ln2_pieces(k, 0), ev1[3:5])
        waits[2]()
        interleave(up_pieces(0), ev1[5:10])
        waits[3]()
        down0 = down_pieces(k, 0)
        interleave(down0[:2], ev1[10:] + wo_pieces(1))
        interleave(down0[2:], ln2_pieces(k, 1))
        finish(k, 0)
        interleave(up_pieces(1))
        interleave(down_pieces(k, 1))
        finish(k, 1)

    def last_block(k, head):
        sc0, ev0 = attn_units(0)
        interleave(sc0[:2])
        interleave([sc0[2], head[0], sc0[3], head[1], sc0[4], head[2], sc0[5]], ev0[:4])
        interleave(ev0[4:])
        interleave(wo_pieces(0))
        interleave(ln2_pieces(k, 0))
        interleave(up_pieces(0))
        interleave(down_pieces(k, 0))
        finish(k, 0)
        sc1, ev1 = attn_units(1)
        interleave(sc1[:2])
        interleave(sc1[2:], ev1[:4])
        interleave(ev1[4:])
        interleave(wo_pieces(1))
        interleave(ln2_pieces(k, 1))
        interleave(up_pieces(1))
        interleave(down_pieces(k, 1))
        finish(k, 1)

    embed(0, 1)
    interleave(ln1_pieces(0, 1))
    interleave(k_pieces(1) + v_pieces(1) + q_pieces(1))

    @pl.when(jnp.logical_not(is_first))
    def _():
        rc_h.wait_recv()

    @pl.when(uses_x)
    def _():
        rc_x.wait_recv()
        xs[0] = xraw[0]
        xbt[0, 0] = xraw[0].astype(BF16)

    embed(0, 0)
    interleave(ln1_pieces(0, 0))
    interleave(k_pieces(0) + q_pieces(0))
    block(0, v_pieces(0), [lambda: None, cp_rest[0].wait, lambda: [cp.wait() for cp in cp_rest[1:5]], cp_rest[5].wait])

    def enter(k):
        chunk_input(k, 0)
        interleave(ln1_pieces(k, 0))
        interleave(k_pieces(0) + v_pieces(0))
        chunk_input(k, 1)
        interleave(q_pieces(0), ln1_pieces(k, 1))
        interleave(k_pieces(1))
        interleave(q_pieces(1))

    def step(k, _):
        enter(k)
        block(k, v_pieces(1), [lambda: None] * 4)
        return 0

    lax.fori_loop(1, STEPS - 1, step, 0)
    enter(STEPS - 1)
    last_block(STEPS - 1, v_pieces(1))

    remote(xfin_out.at[0], xfin.at[oy], xf_send.at[0], xf_recv.at[oy], oy, s).wait_recv()

    @pl.when(jnp.logical_not(is_last))
    def _():
        remote(xfin_out.at[0], xfin.at[y], xf_send.at[0], xf_recv.at[y], y, s).wait_recv()

    for b in range(2):
        xo_ref[b] = xfin[b]

    @pl.when(is_last)
    def _():
        for t in range(STAGES):
            remote(xfin_out.at[0], xfin.at[y], xf_send.at[t], xf_recv.at[y], oy, t).wait_send()
        for t in range(STAGES - 1):
            remote(xfin_out.at[1], xfin.at[y], xf_send.at[STAGES + t], xf_recv.at[y], y, t).wait_send()
        for k in range(STEPS - 1):
            for c in range(2):
                x_copy(k, c).wait_send()

    @pl.when(jnp.logical_not(is_last))
    def _():
        for k in range(STEPS - 1):
            for c in range(2):
                stage_copy(k, c).wait_send()

    @pl.when(jnp.logical_not(jnp.logical_or(is_first, is_last)))
    def _():
        rc_h.wait_send()

    @pl.when(uses_x)
    def _():
        rc_x.wait_send()

    last = remote(outb.at[STEPS - 1, 0], ho_ref.at[oy], ho_send, ho_recv, oy, s)
    last.wait_send()
    last.wait_recv()


def writer(x_ref, h_ref, xo_ref, ho_ref, sems):
    copies = [pltpu.make_async_copy(x_ref, xo_ref, sems.at[0]), pltpu.make_async_copy(h_ref, ho_ref, sems.at[1])]
    for copy in copies:
        copy.start()
    for copy in copies:
        copy.wait()


def solution(mesh):
    hbm = pl.BlockSpec(memory_space=pltpu.HBM)
    smem = pl.BlockSpec(memory_space=pltpu.SMEM)
    vmem = pl.BlockSpec(memory_space=pltpu.VMEM)
    dma = pltpu.SemaphoreType.DMA
    scratch = [
        pltpu.VMEM((3, DIM, DIM), BF16),
        pltpu.VMEM((DIM, DIM), BF16),
        pltpu.VMEM((4, DIM, DIM), BF16),
        pltpu.VMEM((FF, DIM), BF16),
        pltpu.VMEM((LAT, DIM), BF16),
        pltpu.VMEM((LAT, DIM), BF16),
        pltpu.VMEM((STEPS, 6, 1, DIM), F32),
        pltpu.VMEM((2, LAT, ROWS), F32),
        pltpu.VMEM((LAT, ROWS), F32),
        pltpu.VMEM((ROWS, DIM), BF16),
        pltpu.VMEM((STEPS, 2, ROWS, DIM), BF16),
        pltpu.VMEM((STEPS, 2, ROWS, DIM), BF16),
        pltpu.VMEM((STEPS, 2, LAT, ROWS), BF16),
        pltpu.VMEM((STEPS, 2, LAT, ROWS), BF16),
        pltpu.VMEM((2, LAT, ROWS), F32),
        pltpu.VMEM((2, LAT, ROWS), F32),
        pltpu.VMEM((2, LAT, ROWS), F32),
        pltpu.VMEM((2, ROWS, DIM), F32),
        pltpu.VMEM((2, ROWS, DIM), BF16),
        pltpu.VMEM((2, HEADS // 2, 2 * ROWS, 128), BF16),
        pltpu.VMEM((2, ROWS, DIM), BF16),
        pltpu.VMEM((2, DIM, ROWS), BF16),
        pltpu.VMEM((2, ROWS, DIM), BF16),
        pltpu.VMEM((2, ROWS, FF), BF16),
        pltpu.VMEM((2, HEADS // 2, 2 * ROWS, 2 * ROWS), F32),
        pltpu.VMEM((2, HEADS // 2, 2 * ROWS, 2 * ROWS), BF16),
        dma((9,)), dma((7,)), dma((2,)), dma((2,)),
        dma((STEPS - 1, 2)), dma((STEPS - 1, 2)), dma((STEPS - 1, 2)), dma((STEPS - 1, 2)),
        dma((2 * STAGES - 1,)), dma((2,)), dma, dma, pltpu.SemaphoreType.REGULAR,
    ]

    def device_fn(x_init, h_init, w_in, w_out, w_qkv, w_o, w_up, w_down, ada_mod, alpha_coef, beta_coef):
        call = pl.pallas_call(
            kernel,
            name="dit_steps",
            out_shape=(pltpu.VMEM((2, LAT, ROWS), F32), pltpu.VMEM((2, ROWS, DIM), BF16)),
            in_specs=[hbm] * 9 + [smem] * 2,
            out_specs=(vmem, vmem),
            scratch_shapes=scratch,
            compiler_params=pltpu.CompilerParams(collective_id=0, has_side_effects=True, vmem_limit_bytes=58 * 1024 * 1024),
        )
        x_final, h_final = call(x_init.swapaxes(1, 2), h_init, w_in, w_out.T, w_qkv.reshape(DIM, 3 * DIM), w_o.reshape(DIM, DIM),
                                w_up.reshape(DIM, FF), w_down.reshape(FF, DIM), ada_mod.swapaxes(1, 2), alpha_coef, beta_coef)
        x_final, h_final = pl.pallas_call(
            writer,
            name="write_out",
            out_shape=(jax.ShapeDtypeStruct(x_final.shape, F32), jax.ShapeDtypeStruct(h_final.shape, BF16)),
            in_specs=[vmem] * 2,
            out_specs=(hbm, hbm),
            scratch_shapes=[dma((2,))],
        )(pltpu.with_memory_space_constraint(x_final, pltpu.VMEM), pltpu.with_memory_space_constraint(h_final, pltpu.VMEM))
        return x_final.swapaxes(1, 2), h_final[None]

    weight_spec = P("stage", None, None)
    return jax.shard_map(
        device_fn,
        mesh=mesh,
        in_specs=(P("data", "seq", None), P(None, "data", "seq", None), P(), P(), weight_spec, P("stage", None, None, None), weight_spec, weight_spec, P(None, "stage", None, None), P(), P()),
        out_specs=(P("data", "seq", None), P("stage", "data", "seq", None)),
        check_vma=False,
    )
```

```python
import functools

import jax
import jax.numpy as jnp
from jax import lax
from jax.experimental import pallas as pl
from jax.experimental.pallas import tpu as pltpu
from jax.sharding import PartitionSpec as P

LN_EPS = 1e-6
MESH = pl.DeviceIdType.MESH
BF16 = jnp.bfloat16
F32 = jnp.float32

STEPS = 4
STAGES = 4
DIM = 768
FF = 3072
HEADS = 12
HD = 64
ROWS = 128
LAT = 48
EXP2_SCALE = HD ** -0.5 * 1.4426950408889634
GELU_C0 = 0.7978845608028654
GELU_C1 = GELU_C0 * 0.044715


def layer_norm(hidden):
    mean_val = jnp.mean(hidden, axis=-1, keepdims=True)
    centered = hidden - mean_val
    variance = jnp.mean(centered * centered, axis=-1, keepdims=True)
    return centered * lax.rsqrt(variance + LN_EPS)


def gelu(val):
    half = 0.5 * val
    return half + half * jnp.tanh(val * (GELU_C0 + GELU_C1 * (val * val)))


def mm(lhs, rhs):
    return jnp.dot(lhs, rhs, preferred_element_type=F32)


def interleave(*streams):
    order = []
    for idx, pieces in enumerate(streams):
        for pos in range(len(pieces)):
            order.append(((pos + 0.5) / len(pieces), idx, pos))
    for _, idx, pos in sorted(order):
        streams[idx][pos]()


def kernel(x_hbm, h_hbm, win_hbm, wout_hbm, wqkv_hbm, wo_hbm, wup_hbm, wdown_hbm, mod_hbm, alpha_ref, beta_ref,
           xo_ref, ho_ref,
           wqkv, wo, wup, wdown, win, wout, mod, xraw, xsend, hsend, hin, outb, xbt, xbt_out, xs, xfin_out, xfin,
           hres, unorm, qs, ks, vt, attn, act, s_scr, p_scr,
           w_sem, small_sem, init_send, init_recv, st_send, st_recv, x_send, x_recv, xf_send, xf_recv, ho_send, ho_recv, go_sem, ready_sem):
    y = lax.axis_index("seq")
    s = lax.axis_index("stage")
    z = lax.axis_index("data")
    oy = 1 - y
    is_first = s == 0
    is_last = s == STAGES - 1
    is_waiter = s == STAGES - 2
    uses_x = jnp.logical_or(is_first, is_last)
    h_idx = jnp.maximum(s - 1, 0)

    def local(src, dst, sem):
        return pltpu.make_async_copy(src, dst, sem)

    def remote(src, dst, ssem, rsem, yy, ss):
        return pltpu.make_async_remote_copy(src_ref=src, dst_ref=dst, send_sem=ssem, recv_sem=rsem,
                                            device_id=(z, yy, ss), device_id_type=MESH)

    cp_h = local(h_hbm.at[h_idx, y], hin.at[0, 1], small_sem.at[0])
    cp_x = local(x_hbm.at[y], xraw.at[1], small_sem.at[1])
    cp_mod = local(mod_hbm, mod, small_sem.at[2])
    cp_win = local(win_hbm, win, small_sem.at[3])
    cp_wout = local(wout_hbm, wout, small_sem.at[4])
    cp_wqkv = [local(wqkv_hbm.at[:, pl.ds(j * DIM, DIM)], wqkv.at[j], w_sem.at[j]) for j in range(3)]
    cp_rest = [local(wo_hbm, wo, w_sem.at[3])]
    cp_rest += [local(wup_hbm.at[:, pl.ds(j * DIM, DIM)], wup.at[j], w_sem.at[4 + j]) for j in range(4)]
    cp_rest += [local(wdown_hbm, wdown, w_sem.at[8])]
    cp_hs = local(h_hbm.at[h_idx, oy], hsend, small_sem.at[5])
    cp_xs = local(x_hbm.at[oy], xsend, small_sem.at[6])
    rc_h = remote(hsend, hin.at[0, 0], init_send.at[0], init_recv.at[0], oy, s)
    rc_x = remote(xsend, xraw.at[0], init_send.at[1], init_recv.at[1], oy, s)

    @pl.when(jnp.logical_not(is_first))
    def _():
        cp_hs.start()
        cp_h.start()

    cp_xs.start()
    cp_x.start()
    cp_mod.start()
    cp_win.start()
    cp_wout.start()
    for j in (1, 2, 0):
        cp_wqkv[j].start()

    barrier = pltpu.get_barrier_semaphore()

    def enter_signal(yy, ss):
        pl.semaphore_signal(barrier, inc=1, device_id=(z, yy, ss), device_id_type=MESH)

    is_second = s == 1
    enter_signal(oy, s)

    @pl.when(is_first)
    def _():
        enter_signal(y, STAGES - 1)

    @pl.when(is_second)
    def _():
        enter_signal(y, 0)
        enter_signal(y, 2)

    @pl.when(is_waiter)
    def _():
        enter_signal(y, STAGES - 1)

    @pl.when(is_last)
    def _():
        enter_signal(y, STAGES - 2)

    cp_xs.wait()

    @pl.when(jnp.logical_not(is_first))
    def _():
        cp_hs.wait()

    @pl.when(is_first)
    def _():
        pl.semaphore_wait(barrier, 2)

    @pl.when(is_second)
    def _():
        pl.semaphore_wait(barrier, 1)

    @pl.when(is_waiter)
    def _():
        pl.semaphore_wait(barrier, 3)
        pl.semaphore_signal(ready_sem, inc=1, device_id=(z, y, 1), device_id_type=MESH)

    @pl.when(is_last)
    def _():
        pl.semaphore_wait(barrier, 3)


    @pl.when(uses_x)
    def _():
        rc_x.start()

    @pl.when(jnp.logical_not(jnp.logical_or(is_first, is_waiter)))
    def _():
        rc_h.start()

    for cp in cp_rest:
        cp.start()

    @pl.when(is_last)
    def _():
        rc_h.wait_send()
        pl.semaphore_signal(go_sem, inc=1, device_id=(z, y, s - 1), device_id_type=MESH)

    @pl.when(is_waiter)
    def _():
        pl.semaphore_wait(go_sem, 1)
        rc_h.start()

    cp_x.wait()
    cp_mod.wait()
    cp_win.wait()
    cp_wout.wait()

    @pl.when(jnp.logical_not(is_first))
    def _():
        cp_h.wait()

    @pl.when(uses_x)
    def _():
        xs[1] = xraw[1]
        xbt[0, 1] = xraw[1].astype(BF16)

    for cp in cp_wqkv:
        cp.wait()

    def stage_copy(k, c):
        return remote(outb.at[k, c], hin.at[k + 1, c], st_send.at[k, c], st_recv.at[k, c], y, s + 1)

    def x_copy(k, c):
        return remote(xbt_out.at[k, c], xbt.at[k + 1, c], x_send.at[k, c], x_recv.at[k, c], y, 0)

    lane = lax.broadcasted_iota(jnp.int32, (ROWS, 128), 1)
    PAIRS = HEADS // 2
    LNB = 32

    def embed(k, c):
        @pl.when(is_first)
        def _():
            xb = xbt[k, c].astype(F32).T.astype(BF16)
            hin[k, c] = mm(xb, win[...]).astype(BF16)

    def ln1_pieces(k, c):
        def piece(r):
            def run():
                rows = pl.ds(r, LNB)
                h0 = hin[k, c, rows].astype(F32)
                unorm[c, rows] = (layer_norm(h0) * (1.0 + mod[k, 1]) + mod[k, 0]).astype(BF16)
            return run
        return [piece(r) for r in range(0, ROWS, LNB)]

    def q_pieces(c):
        def piece(n):
            def run():
                val = mm(unorm[c], wqkv[0, :, n:n + 256])
                for p in range(2):
                    part = val[:, p * 128:(p + 1) * 128]
                    qs[c, n // 128 + p, :ROWS] = jnp.where(lane < HD, part, 0.0).astype(BF16)
                    qs[c, n // 128 + p, ROWS:] = jnp.where(lane < HD, 0.0, part).astype(BF16)
            return run
        return [piece(n) for n in range(0, DIM, 256)]

    def k_pieces(c):
        def piece(n):
            def run():
                ks[c, :, n:n + 256] = mm(unorm[c], wqkv[1, :, n:n + 256]).astype(BF16)
            return run
        return [piece(n) for n in range(0, DIM, 256)]

    def v_pieces(c):
        def piece(n):
            def run():
                val = mm(unorm[c], wqkv[2, :, n:n + 256])
                vt[c, n:n + 256, :] = val.T.astype(BF16)
            return run
        return [piece(n) for n in range(0, DIM, 256)]

    def attn_units(c):
        mxs, invs = {}, {}

        def scores(p):
            cols = slice(p * 128, (p + 1) * 128)
            k2 = jnp.concatenate([ks[0, :, cols], ks[1, :, cols]], axis=0)
            st = lax.dot_general(k2, qs[c, p], (((1,), (1,)), ((), ())), preferred_element_type=F32)
            s_scr[c, p] = st
            mxs[p] = jnp.max(st, axis=0, keepdims=True)

        def exps(p, half):
            cols = slice(half * ROWS, (half + 1) * ROWS)
            ex = jnp.exp2((s_scr[c, p, :, cols] - mxs[p][:, cols]) * EXP2_SCALE)
            inv = 1.0 / jnp.sum(ex, axis=0, keepdims=True)
            p_scr[c, p, :, cols] = (ex * inv).astype(BF16)

        def values(p):
            cols = slice(p * 128, (p + 1) * 128)
            v2 = jnp.concatenate([vt[0, cols, :], vt[1, cols, :]], axis=1)
            ot = mm(v2, p_scr[c, p])
            o2 = jnp.concatenate([ot[:HD, :ROWS], ot[HD:, ROWS:]], axis=0)
            attn[c, :, cols] = o2.T.astype(BF16)

        sc = [functools.partial(scores, p) for p in range(PAIRS)]
        ev = []
        for p in range(PAIRS):
            ev.append(functools.partial(exps, p, 0))
            ev.append(functools.partial(exps, p, 1))
            if p:
                ev.append(functools.partial(values, p - 1))
        ev.append(functools.partial(values, PAIRS - 1))
        return sc, ev

    def wo_pieces(c):
        def piece(n):
            def run():
                hres[c, :, n:n + 256] = mm(attn[c], wo[:, n:n + 256])
            return run
        return [piece(n) for n in range(0, DIM, 256)]

    def ln2_pieces(k, c):
        def piece(r):
            def run():
                rows = pl.ds(r, LNB)
                h1 = hin[k, c, rows].astype(F32) + mod[k, 2] * hres[c, rows]
                hres[c, rows] = h1
                unorm[c, rows] = (layer_norm(h1) * (1.0 + mod[k, 4]) + mod[k, 3]).astype(BF16)
            return run
        return [piece(r) for r in range(0, ROWS, LNB)]

    def up_pieces(c):
        def piece(n):
            def run():
                j, m = divmod(n, DIM)
                act[c, :, n:n + 256] = gelu(mm(unorm[c], wup[j, :, m:m + 256])).astype(BF16)
            return run
        return [piece(n) for n in range(0, FF, 256)]

    def down_pieces(k, c):
        def store(n, res):
            out = hres[c, :, n:n + 256] + mod[k, 5][:, n:n + 256] * res
            outb[k, c, :, n:n + 256] = out.astype(BF16)

        def full(n):
            def run():
                store(n, mm(act[c], wdown[:, n:n + 256]))
            return run

        def halves(n):
            def run():
                lo = mm(act[c, :, :FF // 2], wdown[:FF // 2, n:n + 256])
                hi = mm(act[c, :, FF // 2:], wdown[FF // 2:, n:n + 256])
                store(n, lo + hi)
            return run
        return [full(0), full(256), halves(512)]

    def finish(k, c):
        last = isinstance(k, int) and k == STEPS - 1
        if last:
            if c == 0:
                remote(outb.at[k, c], ho_ref.at[y], ho_send, ho_recv, oy, s).start()
            else:
                ho_ref[y] = outb[k, c]
        else:
            @pl.when(jnp.logical_not(is_last))
            def _():
                stage_copy(k, c).start()

        @pl.when(is_last)
        def _():
            eps = lax.dot_general(wout[...], outb[k, c], (((1,), (1,)), ((), ())), preferred_element_type=F32)
            xn = alpha_ref[k] * xs[c] + beta_ref[k] * eps
            if not last:
                xs[c] = xn
                xbt_out[k, c] = xn.astype(BF16)
                x_copy(k, c).start()
            else:
                xfin_out[c] = xn
                if c == 0:
                    for t in range(STAGES):
                        remote(xfin_out.at[c], xfin.at[y], xf_send.at[t], xf_recv.at[y], oy, t).start()
                else:
                    for t in range(STAGES - 1):
                        remote(xfin_out.at[c], xfin.at[y], xf_send.at[STAGES + t], xf_recv.at[y], y, t).start()
                    xfin[y] = xn

    def chunk_input(k, c):
        @pl.when(jnp.logical_not(is_first))
        def _():
            stage_copy(k - 1, c).wait_recv()

        @pl.when(is_first)
        def _():
            x_copy(k - 1, c).wait_recv()

        embed(k, c)

    def block(k, head, waits):
        sc0, ev0 = attn_units(0)
        sc1, ev1 = attn_units(1)
        waits[0]()
        interleave(sc0[:2])
        interleave(head + sc0[2:] + sc1, ev0)
        waits[1]()
        interleave(wo_pieces(0), ev1[:3])
        interleave(ln2_pieces(k, 0), ev1[3:5])
        waits[2]()
        interleave(up_pieces(0), ev1[5:10])
        waits[3]()
        down0 = down_pieces(k, 0)
        interleave(down0[:2], ev1[10:] + wo_pieces(1))
        interleave(down0[2:], ln2_pieces(k, 1))
        finish(k, 0)
        interleave(up_pieces(1))
        interleave(down_pieces(k, 1))
        finish(k, 1)

    def last_block(k, head):
        sc0, ev0 = attn_units(0)
        interleave(sc0[:2])
        interleave([sc0[2], head[0], sc0[3], head[1], sc0[4], head[2], sc0[5]], ev0[:4])
        interleave(ev0[4:])
        interleave(wo_pieces(0))
        interleave(ln2_pieces(k, 0))
        interleave(up_pieces(0))
        interleave(down_pieces(k, 0))
        finish(k, 0)
        sc1, ev1 = attn_units(1)
        interleave(sc1[:2])
        interleave(sc1[2:], ev1[:4])
        interleave(ev1[4:])
        interleave(wo_pieces(1))
        interleave(ln2_pieces(k, 1))
        interleave(up_pieces(1))
        interleave(down_pieces(k, 1))
        finish(k, 1)

    embed(0, 1)
    interleave(ln1_pieces(0, 1))
    interleave(k_pieces(1) + v_pieces(1) + q_pieces(1))

    @pl.when(jnp.logical_not(is_first))
    def _():
        rc_h.wait_recv()

    @pl.when(uses_x)
    def _():
        rc_x.wait_recv()
        xs[0] = xraw[0]
        xbt[0, 0] = xraw[0].astype(BF16)

    @pl.when(is_second)
    def _():
        pl.semaphore_wait(ready_sem, 1)

    embed(0, 0)
    interleave(ln1_pieces(0, 0))
    interleave(k_pieces(0) + q_pieces(0))
    block(0, v_pieces(0), [lambda: None, cp_rest[0].wait, lambda: [cp.wait() for cp in cp_rest[1:5]], cp_rest[5].wait])

    def enter(k):
        chunk_input(k, 0)
        interleave(ln1_pieces(k, 0))
        interleave(k_pieces(0) + v_pieces(0))
        chunk_input(k, 1)
        interleave(q_pieces(0), ln1_pieces(k, 1))
        interleave(k_pieces(1))
        interleave(q_pieces(1))

    def step(k, _):
        enter(k)
        block(k, v_pieces(1), [lambda: None] * 4)
        return 0

    lax.fori_loop(1, STEPS - 1, step, 0)
    enter(STEPS - 1)
    last_block(STEPS - 1, v_pieces(1))

    remote(xfin_out.at[0], xfin.at[oy], xf_send.at[0], xf_recv.at[oy], oy, s).wait_recv()

    @pl.when(jnp.logical_not(is_last))
    def _():
        remote(xfin_out.at[0], xfin.at[y], xf_send.at[0], xf_recv.at[y], y, s).wait_recv()

    for b in range(2):
        xo_ref[b] = xfin[b]

    @pl.when(is_last)
    def _():
        for t in range(STAGES):
            remote(xfin_out.at[0], xfin.at[y], xf_send.at[t], xf_recv.at[y], oy, t).wait_send()
        for t in range(STAGES - 1):
            remote(xfin_out.at[1], xfin.at[y], xf_send.at[STAGES + t], xf_recv.at[y], y, t).wait_send()
        for k in range(STEPS - 1):
            for c in range(2):
                x_copy(k, c).wait_send()

    @pl.when(jnp.logical_not(is_last))
    def _():
        for k in range(STEPS - 1):
            for c in range(2):
                stage_copy(k, c).wait_send()

    @pl.when(jnp.logical_not(jnp.logical_or(is_first, is_last)))
    def _():
        rc_h.wait_send()

    @pl.when(uses_x)
    def _():
        rc_x.wait_send()

    last = remote(outb.at[STEPS - 1, 0], ho_ref.at[oy], ho_send, ho_recv, oy, s)
    last.wait_send()
    last.wait_recv()


def writer(x_ref, h_ref, xo_ref, ho_ref, sems):
    copies = [pltpu.make_async_copy(x_ref, xo_ref, sems.at[0]), pltpu.make_async_copy(h_ref, ho_ref, sems.at[1])]
    for copy in copies:
        copy.start()
    for copy in copies:
        copy.wait()


def solution(mesh):
    hbm = pl.BlockSpec(memory_space=pltpu.HBM)
    smem = pl.BlockSpec(memory_space=pltpu.SMEM)
    vmem = pl.BlockSpec(memory_space=pltpu.VMEM)
    dma = pltpu.SemaphoreType.DMA
    scratch = [
        pltpu.VMEM((3, DIM, DIM), BF16),
        pltpu.VMEM((DIM, DIM), BF16),
        pltpu.VMEM((4, DIM, DIM), BF16),
        pltpu.VMEM((FF, DIM), BF16),
        pltpu.VMEM((LAT, DIM), BF16),
        pltpu.VMEM((LAT, DIM), BF16),
        pltpu.VMEM((STEPS, 6, 1, DIM), F32),
        pltpu.VMEM((2, LAT, ROWS), F32),
        pltpu.VMEM((LAT, ROWS), F32),
        pltpu.VMEM((ROWS, DIM), BF16),
        pltpu.VMEM((STEPS, 2, ROWS, DIM), BF16),
        pltpu.VMEM((STEPS, 2, ROWS, DIM), BF16),
        pltpu.VMEM((STEPS, 2, LAT, ROWS), BF16),
        pltpu.VMEM((STEPS, 2, LAT, ROWS), BF16),
        pltpu.VMEM((2, LAT, ROWS), F32),
        pltpu.VMEM((2, LAT, ROWS), F32),
        pltpu.VMEM((2, LAT, ROWS), F32),
        pltpu.VMEM((2, ROWS, DIM), F32),
        pltpu.VMEM((2, ROWS, DIM), BF16),
        pltpu.VMEM((2, HEADS // 2, 2 * ROWS, 128), BF16),
        pltpu.VMEM((2, ROWS, DIM), BF16),
        pltpu.VMEM((2, DIM, ROWS), BF16),
        pltpu.VMEM((2, ROWS, DIM), BF16),
        pltpu.VMEM((2, ROWS, FF), BF16),
        pltpu.VMEM((2, HEADS // 2, 2 * ROWS, 2 * ROWS), F32),
        pltpu.VMEM((2, HEADS // 2, 2 * ROWS, 2 * ROWS), BF16),
        dma((9,)), dma((7,)), dma((2,)), dma((2,)),
        dma((STEPS - 1, 2)), dma((STEPS - 1, 2)), dma((STEPS - 1, 2)), dma((STEPS - 1, 2)),
        dma((2 * STAGES - 1,)), dma((2,)), dma, dma, pltpu.SemaphoreType.REGULAR, pltpu.SemaphoreType.REGULAR,
    ]

    def device_fn(x_init, h_init, w_in, w_out, w_qkv, w_o, w_up, w_down, ada_mod, alpha_coef, beta_coef):
        call = pl.pallas_call(
            kernel,
            name="dit_steps",
            out_shape=(pltpu.VMEM((2, LAT, ROWS), F32), pltpu.VMEM((2, ROWS, DIM), BF16)),
            in_specs=[hbm] * 9 + [smem] * 2,
            out_specs=(vmem, vmem),
            scratch_shapes=scratch,
            compiler_params=pltpu.CompilerParams(collective_id=0, has_side_effects=True, vmem_limit_bytes=58 * 1024 * 1024),
        )
        x_final, h_final = call(x_init.swapaxes(1, 2), h_init, w_in, w_out.T, w_qkv.reshape(DIM, 3 * DIM), w_o.reshape(DIM, DIM),
                                w_up.reshape(DIM, FF), w_down.reshape(FF, DIM), ada_mod.swapaxes(1, 2), alpha_coef, beta_coef)
        x_final, h_final = pl.pallas_call(
            writer,
            name="write_out",
            out_shape=(jax.ShapeDtypeStruct(x_final.shape, F32), jax.ShapeDtypeStruct(h_final.shape, BF16)),
            in_specs=[vmem] * 2,
            out_specs=(hbm, hbm),
            scratch_shapes=[dma((2,))],
        )(pltpu.with_memory_space_constraint(x_final, pltpu.VMEM), pltpu.with_memory_space_constraint(h_final, pltpu.VMEM))
        return x_final.swapaxes(1, 2), h_final[None]

    weight_spec = P("stage", None, None)
    return jax.shard_map(
        device_fn,
        mesh=mesh,
        in_specs=(P("data", "seq", None), P(None, "data", "seq", None), P(), P(), weight_spec, P("stage", None, None, None), weight_spec, weight_spec, P(None, "stage", None, None), P(), P()),
        out_specs=(P("data", "seq", None), P("stage", "data", "seq", None)),
        check_vma=False,
    )
```

```python
import functools

import jax
import jax.numpy as jnp
from jax import lax
from jax.experimental import pallas as pl
from jax.experimental.pallas import tpu as pltpu
from jax.sharding import PartitionSpec as P

LN_EPS = 1e-6
MESH = pl.DeviceIdType.MESH
BF16 = jnp.bfloat16
F32 = jnp.float32

STEPS = 4
STAGES = 4
DIM = 768
FF = 3072
HEADS = 12
HD = 64
ROWS = 128
LAT = 48
EXP2_SCALE = HD ** -0.5 * 1.4426950408889634
GELU_C0 = 0.7978845608028654
GELU_C1 = GELU_C0 * 0.044715


def layer_norm(hidden):
    mean_val = jnp.mean(hidden, axis=-1, keepdims=True)
    centered = hidden - mean_val
    variance = jnp.mean(centered * centered, axis=-1, keepdims=True)
    return centered * lax.rsqrt(variance + LN_EPS)


def gelu(val):
    half = 0.5 * val
    return half + half * jnp.tanh(val * (GELU_C0 + GELU_C1 * (val * val)))


def mm(lhs, rhs):
    return jnp.dot(lhs, rhs, preferred_element_type=F32)


def interleave(*streams):
    order = []
    for idx, pieces in enumerate(streams):
        for pos in range(len(pieces)):
            order.append(((pos + 0.5) / len(pieces), idx, pos))
    for _, idx, pos in sorted(order):
        streams[idx][pos]()


def kernel(x_hbm, h_hbm, win_hbm, wout_hbm, wqkv_hbm, wo_hbm, wup_hbm, wdown_hbm, mod_hbm, alpha_ref, beta_ref,
           xo_ref, ho_ref,
           wqkv, wo, wup, wdown, win, wout, mod, xraw, xsend, hsend, hin, outb, xbt, xbt_out, xs, xfin_out, xfin,
           hres, unorm, qs, ks, vt, attn, act, s_scr, p_scr,
           w_sem, small_sem, init_send, init_recv, st_send, st_recv, x_send, x_recv, xf_send, xf_recv, ho_send, ho_recv, ready_sem):
    y = lax.axis_index("seq")
    s = lax.axis_index("stage")
    z = lax.axis_index("data")
    oy = 1 - y
    is_first = s == 0
    is_last = s == STAGES - 1
    is_waiter = s == STAGES - 2
    uses_x = jnp.logical_or(is_first, is_last)
    h_idx = jnp.maximum(s - 1, 0)

    def local(src, dst, sem):
        return pltpu.make_async_copy(src, dst, sem)

    def remote(src, dst, ssem, rsem, yy, ss):
        return pltpu.make_async_remote_copy(src_ref=src, dst_ref=dst, send_sem=ssem, recv_sem=rsem,
                                            device_id=(z, yy, ss), device_id_type=MESH)

    cp_h = local(h_hbm.at[h_idx, y], hin.at[0, 1], small_sem.at[0])
    cp_x = local(x_hbm.at[y], xraw.at[1], small_sem.at[1])
    cp_mod = local(mod_hbm, mod, small_sem.at[2])
    cp_win = local(win_hbm, win, small_sem.at[3])
    cp_wout = local(wout_hbm, wout, small_sem.at[4])
    cp_wqkv = [local(wqkv_hbm.at[:, pl.ds(j * DIM, DIM)], wqkv.at[j], w_sem.at[j]) for j in range(3)]
    cp_rest = [local(wo_hbm, wo, w_sem.at[3])]
    cp_rest += [local(wup_hbm.at[:, pl.ds(j * DIM, DIM)], wup.at[j], w_sem.at[4 + j]) for j in range(4)]
    cp_rest += [local(wdown_hbm, wdown, w_sem.at[8])]
    cp_hs = local(h_hbm.at[h_idx, oy], hsend, small_sem.at[5])
    cp_xs = local(x_hbm.at[oy], xsend, small_sem.at[6])
    rc_h = remote(hsend, hin.at[0, 0], init_send.at[0], init_recv.at[0], oy, s)
    rc_x = remote(xsend, xraw.at[0], init_send.at[1], init_recv.at[1], oy, s)

    @pl.when(jnp.logical_not(is_first))
    def _():
        cp_hs.start()
        cp_h.start()

    cp_xs.start()
    cp_x.start()
    cp_mod.start()
    cp_win.start()
    cp_wout.start()
    for j in (1, 2, 0):
        cp_wqkv[j].start()

    barrier = pltpu.get_barrier_semaphore()

    def enter_signal(yy, ss):
        pl.semaphore_signal(barrier, inc=1, device_id=(z, yy, ss), device_id_type=MESH)

    is_second = s == 1
    enter_signal(oy, s)

    @pl.when(is_first)
    def _():
        enter_signal(y, STAGES - 1)

    @pl.when(is_second)
    def _():
        enter_signal(y, 0)
        enter_signal(y, 2)

    @pl.when(is_waiter)
    def _():
        enter_signal(y, STAGES - 1)

    @pl.when(is_last)
    def _():
        enter_signal(y, STAGES - 2)

    cp_xs.wait()

    @pl.when(jnp.logical_not(is_first))
    def _():
        cp_hs.wait()

    @pl.when(is_first)
    def _():
        pl.semaphore_wait(barrier, 2)

    @pl.when(is_second)
    def _():
        pl.semaphore_wait(barrier, 1)

    @pl.when(is_waiter)
    def _():
        pl.semaphore_wait(barrier, 3)
        pl.semaphore_signal(ready_sem, inc=1, device_id=(z, y, 1), device_id_type=MESH)

    @pl.when(is_last)
    def _():
        pl.semaphore_wait(barrier, 3)


    @pl.when(uses_x)
    def _():
        rc_x.start()

    @pl.when(jnp.logical_not(is_first))
    def _():
        rc_h.start()

    for cp in cp_rest:
        cp.start()

    cp_x.wait()
    cp_mod.wait()
    cp_win.wait()
    cp_wout.wait()

    @pl.when(jnp.logical_not(is_first))
    def _():
        cp_h.wait()

    @pl.when(uses_x)
    def _():
        xs[1] = xraw[1]
        xbt[0, 1] = xraw[1].astype(BF16)

    for cp in cp_wqkv:
        cp.wait()

    def stage_copy(k, c):
        return remote(outb.at[k, c], hin.at[k + 1, c], st_send.at[k, c], st_recv.at[k, c], y, s + 1)

    def x_copy(k, c):
        return remote(xbt_out.at[k, c], xbt.at[k + 1, c], x_send.at[k, c], x_recv.at[k, c], y, 0)

    lane = lax.broadcasted_iota(jnp.int32, (ROWS, 128), 1)
    PAIRS = HEADS // 2
    LNB = 32

    def embed(k, c):
        @pl.when(is_first)
        def _():
            xb = xbt[k, c].astype(F32).T.astype(BF16)
            hin[k, c] = mm(xb, win[...]).astype(BF16)

    def ln1_pieces(k, c):
        def piece(r):
            def run():
                rows = pl.ds(r, LNB)
                h0 = hin[k, c, rows].astype(F32)
                unorm[c, rows] = (layer_norm(h0) * (1.0 + mod[k, 1]) + mod[k, 0]).astype(BF16)
            return run
        return [piece(r) for r in range(0, ROWS, LNB)]

    def q_pieces(c):
        def piece(n):
            def run():
                val = mm(unorm[c], wqkv[0, :, n:n + 256])
                for p in range(2):
                    part = val[:, p * 128:(p + 1) * 128]
                    qs[c, n // 128 + p, :ROWS] = jnp.where(lane < HD, part, 0.0).astype(BF16)
                    qs[c, n // 128 + p, ROWS:] = jnp.where(lane < HD, 0.0, part).astype(BF16)
            return run
        return [piece(n) for n in range(0, DIM, 256)]

    def k_pieces(c):
        def piece(n):
            def run():
                ks[c, :, n:n + 256] = mm(unorm[c], wqkv[1, :, n:n + 256]).astype(BF16)
            return run
        return [piece(n) for n in range(0, DIM, 256)]

    def v_pieces(c):
        def piece(n):
            def run():
                val = mm(unorm[c], wqkv[2, :, n:n + 256])
                vt[c, n:n + 256, :] = val.T.astype(BF16)
            return run
        return [piece(n) for n in range(0, DIM, 256)]

    def attn_units(c):
        mxs, invs = {}, {}

        def scores(p):
            cols = slice(p * 128, (p + 1) * 128)
            k2 = jnp.concatenate([ks[0, :, cols], ks[1, :, cols]], axis=0)
            st = lax.dot_general(k2, qs[c, p], (((1,), (1,)), ((), ())), preferred_element_type=F32)
            s_scr[c, p] = st
            mxs[p] = jnp.max(st, axis=0, keepdims=True)

        def exps(p, half):
            cols = slice(half * ROWS, (half + 1) * ROWS)
            ex = jnp.exp2((s_scr[c, p, :, cols] - mxs[p][:, cols]) * EXP2_SCALE)
            inv = 1.0 / jnp.sum(ex, axis=0, keepdims=True)
            p_scr[c, p, :, cols] = (ex * inv).astype(BF16)

        def values(p):
            cols = slice(p * 128, (p + 1) * 128)
            v2 = jnp.concatenate([vt[0, cols, :], vt[1, cols, :]], axis=1)
            ot = mm(v2, p_scr[c, p])
            o2 = jnp.concatenate([ot[:HD, :ROWS], ot[HD:, ROWS:]], axis=0)
            attn[c, :, cols] = o2.T.astype(BF16)

        sc = [functools.partial(scores, p) for p in range(PAIRS)]
        ev = []
        for p in range(PAIRS):
            ev.append(functools.partial(exps, p, 0))
            ev.append(functools.partial(exps, p, 1))
            if p:
                ev.append(functools.partial(values, p - 1))
        ev.append(functools.partial(values, PAIRS - 1))
        return sc, ev

    def wo_pieces(c):
        def piece(n):
            def run():
                hres[c, :, n:n + 256] = mm(attn[c], wo[:, n:n + 256])
            return run
        return [piece(n) for n in range(0, DIM, 256)]

    def ln2_pieces(k, c):
        def piece(r):
            def run():
                rows = pl.ds(r, LNB)
                h1 = hin[k, c, rows].astype(F32) + mod[k, 2] * hres[c, rows]
                hres[c, rows] = h1
                unorm[c, rows] = (layer_norm(h1) * (1.0 + mod[k, 4]) + mod[k, 3]).astype(BF16)
            return run
        return [piece(r) for r in range(0, ROWS, LNB)]

    def up_pieces(c):
        def piece(n):
            def run():
                j, m = divmod(n, DIM)
                act[c, :, n:n + 256] = gelu(mm(unorm[c], wup[j, :, m:m + 256])).astype(BF16)
            return run
        return [piece(n) for n in range(0, FF, 256)]

    def down_pieces(k, c):
        def store(n, res):
            out = hres[c, :, n:n + 256] + mod[k, 5][:, n:n + 256] * res
            outb[k, c, :, n:n + 256] = out.astype(BF16)

        def full(n):
            def run():
                store(n, mm(act[c], wdown[:, n:n + 256]))
            return run

        def halves(n):
            def run():
                lo = mm(act[c, :, :FF // 2], wdown[:FF // 2, n:n + 256])
                hi = mm(act[c, :, FF // 2:], wdown[FF // 2:, n:n + 256])
                store(n, lo + hi)
            return run
        return [full(0), full(256), halves(512)]

    def finish(k, c):
        last = isinstance(k, int) and k == STEPS - 1
        if last:
            if c == 0:
                remote(outb.at[k, c], ho_ref.at[y], ho_send, ho_recv, oy, s).start()
            else:
                ho_ref[y] = outb[k, c]
        else:
            @pl.when(jnp.logical_not(is_last))
            def _():
                stage_copy(k, c).start()

        @pl.when(is_last)
        def _():
            eps = lax.dot_general(wout[...], outb[k, c], (((1,), (1,)), ((), ())), preferred_element_type=F32)
            xn = alpha_ref[k] * xs[c] + beta_ref[k] * eps
            if not last:
                xs[c] = xn
                xbt_out[k, c] = xn.astype(BF16)
                x_copy(k, c).start()
            else:
                xfin_out[c] = xn
                if c == 0:
                    for t in range(STAGES):
                        remote(xfin_out.at[c], xfin.at[y], xf_send.at[t], xf_recv.at[y], oy, t).start()
                else:
                    for t in range(STAGES - 1):
                        remote(xfin_out.at[c], xfin.at[y], xf_send.at[STAGES + t], xf_recv.at[y], y, t).start()
                    xfin[y] = xn

    def chunk_input(k, c):
        @pl.when(jnp.logical_not(is_first))
        def _():
            stage_copy(k - 1, c).wait_recv()

        @pl.when(is_first)
        def _():
            x_copy(k - 1, c).wait_recv()

        embed(k, c)

    def block(k, head, waits):
        sc0, ev0 = attn_units(0)
        sc1, ev1 = attn_units(1)
        waits[0]()
        interleave(sc0[:2])
        interleave(head + sc0[2:] + sc1, ev0)
        waits[1]()
        interleave(wo_pieces(0), ev1[:3])
        interleave(ln2_pieces(k, 0), ev1[3:5])
        waits[2]()
        interleave(up_pieces(0), ev1[5:10])
        waits[3]()
        down0 = down_pieces(k, 0)
        interleave(down0[:2], ev1[10:] + wo_pieces(1))
        interleave(down0[2:], ln2_pieces(k, 1))
        finish(k, 0)
        interleave(up_pieces(1))
        interleave(down_pieces(k, 1))
        finish(k, 1)

    def last_block(k, head):
        sc0, ev0 = attn_units(0)
        interleave(sc0[:2])
        interleave([sc0[2], head[0], sc0[3], head[1], sc0[4], head[2], sc0[5]], ev0[:4])
        interleave(ev0[4:])
        interleave(wo_pieces(0))
        interleave(ln2_pieces(k, 0))
        interleave(up_pieces(0))
        interleave(down_pieces(k, 0))
        finish(k, 0)
        sc1, ev1 = attn_units(1)
        interleave(sc1[:2])
        interleave(sc1[2:], ev1[:4])
        interleave(ev1[4:])
        interleave(wo_pieces(1))
        interleave(ln2_pieces(k, 1))
        interleave(up_pieces(1))
        interleave(down_pieces(k, 1))
        finish(k, 1)

    embed(0, 1)
    interleave(ln1_pieces(0, 1))
    interleave(k_pieces(1) + v_pieces(1) + q_pieces(1))

    @pl.when(jnp.logical_not(is_first))
    def _():
        rc_h.wait_recv()

    @pl.when(uses_x)
    def _():
        rc_x.wait_recv()
        xs[0] = xraw[0]
        xbt[0, 0] = xraw[0].astype(BF16)

    @pl.when(is_second)
    def _():
        pl.semaphore_wait(ready_sem, 1)

    embed(0, 0)
    interleave(ln1_pieces(0, 0))
    interleave(k_pieces(0) + q_pieces(0))
    block(0, v_pieces(0), [lambda: None, cp_rest[0].wait, lambda: [cp.wait() for cp in cp_rest[1:5]], cp_rest[5].wait])

    def enter(k):
        chunk_input(k, 0)
        interleave(ln1_pieces(k, 0))
        interleave(k_pieces(0) + v_pieces(0))
        chunk_input(k, 1)
        interleave(q_pieces(0), ln1_pieces(k, 1))
        interleave(k_pieces(1))
        interleave(q_pieces(1))

    def step(k, _):
        enter(k)
        block(k, v_pieces(1), [lambda: None] * 4)
        return 0

    lax.fori_loop(1, STEPS - 1, step, 0)
    enter(STEPS - 1)
    last_block(STEPS - 1, v_pieces(1))

    remote(xfin_out.at[0], xfin.at[oy], xf_send.at[0], xf_recv.at[oy], oy, s).wait_recv()

    @pl.when(jnp.logical_not(is_last))
    def _():
        remote(xfin_out.at[0], xfin.at[y], xf_send.at[0], xf_recv.at[y], y, s).wait_recv()

    for b in range(2):
        xo_ref[b] = xfin[b]

    @pl.when(is_last)
    def _():
        for t in range(STAGES):
            remote(xfin_out.at[0], xfin.at[y], xf_send.at[t], xf_recv.at[y], oy, t).wait_send()
        for t in range(STAGES - 1):
            remote(xfin_out.at[1], xfin.at[y], xf_send.at[STAGES + t], xf_recv.at[y], y, t).wait_send()
        for k in range(STEPS - 1):
            for c in range(2):
                x_copy(k, c).wait_send()

    @pl.when(jnp.logical_not(is_last))
    def _():
        for k in range(STEPS - 1):
            for c in range(2):
                stage_copy(k, c).wait_send()

    @pl.when(jnp.logical_not(is_first))
    def _():
        rc_h.wait_send()

    @pl.when(uses_x)
    def _():
        rc_x.wait_send()

    last = remote(outb.at[STEPS - 1, 0], ho_ref.at[oy], ho_send, ho_recv, oy, s)
    last.wait_send()
    last.wait_recv()


def writer(x_ref, h_ref, xo_ref, ho_ref, sems):
    copies = [pltpu.make_async_copy(x_ref, xo_ref, sems.at[0]), pltpu.make_async_copy(h_ref, ho_ref, sems.at[1])]
    for copy in copies:
        copy.start()
    for copy in copies:
        copy.wait()


def solution(mesh):
    hbm = pl.BlockSpec(memory_space=pltpu.HBM)
    smem = pl.BlockSpec(memory_space=pltpu.SMEM)
    vmem = pl.BlockSpec(memory_space=pltpu.VMEM)
    dma = pltpu.SemaphoreType.DMA
    scratch = [
        pltpu.VMEM((3, DIM, DIM), BF16),
        pltpu.VMEM((DIM, DIM), BF16),
        pltpu.VMEM((4, DIM, DIM), BF16),
        pltpu.VMEM((FF, DIM), BF16),
        pltpu.VMEM((LAT, DIM), BF16),
        pltpu.VMEM((LAT, DIM), BF16),
        pltpu.VMEM((STEPS, 6, 1, DIM), F32),
        pltpu.VMEM((2, LAT, ROWS), F32),
        pltpu.VMEM((LAT, ROWS), F32),
        pltpu.VMEM((ROWS, DIM), BF16),
        pltpu.VMEM((STEPS, 2, ROWS, DIM), BF16),
        pltpu.VMEM((STEPS, 2, ROWS, DIM), BF16),
        pltpu.VMEM((STEPS, 2, LAT, ROWS), BF16),
        pltpu.VMEM((STEPS, 2, LAT, ROWS), BF16),
        pltpu.VMEM((2, LAT, ROWS), F32),
        pltpu.VMEM((2, LAT, ROWS), F32),
        pltpu.VMEM((2, LAT, ROWS), F32),
        pltpu.VMEM((2, ROWS, DIM), F32),
        pltpu.VMEM((2, ROWS, DIM), BF16),
        pltpu.VMEM((2, HEADS // 2, 2 * ROWS, 128), BF16),
        pltpu.VMEM((2, ROWS, DIM), BF16),
        pltpu.VMEM((2, DIM, ROWS), BF16),
        pltpu.VMEM((2, ROWS, DIM), BF16),
        pltpu.VMEM((2, ROWS, FF), BF16),
        pltpu.VMEM((2, HEADS // 2, 2 * ROWS, 2 * ROWS), F32),
        pltpu.VMEM((2, HEADS // 2, 2 * ROWS, 2 * ROWS), BF16),
        dma((9,)), dma((7,)), dma((2,)), dma((2,)),
        dma((STEPS - 1, 2)), dma((STEPS - 1, 2)), dma((STEPS - 1, 2)), dma((STEPS - 1, 2)),
        dma((2 * STAGES - 1,)), dma((2,)), dma, dma, pltpu.SemaphoreType.REGULAR,
    ]

    def device_fn(x_init, h_init, w_in, w_out, w_qkv, w_o, w_up, w_down, ada_mod, alpha_coef, beta_coef):
        call = pl.pallas_call(
            kernel,
            name="dit_steps",
            out_shape=(pltpu.VMEM((2, LAT, ROWS), F32), pltpu.VMEM((2, ROWS, DIM), BF16)),
            in_specs=[hbm] * 9 + [smem] * 2,
            out_specs=(vmem, vmem),
            scratch_shapes=scratch,
            compiler_params=pltpu.CompilerParams(collective_id=0, has_side_effects=True, vmem_limit_bytes=58 * 1024 * 1024),
        )
        x_final, h_final = call(x_init.swapaxes(1, 2), h_init, w_in, w_out.T, w_qkv.reshape(DIM, 3 * DIM), w_o.reshape(DIM, DIM),
                                w_up.reshape(DIM, FF), w_down.reshape(FF, DIM), ada_mod.swapaxes(1, 2), alpha_coef, beta_coef)
        x_final, h_final = pl.pallas_call(
            writer,
            name="write_out",
            out_shape=(jax.ShapeDtypeStruct(x_final.shape, F32), jax.ShapeDtypeStruct(h_final.shape, BF16)),
            in_specs=[vmem] * 2,
            out_specs=(hbm, hbm),
            scratch_shapes=[dma((2,))],
        )(pltpu.with_memory_space_constraint(x_final, pltpu.VMEM), pltpu.with_memory_space_constraint(h_final, pltpu.VMEM))
        return x_final.swapaxes(1, 2), h_final[None]

    weight_spec = P("stage", None, None)
    return jax.shard_map(
        device_fn,
        mesh=mesh,
        in_specs=(P("data", "seq", None), P(None, "data", "seq", None), P(), P(), weight_spec, P("stage", None, None, None), weight_spec, weight_spec, P(None, "stage", None, None), P(), P()),
        out_specs=(P("data", "seq", None), P("stage", "data", "seq", None)),
        check_vma=False,
    )
```

```python
import functools

import jax
import jax.numpy as jnp
from jax import lax
from jax.experimental import pallas as pl
from jax.experimental.pallas import tpu as pltpu
from jax.sharding import PartitionSpec as P

LN_EPS = 1e-6
MESH = pl.DeviceIdType.MESH
BF16 = jnp.bfloat16
F32 = jnp.float32

STEPS = 4
STAGES = 4
DIM = 768
FF = 3072
HEADS = 12
HD = 64
ROWS = 128
LAT = 48
EXP2_SCALE = HD ** -0.5 * 1.4426950408889634
GELU_C0 = 0.7978845608028654
GELU_C1 = GELU_C0 * 0.044715


def layer_norm(hidden):
    mean_val = jnp.mean(hidden, axis=-1, keepdims=True)
    centered = hidden - mean_val
    variance = jnp.mean(centered * centered, axis=-1, keepdims=True)
    return centered * lax.rsqrt(variance + LN_EPS)


def gelu(val):
    half = 0.5 * val
    return half + half * jnp.tanh(val * (GELU_C0 + GELU_C1 * (val * val)))


def mm(lhs, rhs):
    return jnp.dot(lhs, rhs, preferred_element_type=F32)


def interleave(*streams):
    order = []
    for idx, pieces in enumerate(streams):
        for pos in range(len(pieces)):
            order.append(((pos + 0.5) / len(pieces), idx, pos))
    for _, idx, pos in sorted(order):
        streams[idx][pos]()


def kernel(x_hbm, h_hbm, win_hbm, wout_hbm, wqkv_hbm, wo_hbm, wup_hbm, wdown_hbm, mod_hbm, alpha_ref, beta_ref,
           xo_ref, ho_ref,
           wqkv, wo, wup, wdown, win, wout, mod, xraw, xsend, hsend, hin, outb, xbt, xbt_out, xs, xfin_out, xfin,
           hres, unorm, qs, ks, vt, attn, act, s_scr, p_scr,
           w_sem, small_sem, init_send, init_recv, st_send, st_recv, x_send, x_recv, xf_send, xf_recv, ho_send, ho_recv, ready_sem, go_sem):
    y = lax.axis_index("seq")
    s = lax.axis_index("stage")
    z = lax.axis_index("data")
    oy = 1 - y
    is_first = s == 0
    is_last = s == STAGES - 1
    is_waiter = s == STAGES - 2
    uses_x = jnp.logical_or(is_first, is_last)
    h_idx = jnp.maximum(s - 1, 0)

    def local(src, dst, sem):
        return pltpu.make_async_copy(src, dst, sem)

    def remote(src, dst, ssem, rsem, yy, ss):
        return pltpu.make_async_remote_copy(src_ref=src, dst_ref=dst, send_sem=ssem, recv_sem=rsem,
                                            device_id=(z, yy, ss), device_id_type=MESH)

    cp_h = local(h_hbm.at[h_idx, y], hin.at[0, 1], small_sem.at[0])
    cp_x = local(x_hbm.at[y], xraw.at[1], small_sem.at[1])
    cp_mod = local(mod_hbm, mod, small_sem.at[2])
    cp_win = local(win_hbm, win, small_sem.at[3])
    cp_wout = local(wout_hbm, wout, small_sem.at[4])
    cp_wqkv = [local(wqkv_hbm.at[:, pl.ds(j * DIM, DIM)], wqkv.at[j], w_sem.at[j]) for j in range(3)]
    cp_rest = [local(wo_hbm, wo, w_sem.at[3])]
    cp_rest += [local(wup_hbm.at[:, pl.ds(j * DIM, DIM)], wup.at[j], w_sem.at[4 + j]) for j in range(4)]
    cp_rest += [local(wdown_hbm, wdown, w_sem.at[8])]
    cp_hs = local(h_hbm.at[h_idx, oy], hsend, small_sem.at[5])
    cp_xs = local(x_hbm.at[oy], xsend, small_sem.at[6])
    rc_ha = remote(hsend.at[pl.ds(0, 16)], hin.at[0, 0, pl.ds(0, 16)], init_send.at[0], init_recv.at[0], oy, s)
    rc_hb = remote(hsend.at[pl.ds(16, ROWS - 16)], hin.at[0, 0, pl.ds(16, ROWS - 16)], init_send.at[2], init_recv.at[2], oy, s)
    rc_x = remote(xsend, xraw.at[0], init_send.at[1], init_recv.at[1], oy, s)

    @pl.when(jnp.logical_not(is_first))
    def _():
        cp_hs.start()
        cp_h.start()

    cp_xs.start()
    cp_x.start()
    cp_mod.start()
    cp_win.start()
    cp_wout.start()
    for j in (1, 2, 0):
        cp_wqkv[j].start()

    barrier = pltpu.get_barrier_semaphore()

    def enter_signal(yy, ss):
        pl.semaphore_signal(barrier, inc=1, device_id=(z, yy, ss), device_id_type=MESH)

    is_second = s == 1
    enter_signal(oy, s)

    @pl.when(is_first)
    def _():
        enter_signal(y, STAGES - 1)

    @pl.when(is_second)
    def _():
        enter_signal(y, 0)
        enter_signal(y, 2)

    @pl.when(is_waiter)
    def _():
        enter_signal(y, STAGES - 1)

    @pl.when(is_last)
    def _():
        enter_signal(y, STAGES - 2)

    cp_xs.wait()

    @pl.when(jnp.logical_not(is_first))
    def _():
        cp_hs.wait()

    @pl.when(is_first)
    def _():
        pl.semaphore_wait(barrier, 2)

    @pl.when(is_second)
    def _():
        pl.semaphore_wait(barrier, 1)

    @pl.when(is_waiter)
    def _():
        pl.semaphore_wait(barrier, 3)
        pl.semaphore_signal(ready_sem, inc=1, device_id=(z, y, 1), device_id_type=MESH)

    @pl.when(is_last)
    def _():
        pl.semaphore_wait(barrier, 3)


    @pl.when(uses_x)
    def _():
        rc_x.start()

    @pl.when(jnp.logical_or(is_second, is_waiter))
    def _():
        rc_ha.start()
        rc_hb.start()

    for cp in cp_rest:
        cp.start()

    @pl.when(is_waiter)
    def _():
        rc_ha.wait_send()
        pl.semaphore_signal(go_sem, inc=1, device_id=(z, y, STAGES - 1), device_id_type=MESH)

    @pl.when(is_last)
    def _():
        pl.semaphore_wait(go_sem, 1)
        rc_ha.start()
        rc_hb.start()

    cp_x.wait()
    cp_mod.wait()
    cp_win.wait()
    cp_wout.wait()

    @pl.when(jnp.logical_not(is_first))
    def _():
        cp_h.wait()

    @pl.when(uses_x)
    def _():
        xs[1] = xraw[1]
        xbt[0, 1] = xraw[1].astype(BF16)

    for cp in cp_wqkv:
        cp.wait()

    def stage_copy(k, c):
        return remote(outb.at[k, c], hin.at[k + 1, c], st_send.at[k, c], st_recv.at[k, c], y, s + 1)

    def x_copy(k, c):
        return remote(xbt_out.at[k, c], xbt.at[k + 1, c], x_send.at[k, c], x_recv.at[k, c], y, 0)

    lane = lax.broadcasted_iota(jnp.int32, (ROWS, 128), 1)
    PAIRS = HEADS // 2
    LNB = 32

    def embed(k, c):
        @pl.when(is_first)
        def _():
            xb = xbt[k, c].astype(F32).T.astype(BF16)
            hin[k, c] = mm(xb, win[...]).astype(BF16)

    def ln1_pieces(k, c):
        def piece(r):
            def run():
                rows = pl.ds(r, LNB)
                h0 = hin[k, c, rows].astype(F32)
                unorm[c, rows] = (layer_norm(h0) * (1.0 + mod[k, 1]) + mod[k, 0]).astype(BF16)
            return run
        return [piece(r) for r in range(0, ROWS, LNB)]

    def q_pieces(c):
        def piece(n):
            def run():
                val = mm(unorm[c], wqkv[0, :, n:n + 256])
                for p in range(2):
                    part = val[:, p * 128:(p + 1) * 128]
                    qs[c, n // 128 + p, :ROWS] = jnp.where(lane < HD, part, 0.0).astype(BF16)
                    qs[c, n // 128 + p, ROWS:] = jnp.where(lane < HD, 0.0, part).astype(BF16)
            return run
        return [piece(n) for n in range(0, DIM, 256)]

    def k_pieces(c):
        def piece(n):
            def run():
                ks[c, :, n:n + 256] = mm(unorm[c], wqkv[1, :, n:n + 256]).astype(BF16)
            return run
        return [piece(n) for n in range(0, DIM, 256)]

    def v_pieces(c):
        def piece(n):
            def run():
                val = mm(unorm[c], wqkv[2, :, n:n + 256])
                vt[c, n:n + 256, :] = val.T.astype(BF16)
            return run
        return [piece(n) for n in range(0, DIM, 256)]

    def attn_units(c):
        mxs, invs = {}, {}

        def scores(p):
            cols = slice(p * 128, (p + 1) * 128)
            k2 = jnp.concatenate([ks[0, :, cols], ks[1, :, cols]], axis=0)
            st = lax.dot_general(k2, qs[c, p], (((1,), (1,)), ((), ())), preferred_element_type=F32)
            s_scr[c, p] = st
            mxs[p] = jnp.max(st, axis=0, keepdims=True)

        def exps(p, half):
            cols = slice(half * ROWS, (half + 1) * ROWS)
            ex = jnp.exp2((s_scr[c, p, :, cols] - mxs[p][:, cols]) * EXP2_SCALE)
            inv = 1.0 / jnp.sum(ex, axis=0, keepdims=True)
            p_scr[c, p, :, cols] = (ex * inv).astype(BF16)

        def values(p):
            cols = slice(p * 128, (p + 1) * 128)
            v2 = jnp.concatenate([vt[0, cols, :], vt[1, cols, :]], axis=1)
            ot = mm(v2, p_scr[c, p])
            o2 = jnp.concatenate([ot[:HD, :ROWS], ot[HD:, ROWS:]], axis=0)
            attn[c, :, cols] = o2.T.astype(BF16)

        sc = [functools.partial(scores, p) for p in range(PAIRS)]
        ev = []
        for p in range(PAIRS):
            ev.append(functools.partial(exps, p, 0))
            ev.append(functools.partial(exps, p, 1))
            if p:
                ev.append(functools.partial(values, p - 1))
        ev.append(functools.partial(values, PAIRS - 1))
        return sc, ev

    def wo_pieces(c):
        def piece(n):
            def run():
                hres[c, :, n:n + 256] = mm(attn[c], wo[:, n:n + 256])
            return run
        return [piece(n) for n in range(0, DIM, 256)]

    def ln2_pieces(k, c):
        def piece(r):
            def run():
                rows = pl.ds(r, LNB)
                h1 = hin[k, c, rows].astype(F32) + mod[k, 2] * hres[c, rows]
                hres[c, rows] = h1
                unorm[c, rows] = (layer_norm(h1) * (1.0 + mod[k, 4]) + mod[k, 3]).astype(BF16)
            return run
        return [piece(r) for r in range(0, ROWS, LNB)]

    def up_pieces(c):
        def piece(n):
            def run():
                j, m = divmod(n, DIM)
                act[c, :, n:n + 256] = gelu(mm(unorm[c], wup[j, :, m:m + 256])).astype(BF16)
            return run
        return [piece(n) for n in range(0, FF, 256)]

    def down_pieces(k, c):
        def store(n, res):
            out = hres[c, :, n:n + 256] + mod[k, 5][:, n:n + 256] * res
            outb[k, c, :, n:n + 256] = out.astype(BF16)

        def full(n):
            def run():
                store(n, mm(act[c], wdown[:, n:n + 256]))
            return run

        def halves(n):
            def run():
                lo = mm(act[c, :, :FF // 2], wdown[:FF // 2, n:n + 256])
                hi = mm(act[c, :, FF // 2:], wdown[FF // 2:, n:n + 256])
                store(n, lo + hi)
            return run
        return [full(0), full(256), halves(512)]

    def finish(k, c):
        last = isinstance(k, int) and k == STEPS - 1
        if last:
            if c == 0:
                remote(outb.at[k, c], ho_ref.at[y], ho_send, ho_recv, oy, s).start()
            else:
                ho_ref[y] = outb[k, c]
        else:
            @pl.when(jnp.logical_not(is_last))
            def _():
                stage_copy(k, c).start()

        @pl.when(is_last)
        def _():
            eps = lax.dot_general(wout[...], outb[k, c], (((1,), (1,)), ((), ())), preferred_element_type=F32)
            xn = alpha_ref[k] * xs[c] + beta_ref[k] * eps
            if not last:
                xs[c] = xn
                xbt_out[k, c] = xn.astype(BF16)
                x_copy(k, c).start()
            else:
                xfin_out[c] = xn
                if c == 0:
                    for t in range(STAGES):
                        remote(xfin_out.at[c], xfin.at[y], xf_send.at[t], xf_recv.at[y], oy, t).start()
                else:
                    for t in range(STAGES - 1):
                        remote(xfin_out.at[c], xfin.at[y], xf_send.at[STAGES + t], xf_recv.at[y], y, t).start()
                    xfin[y] = xn

    def chunk_input(k, c):
        @pl.when(jnp.logical_not(is_first))
        def _():
            stage_copy(k - 1, c).wait_recv()

        @pl.when(is_first)
        def _():
            x_copy(k - 1, c).wait_recv()

        embed(k, c)

    def block(k, head, waits):
        sc0, ev0 = attn_units(0)
        sc1, ev1 = attn_units(1)
        waits[0]()
        interleave(sc0[:2])
        interleave(head + sc0[2:] + sc1, ev0)
        waits[1]()
        interleave(wo_pieces(0), ev1[:3])
        interleave(ln2_pieces(k, 0), ev1[3:5])
        waits[2]()
        interleave(up_pieces(0), ev1[5:10])
        waits[3]()
        down0 = down_pieces(k, 0)
        interleave(down0[:2], ev1[10:] + wo_pieces(1))
        interleave(down0[2:], ln2_pieces(k, 1))
        finish(k, 0)
        interleave(up_pieces(1))
        interleave(down_pieces(k, 1))
        finish(k, 1)

    def last_block(k, head):
        sc0, ev0 = attn_units(0)
        interleave(sc0[:2])
        interleave([sc0[2], head[0], sc0[3], head[1], sc0[4], head[2], sc0[5]], ev0[:4])
        interleave(ev0[4:])
        interleave(wo_pieces(0))
        interleave(ln2_pieces(k, 0))
        interleave(up_pieces(0))
        interleave(down_pieces(k, 0))
        finish(k, 0)
        sc1, ev1 = attn_units(1)
        interleave(sc1[:2])
        interleave(sc1[2:], ev1[:4])
        interleave(ev1[4:])
        interleave(wo_pieces(1))
        interleave(ln2_pieces(k, 1))
        interleave(up_pieces(1))
        interleave(down_pieces(k, 1))
        finish(k, 1)

    embed(0, 1)
    interleave(ln1_pieces(0, 1))
    interleave(k_pieces(1) + v_pieces(1) + q_pieces(1))

    @pl.when(jnp.logical_not(is_first))
    def _():
        rc_ha.wait_recv()
        rc_hb.wait_recv()

    @pl.when(uses_x)
    def _():
        rc_x.wait_recv()
        xs[0] = xraw[0]
        xbt[0, 0] = xraw[0].astype(BF16)

    @pl.when(is_second)
    def _():
        pl.semaphore_wait(ready_sem, 1)

    embed(0, 0)
    interleave(ln1_pieces(0, 0))
    interleave(k_pieces(0) + q_pieces(0))
    block(0, v_pieces(0), [lambda: None, cp_rest[0].wait, lambda: [cp.wait() for cp in cp_rest[1:5]], cp_rest[5].wait])

    def enter(k):
        chunk_input(k, 0)
        interleave(ln1_pieces(k, 0))
        interleave(k_pieces(0) + v_pieces(0))
        chunk_input(k, 1)
        interleave(q_pieces(0), ln1_pieces(k, 1))
        interleave(k_pieces(1))
        interleave(q_pieces(1))

    def step(k, _):
        enter(k)
        block(k, v_pieces(1), [lambda: None] * 4)
        return 0

    lax.fori_loop(1, STEPS - 1, step, 0)
    enter(STEPS - 1)
    last_block(STEPS - 1, v_pieces(1))

    remote(xfin_out.at[0], xfin.at[oy], xf_send.at[0], xf_recv.at[oy], oy, s).wait_recv()

    @pl.when(jnp.logical_not(is_last))
    def _():
        remote(xfin_out.at[0], xfin.at[y], xf_send.at[0], xf_recv.at[y], y, s).wait_recv()

    for b in range(2):
        xo_ref[b] = xfin[b]

    @pl.when(is_last)
    def _():
        for t in range(STAGES):
            remote(xfin_out.at[0], xfin.at[y], xf_send.at[t], xf_recv.at[y], oy, t).wait_send()
        for t in range(STAGES - 1):
            remote(xfin_out.at[1], xfin.at[y], xf_send.at[STAGES + t], xf_recv.at[y], y, t).wait_send()
        for k in range(STEPS - 1):
            for c in range(2):
                x_copy(k, c).wait_send()

    @pl.when(jnp.logical_not(is_last))
    def _():
        for k in range(STEPS - 1):
            for c in range(2):
                stage_copy(k, c).wait_send()

    @pl.when(jnp.logical_not(jnp.logical_or(is_first, is_waiter)))
    def _():
        rc_ha.wait_send()

    @pl.when(jnp.logical_not(is_first))
    def _():
        rc_hb.wait_send()

    @pl.when(uses_x)
    def _():
        rc_x.wait_send()

    last = remote(outb.at[STEPS - 1, 0], ho_ref.at[oy], ho_send, ho_recv, oy, s)
    last.wait_send()
    last.wait_recv()


def writer(x_ref, h_ref, xo_ref, ho_ref, sems):
    copies = [pltpu.make_async_copy(x_ref, xo_ref, sems.at[0]), pltpu.make_async_copy(h_ref, ho_ref, sems.at[1])]
    for copy in copies:
        copy.start()
    for copy in copies:
        copy.wait()


def solution(mesh):
    hbm = pl.BlockSpec(memory_space=pltpu.HBM)
    smem = pl.BlockSpec(memory_space=pltpu.SMEM)
    vmem = pl.BlockSpec(memory_space=pltpu.VMEM)
    dma = pltpu.SemaphoreType.DMA
    scratch = [
        pltpu.VMEM((3, DIM, DIM), BF16),
        pltpu.VMEM((DIM, DIM), BF16),
        pltpu.VMEM((4, DIM, DIM), BF16),
        pltpu.VMEM((FF, DIM), BF16),
        pltpu.VMEM((LAT, DIM), BF16),
        pltpu.VMEM((LAT, DIM), BF16),
        pltpu.VMEM((STEPS, 6, 1, DIM), F32),
        pltpu.VMEM((2, LAT, ROWS), F32),
        pltpu.VMEM((LAT, ROWS), F32),
        pltpu.VMEM((ROWS, DIM), BF16),
        pltpu.VMEM((STEPS, 2, ROWS, DIM), BF16),
        pltpu.VMEM((STEPS, 2, ROWS, DIM), BF16),
        pltpu.VMEM((STEPS, 2, LAT, ROWS), BF16),
        pltpu.VMEM((STEPS, 2, LAT, ROWS), BF16),
        pltpu.VMEM((2, LAT, ROWS), F32),
        pltpu.VMEM((2, LAT, ROWS), F32),
        pltpu.VMEM((2, LAT, ROWS), F32),
        pltpu.VMEM((2, ROWS, DIM), F32),
        pltpu.VMEM((2, ROWS, DIM), BF16),
        pltpu.VMEM((2, HEADS // 2, 2 * ROWS, 128), BF16),
        pltpu.VMEM((2, ROWS, DIM), BF16),
        pltpu.VMEM((2, DIM, ROWS), BF16),
        pltpu.VMEM((2, ROWS, DIM), BF16),
        pltpu.VMEM((2, ROWS, FF), BF16),
        pltpu.VMEM((2, HEADS // 2, 2 * ROWS, 2 * ROWS), F32),
        pltpu.VMEM((2, HEADS // 2, 2 * ROWS, 2 * ROWS), BF16),
        dma((9,)), dma((7,)), dma((3,)), dma((3,)),
        dma((STEPS - 1, 2)), dma((STEPS - 1, 2)), dma((STEPS - 1, 2)), dma((STEPS - 1, 2)),
        dma((2 * STAGES - 1,)), dma((2,)), dma, dma, pltpu.SemaphoreType.REGULAR, pltpu.SemaphoreType.REGULAR,
    ]

    def device_fn(x_init, h_init, w_in, w_out, w_qkv, w_o, w_up, w_down, ada_mod, alpha_coef, beta_coef):
        call = pl.pallas_call(
            kernel,
            name="dit_steps",
            out_shape=(pltpu.VMEM((2, LAT, ROWS), F32), pltpu.VMEM((2, ROWS, DIM), BF16)),
            in_specs=[hbm] * 9 + [smem] * 2,
            out_specs=(vmem, vmem),
            scratch_shapes=scratch,
            compiler_params=pltpu.CompilerParams(collective_id=0, has_side_effects=True, vmem_limit_bytes=58 * 1024 * 1024),
        )
        x_final, h_final = call(x_init.swapaxes(1, 2), h_init, w_in, w_out.T, w_qkv.reshape(DIM, 3 * DIM), w_o.reshape(DIM, DIM),
                                w_up.reshape(DIM, FF), w_down.reshape(FF, DIM), ada_mod.swapaxes(1, 2), alpha_coef, beta_coef)
        x_final, h_final = pl.pallas_call(
            writer,
            name="write_out",
            out_shape=(jax.ShapeDtypeStruct(x_final.shape, F32), jax.ShapeDtypeStruct(h_final.shape, BF16)),
            in_specs=[vmem] * 2,
            out_specs=(hbm, hbm),
            scratch_shapes=[dma((2,))],
        )(pltpu.with_memory_space_constraint(x_final, pltpu.VMEM), pltpu.with_memory_space_constraint(h_final, pltpu.VMEM))
        return x_final.swapaxes(1, 2), h_final[None]

    weight_spec = P("stage", None, None)
    return jax.shard_map(
        device_fn,
        mesh=mesh,
        in_specs=(P("data", "seq", None), P(None, "data", "seq", None), P(), P(), weight_spec, P("stage", None, None, None), weight_spec, weight_spec, P(None, "stage", None, None), P(), P()),
        out_specs=(P("data", "seq", None), P("stage", "data", "seq", None)),
        check_vma=False,
    )
```

```python
import functools

import jax
import jax.numpy as jnp
from jax import lax
from jax.experimental import pallas as pl
from jax.experimental.pallas import tpu as pltpu
from jax.sharding import PartitionSpec as P

LN_EPS = 1e-6
MESH = pl.DeviceIdType.MESH
BF16 = jnp.bfloat16
F32 = jnp.float32

STEPS = 4
STAGES = 4
DIM = 768
FF = 3072
HEADS = 12
HD = 64
ROWS = 128
LAT = 48
EXP2_SCALE = HD ** -0.5 * 1.4426950408889634
GELU_C0 = 0.7978845608028654
GELU_C1 = GELU_C0 * 0.044715


def layer_norm(hidden):
    mean_val = jnp.mean(hidden, axis=-1, keepdims=True)
    centered = hidden - mean_val
    variance = jnp.mean(centered * centered, axis=-1, keepdims=True)
    return centered * lax.rsqrt(variance + LN_EPS)


def gelu(val):
    half = 0.5 * val
    return half + half * jnp.tanh(val * (GELU_C0 + GELU_C1 * (val * val)))


def mm(lhs, rhs):
    return jnp.dot(lhs, rhs, preferred_element_type=F32)


def interleave(*streams):
    order = []
    for idx, pieces in enumerate(streams):
        for pos in range(len(pieces)):
            order.append(((pos + 0.5) / len(pieces), idx, pos))
    for _, idx, pos in sorted(order):
        streams[idx][pos]()


def kernel(x_hbm, h_hbm, win_hbm, wout_hbm, wqkv_hbm, wo_hbm, wup_hbm, wdown_hbm, mod_hbm, alpha_ref, beta_ref,
           xo_ref, ho_ref,
           wqkv, wo, wup, wdown, win, wout, mod, xraw, xsend, hsend, hin, outb, xbt, xbt_out, xs, xfin_out, xfin,
           hres, unorm, qs, ks, vt, attn, act, s_scr, p_scr,
           w_sem, small_sem, init_send, init_recv, st_send, st_recv, x_send, x_recv, xf_send, xf_recv, ho_send, ho_recv, ready_sem):
    y = lax.axis_index("seq")
    s = lax.axis_index("stage")
    z = lax.axis_index("data")
    oy = 1 - y
    is_first = s == 0
    is_last = s == STAGES - 1
    is_waiter = s == STAGES - 2
    uses_x = jnp.logical_or(is_first, is_last)
    h_idx = jnp.maximum(s - 1, 0)

    def local(src, dst, sem):
        return pltpu.make_async_copy(src, dst, sem)

    def remote(src, dst, ssem, rsem, yy, ss):
        return pltpu.make_async_remote_copy(src_ref=src, dst_ref=dst, send_sem=ssem, recv_sem=rsem,
                                            device_id=(z, yy, ss), device_id_type=MESH)

    cp_h = local(h_hbm.at[h_idx, y], hin.at[0, 1], small_sem.at[0])
    cp_x = local(x_hbm.at[y], xraw.at[1], small_sem.at[1])
    cp_mod = local(mod_hbm, mod, small_sem.at[2])
    cp_win = local(win_hbm, win, small_sem.at[3])
    cp_wout = local(wout_hbm, wout, small_sem.at[4])
    cp_wqkv = [local(wqkv_hbm.at[:, pl.ds(j * DIM, DIM)], wqkv.at[j], w_sem.at[j]) for j in range(3)]
    cp_rest = [local(wo_hbm, wo, w_sem.at[3])]
    cp_rest += [local(wup_hbm.at[:, pl.ds(j * DIM, DIM)], wup.at[j], w_sem.at[4 + j]) for j in range(4)]
    cp_rest += [local(wdown_hbm, wdown, w_sem.at[8])]
    cp_hs = local(h_hbm.at[h_idx, oy], hsend, small_sem.at[5])
    cp_xs = local(x_hbm.at[oy], xsend, small_sem.at[6])
    rc_h = remote(hsend, hin.at[0, 0], init_send.at[0], init_recv.at[0], oy, s)
    rc_x = remote(xsend, xraw.at[0], init_send.at[1], init_recv.at[1], oy, s)

    @pl.when(jnp.logical_not(is_first))
    def _():
        cp_hs.start()
        cp_h.start()

    cp_xs.start()
    cp_x.start()
    cp_mod.start()
    cp_win.start()
    cp_wout.start()
    for j in (1, 2, 0):
        cp_wqkv[j].start()

    barrier = pltpu.get_barrier_semaphore()

    def enter_signal(yy, ss):
        pl.semaphore_signal(barrier, inc=1, device_id=(z, yy, ss), device_id_type=MESH)

    is_second = s == 1
    enter_signal(oy, s)

    @pl.when(is_first)
    def _():
        enter_signal(y, STAGES - 1)

    @pl.when(is_second)
    def _():
        enter_signal(y, 0)
        enter_signal(y, 2)

    @pl.when(is_waiter)
    def _():
        enter_signal(y, STAGES - 1)

    @pl.when(is_last)
    def _():
        enter_signal(y, STAGES - 2)

    cp_xs.wait()

    @pl.when(jnp.logical_not(is_first))
    def _():
        cp_hs.wait()

    @pl.when(is_first)
    def _():
        pl.semaphore_wait(barrier, 2)

    @pl.when(is_second)
    def _():
        pl.semaphore_wait(barrier, 1)

    @pl.when(is_waiter)
    def _():
        pl.semaphore_wait(barrier, 3)
        pl.semaphore_signal(ready_sem, inc=1, device_id=(z, y, 1), device_id_type=MESH)

    @pl.when(is_last)
    def _():
        pl.semaphore_wait(barrier, 3)


    @pl.when(uses_x)
    def _():
        rc_x.start()

    @pl.when(jnp.logical_not(is_first))
    def _():
        rc_h.start()

    for cp in cp_rest:
        cp.start()

    cp_x.wait()
    cp_mod.wait()
    cp_win.wait()
    cp_wout.wait()

    @pl.when(jnp.logical_not(is_first))
    def _():
        cp_h.wait()

    @pl.when(uses_x)
    def _():
        xs[1] = xraw[1]
        xbt[0, 1] = xraw[1].astype(BF16)

    for cp in cp_wqkv:
        cp.wait()

    def stage_copy(k, c):
        return remote(outb.at[k, c], hin.at[k + 1, c], st_send.at[k, c], st_recv.at[k, c], y, s + 1)

    def x_copy(k, c):
        return remote(xbt_out.at[k, c], xbt.at[k + 1, c], x_send.at[k, c], x_recv.at[k, c], y, 0)

    lane = lax.broadcasted_iota(jnp.int32, (ROWS, 128), 1)
    PAIRS = HEADS // 2
    LNB = 32

    def embed(k, c):
        @pl.when(is_first)
        def _():
            xb = xbt[k, c].astype(F32).T.astype(BF16)
            hin[k, c] = mm(xb, win[...]).astype(BF16)

    def ln1_pieces(k, c):
        def piece(r):
            def run():
                rows = pl.ds(r, LNB)
                h0 = hin[k, c, rows].astype(F32)
                unorm[c, rows] = (layer_norm(h0) * (1.0 + mod[k, 1]) + mod[k, 0]).astype(BF16)
            return run
        return [piece(r) for r in range(0, ROWS, LNB)]

    def q_pieces(c):
        def piece(n):
            def run():
                val = mm(unorm[c], wqkv[0, :, n:n + 256])
                for p in range(2):
                    part = val[:, p * 128:(p + 1) * 128]
                    qs[c, n // 128 + p, :ROWS] = jnp.where(lane < HD, part, 0.0).astype(BF16)
                    qs[c, n // 128 + p, ROWS:] = jnp.where(lane < HD, 0.0, part).astype(BF16)
            return run
        return [piece(n) for n in range(0, DIM, 256)]

    def k_pieces(c):
        def piece(n):
            def run():
                ks[c, :, n:n + 256] = mm(unorm[c], wqkv[1, :, n:n + 256]).astype(BF16)
            return run
        return [piece(n) for n in range(0, DIM, 256)]

    def v_pieces(c):
        def piece(n):
            def run():
                val = mm(unorm[c], wqkv[2, :, n:n + 256])
                vt[c, n:n + 256, :] = val.T.astype(BF16)
            return run
        return [piece(n) for n in range(0, DIM, 256)]

    def attn_units(c):
        mxs, invs = {}, {}

        def scores(p):
            cols = slice(p * 128, (p + 1) * 128)
            k2 = jnp.concatenate([ks[0, :, cols], ks[1, :, cols]], axis=0)
            st = lax.dot_general(k2, qs[c, p], (((1,), (1,)), ((), ())), preferred_element_type=F32)
            s_scr[c, p] = st
            mxs[p] = jnp.max(st, axis=0, keepdims=True)

        def exps(p, half):
            cols = slice(half * ROWS, (half + 1) * ROWS)
            ex = jnp.exp2((s_scr[c, p, :, cols] - mxs[p][:, cols]) * EXP2_SCALE)
            inv = 1.0 / jnp.sum(ex, axis=0, keepdims=True)
            p_scr[c, p, :, cols] = (ex * inv).astype(BF16)

        def values(p):
            cols = slice(p * 128, (p + 1) * 128)
            v2 = jnp.concatenate([vt[0, cols, :], vt[1, cols, :]], axis=1)
            ot = mm(v2, p_scr[c, p])
            o2 = jnp.concatenate([ot[:HD, :ROWS], ot[HD:, ROWS:]], axis=0)
            attn[c, :, cols] = o2.T.astype(BF16)

        sc = [functools.partial(scores, p) for p in range(PAIRS)]
        ev = []
        for p in range(PAIRS):
            ev.append(functools.partial(exps, p, 0))
            ev.append(functools.partial(exps, p, 1))
            if p:
                ev.append(functools.partial(values, p - 1))
        ev.append(functools.partial(values, PAIRS - 1))
        return sc, ev

    def wo_pieces(c):
        def piece(n):
            def run():
                hres[c, :, n:n + 256] = mm(attn[c], wo[:, n:n + 256])
            return run
        return [piece(n) for n in range(0, DIM, 256)]

    def ln2_pieces(k, c):
        def piece(r):
            def run():
                rows = pl.ds(r, LNB)
                h1 = hin[k, c, rows].astype(F32) + mod[k, 2] * hres[c, rows]
                hres[c, rows] = h1
                unorm[c, rows] = (layer_norm(h1) * (1.0 + mod[k, 4]) + mod[k, 3]).astype(BF16)
            return run
        return [piece(r) for r in range(0, ROWS, LNB)]

    def up_pieces(c):
        def piece(n):
            def run():
                j, m = divmod(n, DIM)
                act[c, :, n:n + 256] = gelu(mm(unorm[c], wup[j, :, m:m + 256])).astype(BF16)
            return run
        return [piece(n) for n in range(0, FF, 256)]

    def down_pieces(k, c):
        def store(n, res):
            out = hres[c, :, n:n + 256] + mod[k, 5][:, n:n + 256] * res
            outb[k, c, :, n:n + 256] = out.astype(BF16)

        def full(n):
            def run():
                store(n, mm(act[c], wdown[:, n:n + 256]))
            return run

        def halves(n):
            def run():
                lo = mm(act[c, :, :FF // 2], wdown[:FF // 2, n:n + 256])
                hi = mm(act[c, :, FF // 2:], wdown[FF // 2:, n:n + 256])
                store(n, lo + hi)
            return run
        return [full(0), full(256), halves(512)]

    def finish(k, c):
        last = isinstance(k, int) and k == STEPS - 1
        if last:
            if c == 0:
                remote(outb.at[k, c], ho_ref.at[y], ho_send, ho_recv, oy, s).start()
            else:
                ho_ref[y] = outb[k, c]
        else:
            @pl.when(jnp.logical_not(is_last))
            def _():
                stage_copy(k, c).start()

        @pl.when(is_last)
        def _():
            eps = lax.dot_general(wout[...], outb[k, c], (((1,), (1,)), ((), ())), preferred_element_type=F32)
            xn = alpha_ref[k] * xs[c] + beta_ref[k] * eps
            if not last:
                xs[c] = xn
                xbt_out[k, c] = xn.astype(BF16)
                x_copy(k, c).start()
            else:
                xfin_out[c] = xn
                if c == 0:
                    for t in range(STAGES):
                        remote(xfin_out.at[c], xfin.at[y], xf_send.at[t], xf_recv.at[y], oy, t).start()
                else:
                    for t in range(STAGES - 1):
                        remote(xfin_out.at[c], xfin.at[y], xf_send.at[STAGES + t], xf_recv.at[y], y, t).start()
                    xfin[y] = xn

    def chunk_input(k, c):
        @pl.when(jnp.logical_not(is_first))
        def _():
            stage_copy(k - 1, c).wait_recv()

        @pl.when(is_first)
        def _():
            x_copy(k - 1, c).wait_recv()

        embed(k, c)

    def block(k, head, waits):
        sc0, ev0 = attn_units(0)
        sc1, ev1 = attn_units(1)
        waits[0]()
        interleave(sc0[:2])
        interleave(head + sc0[2:] + sc1, ev0)
        waits[1]()
        interleave(wo_pieces(0), ev1[:3])
        interleave(ln2_pieces(k, 0), ev1[3:5])
        waits[2]()
        interleave(up_pieces(0), ev1[5:10])
        waits[3]()
        down0 = down_pieces(k, 0)
        interleave(down0[:2], ev1[10:] + wo_pieces(1))
        interleave(down0[2:], ln2_pieces(k, 1))
        finish(k, 0)
        interleave(up_pieces(1))
        interleave(down_pieces(k, 1))
        finish(k, 1)

    def last_block(k, head):
        sc0, ev0 = attn_units(0)
        interleave(sc0[:2])
        interleave([sc0[2], head[0], sc0[3], head[1], sc0[4], head[2], sc0[5]], ev0[:4])
        interleave(ev0[4:])
        interleave(wo_pieces(0))
        interleave(ln2_pieces(k, 0))
        interleave(up_pieces(0))
        interleave(down_pieces(k, 0))
        finish(k, 0)
        sc1, ev1 = attn_units(1)
        interleave(sc1[:2])
        interleave(sc1[2:], ev1[:4])
        interleave(ev1[4:])
        interleave(wo_pieces(1))
        interleave(ln2_pieces(k, 1))
        interleave(up_pieces(1))
        interleave(down_pieces(k, 1))
        finish(k, 1)

    embed(0, 1)
    interleave(ln1_pieces(0, 1))
    interleave(k_pieces(1) + v_pieces(1) + q_pieces(1))

    @pl.when(jnp.logical_not(is_first))
    def _():
        rc_h.wait_recv()

    @pl.when(uses_x)
    def _():
        rc_x.wait_recv()
        xs[0] = xraw[0]
        xbt[0, 0] = xraw[0].astype(BF16)

    @pl.when(is_second)
    def _():
        pl.semaphore_wait(ready_sem, 1)

    for cp in cp_rest:
        cp.wait()

    embed(0, 0)
    interleave(ln1_pieces(0, 0))
    interleave(k_pieces(0) + q_pieces(0))
    block(0, v_pieces(0), [lambda: None] * 4)

    def enter(k):
        chunk_input(k, 0)
        interleave(ln1_pieces(k, 0))
        interleave(k_pieces(0) + v_pieces(0))
        chunk_input(k, 1)
        interleave(q_pieces(0), ln1_pieces(k, 1))
        interleave(k_pieces(1))
        interleave(q_pieces(1))

    def step(k, _):
        enter(k)
        block(k, v_pieces(1), [lambda: None] * 4)
        return 0

    lax.fori_loop(1, STEPS - 1, step, 0)
    enter(STEPS - 1)
    last_block(STEPS - 1, v_pieces(1))

    remote(xfin_out.at[0], xfin.at[oy], xf_send.at[0], xf_recv.at[oy], oy, s).wait_recv()

    @pl.when(jnp.logical_not(is_last))
    def _():
        remote(xfin_out.at[0], xfin.at[y], xf_send.at[0], xf_recv.at[y], y, s).wait_recv()

    for b in range(2):
        xo_ref[b] = xfin[b]

    @pl.when(is_last)
    def _():
        for t in range(STAGES):
            remote(xfin_out.at[0], xfin.at[y], xf_send.at[t], xf_recv.at[y], oy, t).wait_send()
        for t in range(STAGES - 1):
            remote(xfin_out.at[1], xfin.at[y], xf_send.at[STAGES + t], xf_recv.at[y], y, t).wait_send()
        for k in range(STEPS - 1):
            for c in range(2):
                x_copy(k, c).wait_send()

    @pl.when(jnp.logical_not(is_last))
    def _():
        for k in range(STEPS - 1):
            for c in range(2):
                stage_copy(k, c).wait_send()

    @pl.when(jnp.logical_not(is_first))
    def _():
        rc_h.wait_send()

    @pl.when(uses_x)
    def _():
        rc_x.wait_send()

    last = remote(outb.at[STEPS - 1, 0], ho_ref.at[oy], ho_send, ho_recv, oy, s)
    last.wait_send()
    last.wait_recv()


def writer(x_ref, h_ref, xo_ref, ho_ref, sems):
    copies = [pltpu.make_async_copy(x_ref, xo_ref, sems.at[0]), pltpu.make_async_copy(h_ref, ho_ref, sems.at[1])]
    for copy in copies:
        copy.start()
    for copy in copies:
        copy.wait()


def solution(mesh):
    hbm = pl.BlockSpec(memory_space=pltpu.HBM)
    smem = pl.BlockSpec(memory_space=pltpu.SMEM)
    vmem = pl.BlockSpec(memory_space=pltpu.VMEM)
    dma = pltpu.SemaphoreType.DMA
    scratch = [
        pltpu.VMEM((3, DIM, DIM), BF16),
        pltpu.VMEM((DIM, DIM), BF16),
        pltpu.VMEM((4, DIM, DIM), BF16),
        pltpu.VMEM((FF, DIM), BF16),
        pltpu.VMEM((LAT, DIM), BF16),
        pltpu.VMEM((LAT, DIM), BF16),
        pltpu.VMEM((STEPS, 6, 1, DIM), F32),
        pltpu.VMEM((2, LAT, ROWS), F32),
        pltpu.VMEM((LAT, ROWS), F32),
        pltpu.VMEM((ROWS, DIM), BF16),
        pltpu.VMEM((STEPS, 2, ROWS, DIM), BF16),
        pltpu.VMEM((STEPS, 2, ROWS, DIM), BF16),
        pltpu.VMEM((STEPS, 2, LAT, ROWS), BF16),
        pltpu.VMEM((STEPS, 2, LAT, ROWS), BF16),
        pltpu.VMEM((2, LAT, ROWS), F32),
        pltpu.VMEM((2, LAT, ROWS), F32),
        pltpu.VMEM((2, LAT, ROWS), F32),
        pltpu.VMEM((2, ROWS, DIM), F32),
        pltpu.VMEM((2, ROWS, DIM), BF16),
        pltpu.VMEM((2, HEADS // 2, 2 * ROWS, 128), BF16),
        pltpu.VMEM((2, ROWS, DIM), BF16),
        pltpu.VMEM((2, DIM, ROWS), BF16),
        pltpu.VMEM((2, ROWS, DIM), BF16),
        pltpu.VMEM((2, ROWS, FF), BF16),
        pltpu.VMEM((2, HEADS // 2, 2 * ROWS, 2 * ROWS), F32),
        pltpu.VMEM((2, HEADS // 2, 2 * ROWS, 2 * ROWS), BF16),
        dma((9,)), dma((7,)), dma((2,)), dma((2,)),
        dma((STEPS - 1, 2)), dma((STEPS - 1, 2)), dma((STEPS - 1, 2)), dma((STEPS - 1, 2)),
        dma((2 * STAGES - 1,)), dma((2,)), dma, dma, pltpu.SemaphoreType.REGULAR,
    ]

    def device_fn(x_init, h_init, w_in, w_out, w_qkv, w_o, w_up, w_down, ada_mod, alpha_coef, beta_coef):
        call = pl.pallas_call(
            kernel,
            name="dit_steps",
            out_shape=(pltpu.VMEM((2, LAT, ROWS), F32), pltpu.VMEM((2, ROWS, DIM), BF16)),
            in_specs=[hbm] * 9 + [smem] * 2,
            out_specs=(vmem, vmem),
            scratch_shapes=scratch,
            compiler_params=pltpu.CompilerParams(collective_id=0, has_side_effects=True, vmem_limit_bytes=58 * 1024 * 1024),
        )
        x_final, h_final = call(x_init.swapaxes(1, 2), h_init, w_in, w_out.T, w_qkv.reshape(DIM, 3 * DIM), w_o.reshape(DIM, DIM),
                                w_up.reshape(DIM, FF), w_down.reshape(FF, DIM), ada_mod.swapaxes(1, 2), alpha_coef, beta_coef)
        x_final, h_final = pl.pallas_call(
            writer,
            name="write_out",
            out_shape=(jax.ShapeDtypeStruct(x_final.shape, F32), jax.ShapeDtypeStruct(h_final.shape, BF16)),
            in_specs=[vmem] * 2,
            out_specs=(hbm, hbm),
            scratch_shapes=[dma((2,))],
        )(pltpu.with_memory_space_constraint(x_final, pltpu.VMEM), pltpu.with_memory_space_constraint(h_final, pltpu.VMEM))
        return x_final.swapaxes(1, 2), h_final[None]

    weight_spec = P("stage", None, None)
    return jax.shard_map(
        device_fn,
        mesh=mesh,
        in_specs=(P("data", "seq", None), P(None, "data", "seq", None), P(), P(), weight_spec, P("stage", None, None, None), weight_spec, weight_spec, P(None, "stage", None, None), P(), P()),
        out_specs=(P("data", "seq", None), P("stage", "data", "seq", None)),
        check_vma=False,
    )
```

```python
import functools

import jax
import jax.numpy as jnp
from jax import lax
from jax.experimental import pallas as pl
from jax.experimental.pallas import tpu as pltpu
from jax.sharding import PartitionSpec as P

LN_EPS = 1e-6
MESH = pl.DeviceIdType.MESH
BF16 = jnp.bfloat16
F32 = jnp.float32

STEPS = 4
STAGES = 4
DIM = 768
FF = 3072
HEADS = 12
HD = 64
ROWS = 128
LAT = 48
EXP2_SCALE = HD ** -0.5 * 1.4426950408889634
GELU_C0 = 0.7978845608028654
GELU_C1 = GELU_C0 * 0.044715


def layer_norm(hidden):
    mean_val = jnp.mean(hidden, axis=-1, keepdims=True)
    centered = hidden - mean_val
    variance = jnp.mean(centered * centered, axis=-1, keepdims=True)
    return centered * lax.rsqrt(variance + LN_EPS)


def gelu(val):
    half = 0.5 * val
    return half + half * jnp.tanh(val * (GELU_C0 + GELU_C1 * (val * val)))


def mm(lhs, rhs):
    return jnp.dot(lhs, rhs, preferred_element_type=F32)


def interleave(*streams):
    order = []
    for idx, pieces in enumerate(streams):
        for pos in range(len(pieces)):
            order.append(((pos + 0.5) / len(pieces), idx, pos))
    for _, idx, pos in sorted(order):
        streams[idx][pos]()


def kernel(x_hbm, h_hbm, win_hbm, wout_hbm, wqkv_hbm, wo_hbm, wup_hbm, wdown_hbm, mod_hbm, alpha_ref, beta_ref,
           xo_ref, ho_ref,
           wqkv, wo, wup, wdown, win, wout, mod, xraw, xsend, hsend, hin, outb, xbt, xbt_out, xs, xfin_out, xfin,
           hres, unorm, qs, ks, vt, attn, act, s_scr, p_scr,
           w_sem, small_sem, init_send, init_recv, st_send, st_recv, x_send, x_recv, xf_send, xf_recv, ho_send, ho_recv, ready_sem):
    y = lax.axis_index("seq")
    s = lax.axis_index("stage")
    z = lax.axis_index("data")
    oy = 1 - y
    is_first = s == 0
    is_last = s == STAGES - 1
    is_waiter = s == STAGES - 2
    uses_x = jnp.logical_or(is_first, is_last)
    h_idx = jnp.maximum(s - 1, 0)

    def local(src, dst, sem):
        return pltpu.make_async_copy(src, dst, sem)

    def remote(src, dst, ssem, rsem, yy, ss):
        return pltpu.make_async_remote_copy(src_ref=src, dst_ref=dst, send_sem=ssem, recv_sem=rsem,
                                            device_id=(z, yy, ss), device_id_type=MESH)

    cp_h = local(h_hbm.at[h_idx, y], hin.at[0, 1], small_sem.at[0])
    cp_x = local(x_hbm.at[y], xraw.at[1], small_sem.at[1])
    cp_mod = local(mod_hbm, mod, small_sem.at[2])
    cp_win = local(win_hbm, win, small_sem.at[3])
    cp_wout = local(wout_hbm, wout, small_sem.at[4])
    cp_wqkv = [local(wqkv_hbm.at[:, pl.ds(j * DIM, DIM)], wqkv.at[j], w_sem.at[j]) for j in range(3)]
    cp_rest = [local(wo_hbm, wo, w_sem.at[3])]
    cp_rest += [local(wup_hbm.at[:, pl.ds(j * DIM, DIM)], wup.at[j], w_sem.at[4 + j]) for j in range(4)]
    cp_rest += [local(wdown_hbm, wdown, w_sem.at[8])]
    cp_hs = local(h_hbm.at[h_idx, oy], hsend, small_sem.at[5])
    cp_xs = local(x_hbm.at[oy], xsend, small_sem.at[6])
    rc_h = remote(hsend, hin.at[0, 0], init_send.at[0], init_recv.at[0], oy, s)
    rc_x = remote(xsend, xraw.at[0], init_send.at[1], init_recv.at[1], oy, s)

    @pl.when(jnp.logical_not(is_first))
    def _():
        cp_hs.start()
        cp_h.start()

    cp_xs.start()
    cp_x.start()
    cp_mod.start()
    cp_win.start()
    cp_wout.start()
    for j in (1, 2, 0):
        cp_wqkv[j].start()

    barrier = pltpu.get_barrier_semaphore()

    def enter_signal(yy, ss):
        pl.semaphore_signal(barrier, inc=1, device_id=(z, yy, ss), device_id_type=MESH)

    is_second = s == 1
    enter_signal(oy, s)

    @pl.when(is_first)
    def _():
        enter_signal(y, STAGES - 1)

    @pl.when(is_second)
    def _():
        enter_signal(y, 0)
        enter_signal(y, 2)

    @pl.when(is_waiter)
    def _():
        enter_signal(y, STAGES - 1)

    @pl.when(is_last)
    def _():
        enter_signal(y, STAGES - 2)

    cp_xs.wait()

    @pl.when(jnp.logical_not(is_first))
    def _():
        cp_hs.wait()

    @pl.when(is_first)
    def _():
        pl.semaphore_wait(barrier, 2)

    @pl.when(is_second)
    def _():
        pl.semaphore_wait(barrier, 1)

    @pl.when(is_waiter)
    def _():
        pl.semaphore_wait(barrier, 3)
        pl.semaphore_signal(ready_sem, inc=1, device_id=(z, y, 1), device_id_type=MESH)

    @pl.when(is_last)
    def _():
        pl.semaphore_wait(barrier, 3)


    @pl.when(uses_x)
    def _():
        rc_x.start()

    @pl.when(jnp.logical_not(is_first))
    def _():
        rc_h.start()

    for cp in cp_rest:
        cp.start()

    cp_x.wait()
    cp_mod.wait()
    cp_win.wait()
    cp_wout.wait()

    @pl.when(jnp.logical_not(is_first))
    def _():
        cp_h.wait()

    @pl.when(uses_x)
    def _():
        xs[1] = xraw[1]
        xbt[0, 1] = xraw[1].astype(BF16)

    for cp in cp_wqkv:
        cp.wait()

    def stage_copy(k, c):
        return remote(outb.at[k, c], hin.at[k + 1, c], st_send.at[k, c], st_recv.at[k, c], y, s + 1)

    def x_copy(k, c):
        return remote(xbt_out.at[k, c], xbt.at[k + 1, c], x_send.at[k, c], x_recv.at[k, c], y, 0)

    lane = lax.broadcasted_iota(jnp.int32, (ROWS, 128), 1)
    PAIRS = HEADS // 2
    LNB = 32

    def embed(k, c):
        @pl.when(is_first)
        def _():
            xb = xbt[k, c].astype(F32).T.astype(BF16)
            hin[k, c] = mm(xb, win[...]).astype(BF16)

    def ln1_pieces(k, c):
        def piece(r):
            def run():
                rows = pl.ds(r, LNB)
                h0 = hin[k, c, rows].astype(F32)
                unorm[c, rows] = (layer_norm(h0) * (1.0 + mod[k, 1]) + mod[k, 0]).astype(BF16)
            return run
        return [piece(r) for r in range(0, ROWS, LNB)]

    def q_pieces(c):
        def piece(n):
            def run():
                val = mm(unorm[c], wqkv[0, :, n:n + 256])
                for p in range(2):
                    part = val[:, p * 128:(p + 1) * 128]
                    qs[c, n // 128 + p, :ROWS] = jnp.where(lane < HD, part, 0.0).astype(BF16)
                    qs[c, n // 128 + p, ROWS:] = jnp.where(lane < HD, 0.0, part).astype(BF16)
            return run
        return [piece(n) for n in range(0, DIM, 256)]

    def k_pieces(c):
        def piece(n):
            def run():
                ks[c, :, n:n + 256] = mm(unorm[c], wqkv[1, :, n:n + 256]).astype(BF16)
            return run
        return [piece(n) for n in range(0, DIM, 256)]

    def v_pieces(c):
        def piece(n):
            def run():
                val = mm(unorm[c], wqkv[2, :, n:n + 256])
                vt[c, n:n + 256, :] = val.T.astype(BF16)
            return run
        return [piece(n) for n in range(0, DIM, 256)]

    def attn_units(c):
        mxs, invs = {}, {}

        def scores(p):
            cols = slice(p * 128, (p + 1) * 128)
            k2 = jnp.concatenate([ks[0, :, cols], ks[1, :, cols]], axis=0)
            st = lax.dot_general(k2, qs[c, p], (((1,), (1,)), ((), ())), preferred_element_type=F32)
            s_scr[c, p] = st
            mxs[p] = jnp.max(st, axis=0, keepdims=True)

        def exps(p, half):
            cols = slice(half * ROWS, (half + 1) * ROWS)
            ex = jnp.exp2((s_scr[c, p, :, cols] - mxs[p][:, cols]) * EXP2_SCALE)
            inv = 1.0 / jnp.sum(ex, axis=0, keepdims=True)
            p_scr[c, p, :, cols] = (ex * inv).astype(BF16)

        def values(p):
            cols = slice(p * 128, (p + 1) * 128)
            v2 = jnp.concatenate([vt[0, cols, :], vt[1, cols, :]], axis=1)
            ot = mm(v2, p_scr[c, p])
            o2 = jnp.concatenate([ot[:HD, :ROWS], ot[HD:, ROWS:]], axis=0)
            attn[c, :, cols] = o2.T.astype(BF16)

        sc = [functools.partial(scores, p) for p in range(PAIRS)]
        ev = []
        for p in range(PAIRS):
            ev.append(functools.partial(exps, p, 0))
            ev.append(functools.partial(exps, p, 1))
            if p:
                ev.append(functools.partial(values, p - 1))
        ev.append(functools.partial(values, PAIRS - 1))
        return sc, ev

    def wo_pieces(c):
        def piece(n):
            def run():
                hres[c, :, n:n + 256] = mm(attn[c], wo[:, n:n + 256])
            return run
        return [piece(n) for n in range(0, DIM, 256)]

    def ln2_pieces(k, c):
        def piece(r):
            def run():
                rows = pl.ds(r, LNB)
                h1 = hin[k, c, rows].astype(F32) + mod[k, 2] * hres[c, rows]
                hres[c, rows] = h1
                unorm[c, rows] = (layer_norm(h1) * (1.0 + mod[k, 4]) + mod[k, 3]).astype(BF16)
            return run
        return [piece(r) for r in range(0, ROWS, LNB)]

    def up_pieces(c):
        def piece(n):
            def run():
                j, m = divmod(n, DIM)
                act[c, :, n:n + 256] = gelu(mm(unorm[c], wup[j, :, m:m + 256])).astype(BF16)
            return run
        return [piece(n) for n in range(0, FF, 256)]

    def down_pieces(k, c):
        def store(n, res):
            out = hres[c, :, n:n + 256] + mod[k, 5][:, n:n + 256] * res
            outb[k, c, :, n:n + 256] = out.astype(BF16)

        def full(n):
            def run():
                store(n, mm(act[c], wdown[:, n:n + 256]))
            return run

        def halves(n):
            def run():
                lo = mm(act[c, :, :FF // 2], wdown[:FF // 2, n:n + 256])
                hi = mm(act[c, :, FF // 2:], wdown[FF // 2:, n:n + 256])
                store(n, lo + hi)
            return run
        return [full(0), full(256), halves(512)]

    def finish(k, c):
        last = isinstance(k, int) and k == STEPS - 1
        if last:
            if c == 0:
                remote(outb.at[k, c], ho_ref.at[y], ho_send, ho_recv, oy, s).start()
            else:
                ho_ref[y] = outb[k, c]
        else:
            @pl.when(jnp.logical_not(is_last))
            def _():
                stage_copy(k, c).start()

        @pl.when(is_last)
        def _():
            eps = lax.dot_general(wout[...], outb[k, c], (((1,), (1,)), ((), ())), preferred_element_type=F32)
            xn = alpha_ref[k] * xs[c] + beta_ref[k] * eps
            if not last:
                xs[c] = xn
                xbt_out[k, c] = xn.astype(BF16)
                x_copy(k, c).start()
            else:
                xfin_out[c] = xn
                if c == 0:
                    for t in range(STAGES):
                        remote(xfin_out.at[c], xfin.at[y], xf_send.at[t], xf_recv.at[y], oy, t).start()
                else:
                    for t in range(STAGES - 1):
                        remote(xfin_out.at[c], xfin.at[y], xf_send.at[STAGES + t], xf_recv.at[y], y, t).start()
                    xfin[y] = xn

    def chunk_input(k, c):
        @pl.when(jnp.logical_not(is_first))
        def _():
            stage_copy(k - 1, c).wait_recv()

        @pl.when(is_first)
        def _():
            x_copy(k - 1, c).wait_recv()

        embed(k, c)

    def block(k, head, waits):
        sc0, ev0 = attn_units(0)
        sc1, ev1 = attn_units(1)
        waits[0]()
        interleave(sc0[:2])
        interleave(head + sc0[2:] + sc1, ev0)
        waits[1]()
        interleave(wo_pieces(0), ev1[:3])
        interleave(ln2_pieces(k, 0), ev1[3:5])
        waits[2]()
        interleave(up_pieces(0), ev1[5:10])
        waits[3]()
        down0 = down_pieces(k, 0)
        interleave(down0[:2], ev1[10:] + wo_pieces(1))
        interleave(down0[2:], ln2_pieces(k, 1))
        finish(k, 0)
        interleave(up_pieces(1))
        interleave(down_pieces(k, 1))
        finish(k, 1)

    def last_block(k, head):
        sc0, ev0 = attn_units(0)
        interleave(sc0[:2])
        interleave([sc0[2], head[0], sc0[3], head[1], sc0[4], head[2], sc0[5]], ev0[:4])
        interleave(ev0[4:])
        interleave(wo_pieces(0))
        interleave(ln2_pieces(k, 0))
        interleave(up_pieces(0))
        interleave(down_pieces(k, 0))
        finish(k, 0)
        sc1, ev1 = attn_units(1)
        interleave(sc1[:2])
        interleave(sc1[2:], ev1[:4])
        interleave(ev1[4:])
        interleave(wo_pieces(1))
        interleave(ln2_pieces(k, 1))
        interleave(up_pieces(1))
        interleave(down_pieces(k, 1))
        finish(k, 1)

    embed(0, 1)
    interleave(ln1_pieces(0, 1))
    interleave(k_pieces(1) + v_pieces(1) + q_pieces(1))

    @pl.when(jnp.logical_not(is_first))
    def _():
        rc_h.wait_recv()

    @pl.when(uses_x)
    def _():
        rc_x.wait_recv()
        xs[0] = xraw[0]
        xbt[0, 0] = xraw[0].astype(BF16)

    @pl.when(is_second)
    def _():
        pl.semaphore_wait(ready_sem, 1)

    for cp in cp_rest[:5]:
        cp.wait()

    embed(0, 0)
    interleave(ln1_pieces(0, 0))
    interleave(k_pieces(0) + q_pieces(0))
    block(0, v_pieces(0), [cp_rest[5].wait] + [lambda: None] * 3)

    def enter(k):
        chunk_input(k, 0)
        interleave(ln1_pieces(k, 0))
        interleave(k_pieces(0) + v_pieces(0))
        chunk_input(k, 1)
        interleave(q_pieces(0), ln1_pieces(k, 1))
        interleave(k_pieces(1))
        interleave(q_pieces(1))

    def step(k, _):
        enter(k)
        block(k, v_pieces(1), [lambda: None] * 4)
        return 0

    lax.fori_loop(1, STEPS - 1, step, 0)
    enter(STEPS - 1)
    last_block(STEPS - 1, v_pieces(1))

    remote(xfin_out.at[0], xfin.at[oy], xf_send.at[0], xf_recv.at[oy], oy, s).wait_recv()

    @pl.when(jnp.logical_not(is_last))
    def _():
        remote(xfin_out.at[0], xfin.at[y], xf_send.at[0], xf_recv.at[y], y, s).wait_recv()

    for b in range(2):
        xo_ref[b] = xfin[b]

    @pl.when(is_last)
    def _():
        for t in range(STAGES):
            remote(xfin_out.at[0], xfin.at[y], xf_send.at[t], xf_recv.at[y], oy, t).wait_send()
        for t in range(STAGES - 1):
            remote(xfin_out.at[1], xfin.at[y], xf_send.at[STAGES + t], xf_recv.at[y], y, t).wait_send()
        for k in range(STEPS - 1):
            for c in range(2):
                x_copy(k, c).wait_send()

    @pl.when(jnp.logical_not(is_last))
    def _():
        for k in range(STEPS - 1):
            for c in range(2):
                stage_copy(k, c).wait_send()

    @pl.when(jnp.logical_not(is_first))
    def _():
        rc_h.wait_send()

    @pl.when(uses_x)
    def _():
        rc_x.wait_send()

    last = remote(outb.at[STEPS - 1, 0], ho_ref.at[oy], ho_send, ho_recv, oy, s)
    last.wait_send()
    last.wait_recv()


def writer(x_ref, h_ref, xo_ref, ho_ref, sems):
    copies = [pltpu.make_async_copy(x_ref, xo_ref, sems.at[0]), pltpu.make_async_copy(h_ref, ho_ref, sems.at[1])]
    for copy in copies:
        copy.start()
    for copy in copies:
        copy.wait()


def solution(mesh):
    hbm = pl.BlockSpec(memory_space=pltpu.HBM)
    smem = pl.BlockSpec(memory_space=pltpu.SMEM)
    vmem = pl.BlockSpec(memory_space=pltpu.VMEM)
    dma = pltpu.SemaphoreType.DMA
    scratch = [
        pltpu.VMEM((3, DIM, DIM), BF16),
        pltpu.VMEM((DIM, DIM), BF16),
        pltpu.VMEM((4, DIM, DIM), BF16),
        pltpu.VMEM((FF, DIM), BF16),
        pltpu.VMEM((LAT, DIM), BF16),
        pltpu.VMEM((LAT, DIM), BF16),
        pltpu.VMEM((STEPS, 6, 1, DIM), F32),
        pltpu.VMEM((2, LAT, ROWS), F32),
        pltpu.VMEM((LAT, ROWS), F32),
        pltpu.VMEM((ROWS, DIM), BF16),
        pltpu.VMEM((STEPS, 2, ROWS, DIM), BF16),
        pltpu.VMEM((STEPS, 2, ROWS, DIM), BF16),
        pltpu.VMEM((STEPS, 2, LAT, ROWS), BF16),
        pltpu.VMEM((STEPS, 2, LAT, ROWS), BF16),
        pltpu.VMEM((2, LAT, ROWS), F32),
        pltpu.VMEM((2, LAT, ROWS), F32),
        pltpu.VMEM((2, LAT, ROWS), F32),
        pltpu.VMEM((2, ROWS, DIM), F32),
        pltpu.VMEM((2, ROWS, DIM), BF16),
        pltpu.VMEM((2, HEADS // 2, 2 * ROWS, 128), BF16),
        pltpu.VMEM((2, ROWS, DIM), BF16),
        pltpu.VMEM((2, DIM, ROWS), BF16),
        pltpu.VMEM((2, ROWS, DIM), BF16),
        pltpu.VMEM((2, ROWS, FF), BF16),
        pltpu.VMEM((2, HEADS // 2, 2 * ROWS, 2 * ROWS), F32),
        pltpu.VMEM((2, HEADS // 2, 2 * ROWS, 2 * ROWS), BF16),
        dma((9,)), dma((7,)), dma((2,)), dma((2,)),
        dma((STEPS - 1, 2)), dma((STEPS - 1, 2)), dma((STEPS - 1, 2)), dma((STEPS - 1, 2)),
        dma((2 * STAGES - 1,)), dma((2,)), dma, dma, pltpu.SemaphoreType.REGULAR,
    ]

    def device_fn(x_init, h_init, w_in, w_out, w_qkv, w_o, w_up, w_down, ada_mod, alpha_coef, beta_coef):
        call = pl.pallas_call(
            kernel,
            name="dit_steps",
            out_shape=(pltpu.VMEM((2, LAT, ROWS), F32), pltpu.VMEM((2, ROWS, DIM), BF16)),
            in_specs=[hbm] * 9 + [smem] * 2,
            out_specs=(vmem, vmem),
            scratch_shapes=scratch,
            compiler_params=pltpu.CompilerParams(collective_id=0, has_side_effects=True, vmem_limit_bytes=58 * 1024 * 1024),
        )
        x_final, h_final = call(x_init.swapaxes(1, 2), h_init, w_in, w_out.T, w_qkv.reshape(DIM, 3 * DIM), w_o.reshape(DIM, DIM),
                                w_up.reshape(DIM, FF), w_down.reshape(FF, DIM), ada_mod.swapaxes(1, 2), alpha_coef, beta_coef)
        x_final, h_final = pl.pallas_call(
            writer,
            name="write_out",
            out_shape=(jax.ShapeDtypeStruct(x_final.shape, F32), jax.ShapeDtypeStruct(h_final.shape, BF16)),
            in_specs=[vmem] * 2,
            out_specs=(hbm, hbm),
            scratch_shapes=[dma((2,))],
        )(pltpu.with_memory_space_constraint(x_final, pltpu.VMEM), pltpu.with_memory_space_constraint(h_final, pltpu.VMEM))
        return x_final.swapaxes(1, 2), h_final[None]

    weight_spec = P("stage", None, None)
    return jax.shard_map(
        device_fn,
        mesh=mesh,
        in_specs=(P("data", "seq", None), P(None, "data", "seq", None), P(), P(), weight_spec, P("stage", None, None, None), weight_spec, weight_spec, P(None, "stage", None, None), P(), P()),
        out_specs=(P("data", "seq", None), P("stage", "data", "seq", None)),
        check_vma=False,
    )
```

```python
import functools

import jax
import jax.numpy as jnp
from jax import lax
from jax.experimental import pallas as pl
from jax.experimental.pallas import tpu as pltpu
from jax.sharding import PartitionSpec as P

LN_EPS = 1e-6
MESH = pl.DeviceIdType.MESH
BF16 = jnp.bfloat16
F32 = jnp.float32

STEPS = 4
STAGES = 4
DIM = 768
FF = 3072
HEADS = 12
HD = 64
ROWS = 128
LAT = 48
EXP2_SCALE = HD ** -0.5 * 1.4426950408889634
GELU_C0 = 0.7978845608028654
GELU_C1 = GELU_C0 * 0.044715


def layer_norm(hidden):
    mean_val = jnp.mean(hidden, axis=-1, keepdims=True)
    centered = hidden - mean_val
    variance = jnp.mean(centered * centered, axis=-1, keepdims=True)
    return centered * lax.rsqrt(variance + LN_EPS)


def gelu(val):
    half = 0.5 * val
    return half + half * jnp.tanh(val * (GELU_C0 + GELU_C1 * (val * val)))


def mm(lhs, rhs):
    return jnp.dot(lhs, rhs, preferred_element_type=F32)


def interleave(*streams):
    order = []
    for idx, pieces in enumerate(streams):
        for pos in range(len(pieces)):
            order.append(((pos + 0.5) / len(pieces), idx, pos))
    for _, idx, pos in sorted(order):
        streams[idx][pos]()


def kernel(x_hbm, h_hbm, win_hbm, wout_hbm, wqkv_hbm, wo_hbm, wup_hbm, wdown_hbm, mod_hbm, alpha_ref, beta_ref,
           xo_ref, ho_ref,
           wqkv, wo, wup, wdown, win, wout, mod, xraw, xsend, hsend, hin, outb, xbt, xbt_out, xs, xfin_out, xfin,
           hres, unorm, qs, ks, vt, attn, act, s_scr, p_scr,
           w_sem, small_sem, init_send, init_recv, st_send, st_recv, x_send, x_recv, xf_send, xf_recv, ho_send, ho_recv, ready_sem):
    y = lax.axis_index("seq")
    s = lax.axis_index("stage")
    z = lax.axis_index("data")
    oy = 1 - y
    is_first = s == 0
    is_last = s == STAGES - 1
    is_waiter = s == STAGES - 2
    uses_x = jnp.logical_or(is_first, is_last)
    h_idx = jnp.maximum(s - 1, 0)

    def local(src, dst, sem):
        return pltpu.make_async_copy(src, dst, sem)

    def remote(src, dst, ssem, rsem, yy, ss):
        return pltpu.make_async_remote_copy(src_ref=src, dst_ref=dst, send_sem=ssem, recv_sem=rsem,
                                            device_id=(z, yy, ss), device_id_type=MESH)

    cp_h = local(h_hbm.at[h_idx, y], hin.at[0, 1], small_sem.at[0])
    cp_x = local(x_hbm.at[y], xraw.at[1], small_sem.at[1])
    cp_mod = local(mod_hbm, mod, small_sem.at[2])
    cp_win = local(win_hbm, win, small_sem.at[3])
    cp_wout = local(wout_hbm, wout, small_sem.at[4])
    cp_wqkv = [local(wqkv_hbm.at[:, pl.ds(j * DIM, DIM)], wqkv.at[j], w_sem.at[j]) for j in range(3)]
    cp_rest = [local(wo_hbm, wo, w_sem.at[3])]
    cp_rest += [local(wup_hbm.at[:, pl.ds(j * DIM, DIM)], wup.at[j], w_sem.at[4 + j]) for j in range(4)]
    cp_rest += [local(wdown_hbm, wdown, w_sem.at[8])]
    cp_hs = local(h_hbm.at[h_idx, oy], hsend, small_sem.at[5])
    cp_xs = local(x_hbm.at[oy], xsend, small_sem.at[6])
    rc_h = remote(hsend, hin.at[0, 0], init_send.at[0], init_recv.at[0], oy, s)
    rc_x = remote(xsend, xraw.at[0], init_send.at[1], init_recv.at[1], oy, s)

    @pl.when(jnp.logical_not(is_first))
    def _():
        cp_hs.start()
        cp_h.start()

    cp_xs.start()
    cp_x.start()
    cp_mod.start()
    cp_win.start()
    cp_wout.start()
    for j in (1, 2, 0):
        cp_wqkv[j].start()

    barrier = pltpu.get_barrier_semaphore()

    def enter_signal(yy, ss):
        pl.semaphore_signal(barrier, inc=1, device_id=(z, yy, ss), device_id_type=MESH)

    is_second = s == 1
    enter_signal(oy, s)

    @pl.when(is_first)
    def _():
        enter_signal(y, STAGES - 1)

    @pl.when(is_second)
    def _():
        enter_signal(y, 0)
        enter_signal(y, 2)

    @pl.when(is_waiter)
    def _():
        enter_signal(y, STAGES - 1)

    @pl.when(is_last)
    def _():
        enter_signal(y, STAGES - 2)

    cp_xs.wait()

    @pl.when(jnp.logical_not(is_first))
    def _():
        cp_hs.wait()

    @pl.when(is_first)
    def _():
        pl.semaphore_wait(barrier, 2)

    @pl.when(is_second)
    def _():
        pl.semaphore_wait(barrier, 1)

    @pl.when(is_waiter)
    def _():
        pl.semaphore_wait(barrier, 3)
        pl.semaphore_signal(ready_sem, inc=1, device_id=(z, y, 1), device_id_type=MESH)

    @pl.when(is_last)
    def _():
        pl.semaphore_wait(barrier, 3)


    @pl.when(uses_x)
    def _():
        rc_x.start()

    @pl.when(jnp.logical_not(is_first))
    def _():
        rc_h.start()

    for cp in cp_rest:
        cp.start()

    cp_x.wait()
    cp_mod.wait()
    cp_win.wait()
    cp_wout.wait()

    @pl.when(jnp.logical_not(is_first))
    def _():
        cp_h.wait()

    @pl.when(uses_x)
    def _():
        xs[1] = xraw[1]
        xbt[0, 1] = xraw[1].astype(BF16)

    for cp in cp_wqkv:
        cp.wait()

    def stage_copy(k, c):
        return remote(outb.at[k, c], hin.at[k + 1, c], st_send.at[k, c], st_recv.at[k, c], y, s + 1)

    def x_copy(k, c):
        return remote(xbt_out.at[k, c], xbt.at[k + 1, c], x_send.at[k, c], x_recv.at[k, c], y, 0)

    lane = lax.broadcasted_iota(jnp.int32, (ROWS, 128), 1)
    PAIRS = HEADS // 2
    LNB = 32

    def embed(k, c):
        @pl.when(is_first)
        def _():
            xb = xbt[k, c].astype(F32).T.astype(BF16)
            hin[k, c] = mm(xb, win[...]).astype(BF16)

    def ln1_pieces(k, c):
        def piece(r):
            def run():
                rows = pl.ds(r, LNB)
                h0 = hin[k, c, rows].astype(F32)
                unorm[c, rows] = (layer_norm(h0) * (1.0 + mod[k, 1]) + mod[k, 0]).astype(BF16)
            return run
        return [piece(r) for r in range(0, ROWS, LNB)]

    def q_pieces(c):
        def piece(n):
            def run():
                val = mm(unorm[c], wqkv[0, :, n:n + 256])
                for p in range(2):
                    part = val[:, p * 128:(p + 1) * 128]
                    qs[c, n // 128 + p, :ROWS] = jnp.where(lane < HD, part, 0.0).astype(BF16)
                    qs[c, n // 128 + p, ROWS:] = jnp.where(lane < HD, 0.0, part).astype(BF16)
            return run
        return [piece(n) for n in range(0, DIM, 256)]

    def k_pieces(c):
        def piece(n):
            def run():
                ks[c, :, n:n + 256] = mm(unorm[c], wqkv[1, :, n:n + 256]).astype(BF16)
            return run
        return [piece(n) for n in range(0, DIM, 256)]

    def v_pieces(c):
        def piece(n):
            def run():
                val = mm(unorm[c], wqkv[2, :, n:n + 256])
                vt[c, n:n + 256, :] = val.T.astype(BF16)
            return run
        return [piece(n) for n in range(0, DIM, 256)]

    def attn_units(c):
        mxs, invs = {}, {}

        def scores(p):
            cols = slice(p * 128, (p + 1) * 128)
            k2 = jnp.concatenate([ks[0, :, cols], ks[1, :, cols]], axis=0)
            st = lax.dot_general(k2, qs[c, p], (((1,), (1,)), ((), ())), preferred_element_type=F32)
            s_scr[c, p] = st
            mxs[p] = jnp.max(st, axis=0, keepdims=True)

        def exps(p, half):
            cols = slice(half * ROWS, (half + 1) * ROWS)
            ex = jnp.exp2((s_scr[c, p, :, cols] - mxs[p][:, cols]) * EXP2_SCALE)
            inv = 1.0 / jnp.sum(ex, axis=0, keepdims=True)
            p_scr[c, p, :, cols] = (ex * inv).astype(BF16)

        def values(p):
            cols = slice(p * 128, (p + 1) * 128)
            v2 = jnp.concatenate([vt[0, cols, :], vt[1, cols, :]], axis=1)
            ot = mm(v2, p_scr[c, p])
            o2 = jnp.concatenate([ot[:HD, :ROWS], ot[HD:, ROWS:]], axis=0)
            attn[c, :, cols] = o2.T.astype(BF16)

        sc = [functools.partial(scores, p) for p in range(PAIRS)]
        ev = []
        for p in range(PAIRS):
            ev.append(functools.partial(exps, p, 0))
            ev.append(functools.partial(exps, p, 1))
            if p:
                ev.append(functools.partial(values, p - 1))
        ev.append(functools.partial(values, PAIRS - 1))
        return sc, ev

    def wo_pieces(c):
        def piece(n):
            def run():
                hres[c, :, n:n + 256] = mm(attn[c], wo[:, n:n + 256])
            return run
        return [piece(n) for n in range(0, DIM, 256)]

    def ln2_pieces(k, c):
        def piece(r):
            def run():
                rows = pl.ds(r, LNB)
                h1 = hin[k, c, rows].astype(F32) + mod[k, 2] * hres[c, rows]
                hres[c, rows] = h1
                unorm[c, rows] = (layer_norm(h1) * (1.0 + mod[k, 4]) + mod[k, 3]).astype(BF16)
            return run
        return [piece(r) for r in range(0, ROWS, LNB)]

    def up_pieces(c):
        def piece(n):
            def run():
                j, m = divmod(n, DIM)
                act[c, :, n:n + 256] = gelu(mm(unorm[c], wup[j, :, m:m + 256])).astype(BF16)
            return run
        return [piece(n) for n in range(0, FF, 256)]

    def down_pieces(k, c):
        def store(n, res):
            out = hres[c, :, n:n + 256] + mod[k, 5][:, n:n + 256] * res
            outb[k, c, :, n:n + 256] = out.astype(BF16)

        def full(n):
            def run():
                store(n, mm(act[c], wdown[:, n:n + 256]))
            return run

        def halves(n):
            def run():
                lo = mm(act[c, :, :FF // 2], wdown[:FF // 2, n:n + 256])
                hi = mm(act[c, :, FF // 2:], wdown[FF // 2:, n:n + 256])
                store(n, lo + hi)
            return run
        return [full(0), full(256), halves(512)]

    def finish(k, c):
        last = isinstance(k, int) and k == STEPS - 1
        if last:
            if c == 0:
                @pl.when(jnp.logical_not(is_second))
                def _():
                    remote(outb.at[k, c], ho_ref.at[y], ho_send, ho_recv, oy, s).start()
            else:
                ho_ref[y] = outb[k, c]
        else:
            @pl.when(jnp.logical_not(is_last))
            def _():
                stage_copy(k, c).start()

        @pl.when(is_last)
        def _():
            eps = lax.dot_general(wout[...], outb[k, c], (((1,), (1,)), ((), ())), preferred_element_type=F32)
            xn = alpha_ref[k] * xs[c] + beta_ref[k] * eps
            if not last:
                xs[c] = xn
                xbt_out[k, c] = xn.astype(BF16)
                x_copy(k, c).start()
            else:
                xfin_out[c] = xn
                if c == 0:
                    for t in range(STAGES):
                        remote(xfin_out.at[c], xfin.at[y], xf_send.at[t], xf_recv.at[y], oy, t).start()
                else:
                    for t in range(STAGES - 1):
                        remote(xfin_out.at[c], xfin.at[y], xf_send.at[STAGES + t], xf_recv.at[y], y, t).start()
                    xfin[y] = xn

    def chunk_input(k, c):
        @pl.when(jnp.logical_not(is_first))
        def _():
            stage_copy(k - 1, c).wait_recv()

        @pl.when(is_first)
        def _():
            x_copy(k - 1, c).wait_recv()

        embed(k, c)

    def block(k, head, waits):
        sc0, ev0 = attn_units(0)
        sc1, ev1 = attn_units(1)
        waits[0]()
        interleave(sc0[:2])
        interleave(head + sc0[2:] + sc1, ev0)
        waits[1]()
        interleave(wo_pieces(0), ev1[:3])
        interleave(ln2_pieces(k, 0), ev1[3:5])
        waits[2]()
        interleave(up_pieces(0), ev1[5:10])
        waits[3]()
        down0 = down_pieces(k, 0)
        interleave(down0[:2], ev1[10:] + wo_pieces(1))
        interleave(down0[2:], ln2_pieces(k, 1))
        finish(k, 0)
        interleave(up_pieces(1))
        interleave(down_pieces(k, 1))
        finish(k, 1)

    def last_block(k, head):
        sc0, ev0 = attn_units(0)
        interleave(sc0[:2])
        interleave([sc0[2], head[0], sc0[3], head[1], sc0[4], head[2], sc0[5]], ev0[:4])
        interleave(ev0[4:])
        interleave(wo_pieces(0))
        interleave(ln2_pieces(k, 0))
        interleave(up_pieces(0))
        interleave(down_pieces(k, 0))
        finish(k, 0)
        sc1, ev1 = attn_units(1)
        interleave(sc1[:2])
        interleave(sc1[2:], ev1[:4])
        interleave(ev1[4:])
        interleave(wo_pieces(1))
        interleave(ln2_pieces(k, 1))
        interleave(up_pieces(1))

        @pl.when(is_second)
        def _():
            remote(outb.at[k, 0], ho_ref.at[y], ho_send, ho_recv, oy, s).start()

        interleave(down_pieces(k, 1))
        finish(k, 1)

    embed(0, 1)
    interleave(ln1_pieces(0, 1))
    interleave(k_pieces(1) + v_pieces(1) + q_pieces(1))

    @pl.when(jnp.logical_not(is_first))
    def _():
        rc_h.wait_recv()

    @pl.when(uses_x)
    def _():
        rc_x.wait_recv()
        xs[0] = xraw[0]
        xbt[0, 0] = xraw[0].astype(BF16)

    @pl.when(is_second)
    def _():
        pl.semaphore_wait(ready_sem, 1)

    for cp in cp_rest[:5]:
        cp.wait()

    embed(0, 0)
    interleave(ln1_pieces(0, 0))
    interleave(k_pieces(0) + q_pieces(0))
    block(0, v_pieces(0), [cp_rest[5].wait] + [lambda: None] * 3)

    def enter(k):
        chunk_input(k, 0)
        interleave(ln1_pieces(k, 0))
        interleave(k_pieces(0) + v_pieces(0))
        chunk_input(k, 1)
        interleave(q_pieces(0), ln1_pieces(k, 1))
        interleave(k_pieces(1))
        interleave(q_pieces(1))

    def step(k, _):
        enter(k)
        block(k, v_pieces(1), [lambda: None] * 4)
        return 0

    lax.fori_loop(1, STEPS - 1, step, 0)
    enter(STEPS - 1)
    last_block(STEPS - 1, v_pieces(1))

    remote(xfin_out.at[0], xfin.at[oy], xf_send.at[0], xf_recv.at[oy], oy, s).wait_recv()

    @pl.when(jnp.logical_not(is_last))
    def _():
        remote(xfin_out.at[0], xfin.at[y], xf_send.at[0], xf_recv.at[y], y, s).wait_recv()

    for b in range(2):
        xo_ref[b] = xfin[b]

    @pl.when(is_last)
    def _():
        for t in range(STAGES):
            remote(xfin_out.at[0], xfin.at[y], xf_send.at[t], xf_recv.at[y], oy, t).wait_send()
        for t in range(STAGES - 1):
            remote(xfin_out.at[1], xfin.at[y], xf_send.at[STAGES + t], xf_recv.at[y], y, t).wait_send()
        for k in range(STEPS - 1):
            for c in range(2):
                x_copy(k, c).wait_send()

    @pl.when(jnp.logical_not(is_last))
    def _():
        for k in range(STEPS - 1):
            for c in range(2):
                stage_copy(k, c).wait_send()

    @pl.when(jnp.logical_not(is_first))
    def _():
        rc_h.wait_send()

    @pl.when(uses_x)
    def _():
        rc_x.wait_send()

    last = remote(outb.at[STEPS - 1, 0], ho_ref.at[oy], ho_send, ho_recv, oy, s)
    last.wait_send()
    last.wait_recv()


def writer(x_ref, h_ref, xo_ref, ho_ref, sems):
    copies = [pltpu.make_async_copy(x_ref, xo_ref, sems.at[0]), pltpu.make_async_copy(h_ref, ho_ref, sems.at[1])]
    for copy in copies:
        copy.start()
    for copy in copies:
        copy.wait()


def solution(mesh):
    hbm = pl.BlockSpec(memory_space=pltpu.HBM)
    smem = pl.BlockSpec(memory_space=pltpu.SMEM)
    vmem = pl.BlockSpec(memory_space=pltpu.VMEM)
    dma = pltpu.SemaphoreType.DMA
    scratch = [
        pltpu.VMEM((3, DIM, DIM), BF16),
        pltpu.VMEM((DIM, DIM), BF16),
        pltpu.VMEM((4, DIM, DIM), BF16),
        pltpu.VMEM((FF, DIM), BF16),
        pltpu.VMEM((LAT, DIM), BF16),
        pltpu.VMEM((LAT, DIM), BF16),
        pltpu.VMEM((STEPS, 6, 1, DIM), F32),
        pltpu.VMEM((2, LAT, ROWS), F32),
        pltpu.VMEM((LAT, ROWS), F32),
        pltpu.VMEM((ROWS, DIM), BF16),
        pltpu.VMEM((STEPS, 2, ROWS, DIM), BF16),
        pltpu.VMEM((STEPS, 2, ROWS, DIM), BF16),
        pltpu.VMEM((STEPS, 2, LAT, ROWS), BF16),
        pltpu.VMEM((STEPS, 2, LAT, ROWS), BF16),
        pltpu.VMEM((2, LAT, ROWS), F32),
        pltpu.VMEM((2, LAT, ROWS), F32),
        pltpu.VMEM((2, LAT, ROWS), F32),
        pltpu.VMEM((2, ROWS, DIM), F32),
        pltpu.VMEM((2, ROWS, DIM), BF16),
        pltpu.VMEM((2, HEADS // 2, 2 * ROWS, 128), BF16),
        pltpu.VMEM((2, ROWS, DIM), BF16),
        pltpu.VMEM((2, DIM, ROWS), BF16),
        pltpu.VMEM((2, ROWS, DIM), BF16),
        pltpu.VMEM((2, ROWS, FF), BF16),
        pltpu.VMEM((2, HEADS // 2, 2 * ROWS, 2 * ROWS), F32),
        pltpu.VMEM((2, HEADS // 2, 2 * ROWS, 2 * ROWS), BF16),
        dma((9,)), dma((7,)), dma((2,)), dma((2,)),
        dma((STEPS - 1, 2)), dma((STEPS - 1, 2)), dma((STEPS - 1, 2)), dma((STEPS - 1, 2)),
        dma((2 * STAGES - 1,)), dma((2,)), dma, dma, pltpu.SemaphoreType.REGULAR,
    ]

    def device_fn(x_init, h_init, w_in, w_out, w_qkv, w_o, w_up, w_down, ada_mod, alpha_coef, beta_coef):
        call = pl.pallas_call(
            kernel,
            name="dit_steps",
            out_shape=(pltpu.VMEM((2, LAT, ROWS), F32), pltpu.VMEM((2, ROWS, DIM), BF16)),
            in_specs=[hbm] * 9 + [smem] * 2,
            out_specs=(vmem, vmem),
            scratch_shapes=scratch,
            compiler_params=pltpu.CompilerParams(collective_id=0, has_side_effects=True, vmem_limit_bytes=58 * 1024 * 1024),
        )
        x_final, h_final = call(x_init.swapaxes(1, 2), h_init, w_in, w_out.T, w_qkv.reshape(DIM, 3 * DIM), w_o.reshape(DIM, DIM),
                                w_up.reshape(DIM, FF), w_down.reshape(FF, DIM), ada_mod.swapaxes(1, 2), alpha_coef, beta_coef)
        x_final, h_final = pl.pallas_call(
            writer,
            name="write_out",
            out_shape=(jax.ShapeDtypeStruct(x_final.shape, F32), jax.ShapeDtypeStruct(h_final.shape, BF16)),
            in_specs=[vmem] * 2,
            out_specs=(hbm, hbm),
            scratch_shapes=[dma((2,))],
        )(pltpu.with_memory_space_constraint(x_final, pltpu.VMEM), pltpu.with_memory_space_constraint(h_final, pltpu.VMEM))
        return x_final.swapaxes(1, 2), h_final[None]

    weight_spec = P("stage", None, None)
    return jax.shard_map(
        device_fn,
        mesh=mesh,
        in_specs=(P("data", "seq", None), P(None, "data", "seq", None), P(), P(), weight_spec, P("stage", None, None, None), weight_spec, weight_spec, P(None, "stage", None, None), P(), P()),
        out_specs=(P("data", "seq", None), P("stage", "data", "seq", None)),
        check_vma=False,
    )
```

```python
import functools

import jax
import jax.numpy as jnp
from jax import lax
from jax.experimental import pallas as pl
from jax.experimental.pallas import tpu as pltpu
from jax.sharding import PartitionSpec as P

LN_EPS = 1e-6
MESH = pl.DeviceIdType.MESH
BF16 = jnp.bfloat16
F32 = jnp.float32

STEPS = 4
STAGES = 4
DIM = 768
FF = 3072
HEADS = 12
HD = 64
ROWS = 128
LAT = 48
EXP2_SCALE = HD ** -0.5 * 1.4426950408889634
GELU_C0 = 0.7978845608028654
GELU_C1 = GELU_C0 * 0.044715


def layer_norm(hidden):
    mean_val = jnp.mean(hidden, axis=-1, keepdims=True)
    centered = hidden - mean_val
    variance = jnp.mean(centered * centered, axis=-1, keepdims=True)
    return centered * lax.rsqrt(variance + LN_EPS)


def gelu(val):
    half = 0.5 * val
    return half + half * jnp.tanh(val * (GELU_C0 + GELU_C1 * (val * val)))


def mm(lhs, rhs):
    return jnp.dot(lhs, rhs, preferred_element_type=F32)


def interleave(*streams):
    order = []
    for idx, pieces in enumerate(streams):
        for pos in range(len(pieces)):
            order.append(((pos + 0.5) / len(pieces), idx, pos))
    for _, idx, pos in sorted(order):
        streams[idx][pos]()


def kernel(x_hbm, h_hbm, win_hbm, wout_hbm, wqkv_hbm, wo_hbm, wup_hbm, wdown_hbm, mod_hbm, alpha_ref, beta_ref,
           xo_ref, ho_ref,
           wqkv, wo, wup, wdown, win, wout, mod, xraw, xsend, hsend, hin, outb, xbt, xbt_out, xs, xfin_out, xfin,
           hres, unorm, qs, ks, vt, attn, act, s_scr, p_scr,
           w_sem, small_sem, init_send, init_recv, st_send, st_recv, x_send, x_recv, xf_send, xf_recv, ho_send, ho_recv, ready_sem):
    y = lax.axis_index("seq")
    s = lax.axis_index("stage")
    z = lax.axis_index("data")
    oy = 1 - y
    is_first = s == 0
    is_last = s == STAGES - 1
    is_waiter = s == STAGES - 2
    uses_x = jnp.logical_or(is_first, is_last)
    h_idx = jnp.maximum(s - 1, 0)

    def local(src, dst, sem):
        return pltpu.make_async_copy(src, dst, sem)

    def remote(src, dst, ssem, rsem, yy, ss):
        return pltpu.make_async_remote_copy(src_ref=src, dst_ref=dst, send_sem=ssem, recv_sem=rsem,
                                            device_id=(z, yy, ss), device_id_type=MESH)

    cp_h = local(h_hbm.at[h_idx, y], hin.at[0, 1], small_sem.at[0])
    cp_x = local(x_hbm.at[y], xraw.at[1], small_sem.at[1])
    cp_mod = local(mod_hbm, mod, small_sem.at[2])
    cp_win = local(win_hbm, win, small_sem.at[3])
    cp_wout = local(wout_hbm, wout, small_sem.at[4])
    cp_wqkv = [local(wqkv_hbm.at[:, pl.ds(j * DIM, DIM)], wqkv.at[j], w_sem.at[j]) for j in range(3)]
    cp_rest = [local(wo_hbm, wo, w_sem.at[3])]
    cp_rest += [local(wup_hbm.at[:, pl.ds(j * DIM, DIM)], wup.at[j], w_sem.at[4 + j]) for j in range(4)]
    cp_rest += [local(wdown_hbm, wdown, w_sem.at[8])]
    cp_hs = local(h_hbm.at[h_idx, oy], hsend, small_sem.at[5])
    cp_xs = local(x_hbm.at[oy], xsend, small_sem.at[6])
    rc_h = remote(hsend, hin.at[0, 0], init_send.at[0], init_recv.at[0], oy, s)
    rc_x = remote(xsend, xraw.at[0], init_send.at[1], init_recv.at[1], oy, s)

    @pl.when(jnp.logical_not(is_first))
    def _():
        cp_hs.start()
        cp_h.start()

    cp_xs.start()
    cp_x.start()
    cp_mod.start()
    cp_win.start()
    cp_wout.start()
    for j in (1, 2, 0):
        cp_wqkv[j].start()

    barrier = pltpu.get_barrier_semaphore()

    def enter_signal(yy, ss):
        pl.semaphore_signal(barrier, inc=1, device_id=(z, yy, ss), device_id_type=MESH)

    is_second = s == 1
    enter_signal(oy, s)

    @pl.when(is_first)
    def _():
        enter_signal(y, STAGES - 1)

    @pl.when(is_second)
    def _():
        enter_signal(y, 0)
        enter_signal(y, 2)

    @pl.when(is_waiter)
    def _():
        enter_signal(y, STAGES - 1)

    @pl.when(is_last)
    def _():
        enter_signal(y, STAGES - 2)

    cp_xs.wait()

    @pl.when(jnp.logical_not(is_first))
    def _():
        cp_hs.wait()

    @pl.when(is_first)
    def _():
        pl.semaphore_wait(barrier, 2)

    @pl.when(is_second)
    def _():
        pl.semaphore_wait(barrier, 1)

    @pl.when(is_waiter)
    def _():
        pl.semaphore_wait(barrier, 3)
        pl.semaphore_signal(ready_sem, inc=1, device_id=(z, y, 1), device_id_type=MESH)

    @pl.when(is_last)
    def _():
        pl.semaphore_wait(barrier, 3)


    @pl.when(uses_x)
    def _():
        rc_x.start()

    @pl.when(jnp.logical_not(is_first))
    def _():
        rc_h.start()

    for cp in cp_rest:
        cp.start()

    cp_x.wait()
    cp_mod.wait()
    cp_win.wait()
    cp_wout.wait()

    @pl.when(jnp.logical_not(is_first))
    def _():
        cp_h.wait()

    @pl.when(uses_x)
    def _():
        xs[1] = xraw[1]
        xbt[0, 1] = xraw[1].astype(BF16)

    for cp in cp_wqkv:
        cp.wait()

    def stage_copy(k, c):
        return remote(outb.at[k, c], hin.at[k + 1, c], st_send.at[k, c], st_recv.at[k, c], y, s + 1)

    def x_copy(k, c):
        return remote(xbt_out.at[k, c], xbt.at[k + 1, c], x_send.at[k, c], x_recv.at[k, c], y, 0)

    lane = lax.broadcasted_iota(jnp.int32, (ROWS, 128), 1)
    PAIRS = HEADS // 2
    LNB = 32

    def embed(k, c):
        @pl.when(is_first)
        def _():
            xb = xbt[k, c].astype(F32).T.astype(BF16)
            hin[k, c] = mm(xb, win[...]).astype(BF16)

    def ln1_pieces(k, c):
        def piece(r):
            def run():
                rows = pl.ds(r, LNB)
                h0 = hin[k, c, rows].astype(F32)
                unorm[c, rows] = (layer_norm(h0) * (1.0 + mod[k, 1]) + mod[k, 0]).astype(BF16)
            return run
        return [piece(r) for r in range(0, ROWS, LNB)]

    def q_pieces(c):
        def piece(n):
            def run():
                val = mm(unorm[c], wqkv[0, :, n:n + 256])
                for p in range(2):
                    part = val[:, p * 128:(p + 1) * 128]
                    qs[c, n // 128 + p, :ROWS] = jnp.where(lane < HD, part, 0.0).astype(BF16)
                    qs[c, n // 128 + p, ROWS:] = jnp.where(lane < HD, 0.0, part).astype(BF16)
            return run
        return [piece(n) for n in range(0, DIM, 256)]

    def k_pieces(c):
        def piece(n):
            def run():
                ks[c, :, n:n + 256] = mm(unorm[c], wqkv[1, :, n:n + 256]).astype(BF16)
            return run
        return [piece(n) for n in range(0, DIM, 256)]

    def v_pieces(c):
        def piece(n):
            def run():
                val = mm(unorm[c], wqkv[2, :, n:n + 256])
                vt[c, n:n + 256, :] = val.T.astype(BF16)
            return run
        return [piece(n) for n in range(0, DIM, 256)]

    def attn_units(c):
        mxs, invs = {}, {}

        def scores(p):
            cols = slice(p * 128, (p + 1) * 128)
            k2 = jnp.concatenate([ks[0, :, cols], ks[1, :, cols]], axis=0)
            st = lax.dot_general(k2, qs[c, p], (((1,), (1,)), ((), ())), preferred_element_type=F32)
            s_scr[c, p] = st
            mxs[p] = jnp.max(st, axis=0, keepdims=True)

        def exps(p, half):
            cols = slice(half * ROWS, (half + 1) * ROWS)
            ex = jnp.exp2((s_scr[c, p, :, cols] - mxs[p][:, cols]) * EXP2_SCALE)
            inv = 1.0 / jnp.sum(ex, axis=0, keepdims=True)
            p_scr[c, p, :, cols] = (ex * inv).astype(BF16)

        def values(p):
            cols = slice(p * 128, (p + 1) * 128)
            v2 = jnp.concatenate([vt[0, cols, :], vt[1, cols, :]], axis=1)
            ot = mm(v2, p_scr[c, p])
            o2 = jnp.concatenate([ot[:HD, :ROWS], ot[HD:, ROWS:]], axis=0)
            attn[c, :, cols] = o2.T.astype(BF16)

        sc = [functools.partial(scores, p) for p in range(PAIRS)]
        ev = []
        for p in range(PAIRS):
            ev.append(functools.partial(exps, p, 0))
            ev.append(functools.partial(exps, p, 1))
            if p:
                ev.append(functools.partial(values, p - 1))
        ev.append(functools.partial(values, PAIRS - 1))
        return sc, ev

    def wo_pieces(c):
        def piece(n):
            def run():
                hres[c, :, n:n + 256] = mm(attn[c], wo[:, n:n + 256])
            return run
        return [piece(n) for n in range(0, DIM, 256)]

    def ln2_pieces(k, c):
        def piece(r):
            def run():
                rows = pl.ds(r, LNB)
                h1 = hin[k, c, rows].astype(F32) + mod[k, 2] * hres[c, rows]
                hres[c, rows] = h1
                unorm[c, rows] = (layer_norm(h1) * (1.0 + mod[k, 4]) + mod[k, 3]).astype(BF16)
            return run
        return [piece(r) for r in range(0, ROWS, LNB)]

    def up_pieces(c):
        def piece(n):
            def run():
                j, m = divmod(n, DIM)
                act[c, :, n:n + 256] = gelu(mm(unorm[c], wup[j, :, m:m + 256])).astype(BF16)
            return run
        return [piece(n) for n in range(0, FF, 256)]

    def down_pieces(k, c):
        def store(n, res):
            out = hres[c, :, n:n + 256] + mod[k, 5][:, n:n + 256] * res
            outb[k, c, :, n:n + 256] = out.astype(BF16)

        def full(n):
            def run():
                store(n, mm(act[c], wdown[:, n:n + 256]))
            return run

        def halves(n):
            def run():
                lo = mm(act[c, :, :FF // 2], wdown[:FF // 2, n:n + 256])
                hi = mm(act[c, :, FF // 2:], wdown[FF // 2:, n:n + 256])
                store(n, lo + hi)
            return run
        return [full(0), full(256), halves(512)]

    def finish(k, c):
        last = isinstance(k, int) and k == STEPS - 1
        if last:
            if c == 0:
                @pl.when(jnp.logical_not(is_second))
                def _():
                    remote(outb.at[k, c], ho_ref.at[y], ho_send, ho_recv, oy, s).start()
            else:
                ho_ref[y] = outb[k, c]
        else:
            @pl.when(jnp.logical_not(is_last))
            def _():
                stage_copy(k, c).start()

        @pl.when(is_last)
        def _():
            eps = lax.dot_general(wout[...], outb[k, c], (((1,), (1,)), ((), ())), preferred_element_type=F32)
            xn = alpha_ref[k] * xs[c] + beta_ref[k] * eps
            if not last:
                xs[c] = xn
                xbt_out[k, c] = xn.astype(BF16)
                x_copy(k, c).start()
            else:
                xfin_out[c] = xn
                if c == 0:
                    for t in range(STAGES):
                        remote(xfin_out.at[c], xfin.at[y], xf_send.at[t], xf_recv.at[y], oy, t).start()
                else:
                    for t in range(STAGES - 1):
                        remote(xfin_out.at[c], xfin.at[y], xf_send.at[STAGES + t], xf_recv.at[y], y, t).start()
                    xfin[y] = xn

    def chunk_input(k, c):
        @pl.when(jnp.logical_not(is_first))
        def _():
            stage_copy(k - 1, c).wait_recv()

        @pl.when(is_first)
        def _():
            x_copy(k - 1, c).wait_recv()

        embed(k, c)

    def block(k, head, waits):
        sc0, ev0 = attn_units(0)
        sc1, ev1 = attn_units(1)
        waits[0]()
        interleave(sc0[:2])
        interleave(head + sc0[2:] + sc1, ev0)
        waits[1]()
        interleave(wo_pieces(0), ev1[:3])
        interleave(ln2_pieces(k, 0), ev1[3:5])
        waits[2]()
        interleave(up_pieces(0), ev1[5:10])
        waits[3]()
        down0 = down_pieces(k, 0)
        interleave(down0[:2], ev1[10:] + wo_pieces(1))
        interleave(down0[2:], ln2_pieces(k, 1))
        finish(k, 0)
        interleave(up_pieces(1))
        interleave(down_pieces(k, 1))
        finish(k, 1)

    def last_block(k, head):
        sc0, ev0 = attn_units(0)
        interleave(sc0[:2])
        interleave([sc0[2], head[0], sc0[3], head[1], sc0[4], head[2], sc0[5]], ev0[:4])
        interleave(ev0[4:])
        interleave(wo_pieces(0))
        interleave(ln2_pieces(k, 0))
        interleave(up_pieces(0))
        interleave(down_pieces(k, 0))
        finish(k, 0)
        interleave(q_pieces(1))
        sc1, ev1 = attn_units(1)
        interleave(sc1[:2])
        interleave(sc1[2:], ev1[:4])
        interleave(ev1[4:])
        interleave(wo_pieces(1))
        interleave(ln2_pieces(k, 1))
        up1 = up_pieces(1)
        interleave(up1[:8])

        @pl.when(is_second)
        def _():
            remote(outb.at[k, 0], ho_ref.at[y], ho_send, ho_recv, oy, s).start()

        interleave(up1[8:])
        interleave(down_pieces(k, 1))
        finish(k, 1)

    embed(0, 1)
    interleave(ln1_pieces(0, 1))
    interleave(k_pieces(1) + v_pieces(1) + q_pieces(1))

    @pl.when(jnp.logical_not(is_first))
    def _():
        rc_h.wait_recv()

    @pl.when(uses_x)
    def _():
        rc_x.wait_recv()
        xs[0] = xraw[0]
        xbt[0, 0] = xraw[0].astype(BF16)

    @pl.when(is_second)
    def _():
        pl.semaphore_wait(ready_sem, 1)

    for cp in cp_rest[:5]:
        cp.wait()

    embed(0, 0)
    interleave(ln1_pieces(0, 0))
    interleave(k_pieces(0) + q_pieces(0))
    block(0, v_pieces(0), [cp_rest[5].wait] + [lambda: None] * 3)

    def enter(k):
        chunk_input(k, 0)
        interleave(ln1_pieces(k, 0))
        interleave(k_pieces(0) + v_pieces(0))
        chunk_input(k, 1)
        interleave(q_pieces(0), ln1_pieces(k, 1))
        interleave(k_pieces(1))

    def step(k, _):
        enter(k)
        interleave(q_pieces(1))
        block(k, v_pieces(1), [lambda: None] * 4)
        return 0

    lax.fori_loop(1, STEPS - 1, step, 0)
    enter(STEPS - 1)
    last_block(STEPS - 1, v_pieces(1))

    remote(xfin_out.at[0], xfin.at[oy], xf_send.at[0], xf_recv.at[oy], oy, s).wait_recv()

    @pl.when(jnp.logical_not(is_last))
    def _():
        remote(xfin_out.at[0], xfin.at[y], xf_send.at[0], xf_recv.at[y], y, s).wait_recv()

    for b in range(2):
        xo_ref[b] = xfin[b]

    @pl.when(is_last)
    def _():
        for t in range(STAGES):
            remote(xfin_out.at[0], xfin.at[y], xf_send.at[t], xf_recv.at[y], oy, t).wait_send()
        for t in range(STAGES - 1):
            remote(xfin_out.at[1], xfin.at[y], xf_send.at[STAGES + t], xf_recv.at[y], y, t).wait_send()
        for k in range(STEPS - 1):
            for c in range(2):
                x_copy(k, c).wait_send()

    @pl.when(jnp.logical_not(is_last))
    def _():
        for k in range(STEPS - 1):
            for c in range(2):
                stage_copy(k, c).wait_send()

    @pl.when(jnp.logical_not(is_first))
    def _():
        rc_h.wait_send()

    @pl.when(uses_x)
    def _():
        rc_x.wait_send()

    last = remote(outb.at[STEPS - 1, 0], ho_ref.at[oy], ho_send, ho_recv, oy, s)
    last.wait_send()
    last.wait_recv()


def writer(x_ref, h_ref, xo_ref, ho_ref, sems):
    copies = [pltpu.make_async_copy(x_ref, xo_ref, sems.at[0]), pltpu.make_async_copy(h_ref, ho_ref, sems.at[1])]
    for copy in copies:
        copy.start()
    for copy in copies:
        copy.wait()


def solution(mesh):
    hbm = pl.BlockSpec(memory_space=pltpu.HBM)
    smem = pl.BlockSpec(memory_space=pltpu.SMEM)
    vmem = pl.BlockSpec(memory_space=pltpu.VMEM)
    dma = pltpu.SemaphoreType.DMA
    scratch = [
        pltpu.VMEM((3, DIM, DIM), BF16),
        pltpu.VMEM((DIM, DIM), BF16),
        pltpu.VMEM((4, DIM, DIM), BF16),
        pltpu.VMEM((FF, DIM), BF16),
        pltpu.VMEM((LAT, DIM), BF16),
        pltpu.VMEM((LAT, DIM), BF16),
        pltpu.VMEM((STEPS, 6, 1, DIM), F32),
        pltpu.VMEM((2, LAT, ROWS), F32),
        pltpu.VMEM((LAT, ROWS), F32),
        pltpu.VMEM((ROWS, DIM), BF16),
        pltpu.VMEM((STEPS, 2, ROWS, DIM), BF16),
        pltpu.VMEM((STEPS, 2, ROWS, DIM), BF16),
        pltpu.VMEM((STEPS, 2, LAT, ROWS), BF16),
        pltpu.VMEM((STEPS, 2, LAT, ROWS), BF16),
        pltpu.VMEM((2, LAT, ROWS), F32),
        pltpu.VMEM((2, LAT, ROWS), F32),
        pltpu.VMEM((2, LAT, ROWS), F32),
        pltpu.VMEM((2, ROWS, DIM), F32),
        pltpu.VMEM((2, ROWS, DIM), BF16),
        pltpu.VMEM((2, HEADS // 2, 2 * ROWS, 128), BF16),
        pltpu.VMEM((2, ROWS, DIM), BF16),
        pltpu.VMEM((2, DIM, ROWS), BF16),
        pltpu.VMEM((2, ROWS, DIM), BF16),
        pltpu.VMEM((2, ROWS, FF), BF16),
        pltpu.VMEM((2, HEADS // 2, 2 * ROWS, 2 * ROWS), F32),
        pltpu.VMEM((2, HEADS // 2, 2 * ROWS, 2 * ROWS), BF16),
        dma((9,)), dma((7,)), dma((2,)), dma((2,)),
        dma((STEPS - 1, 2)), dma((STEPS - 1, 2)), dma((STEPS - 1, 2)), dma((STEPS - 1, 2)),
        dma((2 * STAGES - 1,)), dma((2,)), dma, dma, pltpu.SemaphoreType.REGULAR,
    ]

    def device_fn(x_init, h_init, w_in, w_out, w_qkv, w_o, w_up, w_down, ada_mod, alpha_coef, beta_coef):
        call = pl.pallas_call(
            kernel,
            name="dit_steps",
            out_shape=(pltpu.VMEM((2, LAT, ROWS), F32), pltpu.VMEM((2, ROWS, DIM), BF16)),
            in_specs=[hbm] * 9 + [smem] * 2,
            out_specs=(vmem, vmem),
            scratch_shapes=scratch,
            compiler_params=pltpu.CompilerParams(collective_id=0, has_side_effects=True, vmem_limit_bytes=58 * 1024 * 1024),
        )
        x_final, h_final = call(x_init.swapaxes(1, 2), h_init, w_in, w_out.T, w_qkv.reshape(DIM, 3 * DIM), w_o.reshape(DIM, DIM),
                                w_up.reshape(DIM, FF), w_down.reshape(FF, DIM), ada_mod.swapaxes(1, 2), alpha_coef, beta_coef)
        x_final, h_final = pl.pallas_call(
            writer,
            name="write_out",
            out_shape=(jax.ShapeDtypeStruct(x_final.shape, F32), jax.ShapeDtypeStruct(h_final.shape, BF16)),
            in_specs=[vmem] * 2,
            out_specs=(hbm, hbm),
            scratch_shapes=[dma((2,))],
        )(pltpu.with_memory_space_constraint(x_final, pltpu.VMEM), pltpu.with_memory_space_constraint(h_final, pltpu.VMEM))
        return x_final.swapaxes(1, 2), h_final[None]

    weight_spec = P("stage", None, None)
    return jax.shard_map(
        device_fn,
        mesh=mesh,
        in_specs=(P("data", "seq", None), P(None, "data", "seq", None), P(), P(), weight_spec, P("stage", None, None, None), weight_spec, weight_spec, P(None, "stage", None, None), P(), P()),
        out_specs=(P("data", "seq", None), P("stage", "data", "seq", None)),
        check_vma=False,
    )
```

```python
import functools

import jax
import jax.numpy as jnp
from jax import lax
from jax.experimental import pallas as pl
from jax.experimental.pallas import tpu as pltpu
from jax.sharding import PartitionSpec as P

LN_EPS = 1e-6
MESH = pl.DeviceIdType.MESH
BF16 = jnp.bfloat16
F32 = jnp.float32

STEPS = 4
STAGES = 4
DIM = 768
FF = 3072
HEADS = 12
HD = 64
ROWS = 128
LAT = 48
EXP2_SCALE = HD ** -0.5 * 1.4426950408889634
GELU_C0 = 0.7978845608028654
GELU_C1 = GELU_C0 * 0.044715


def layer_norm(hidden):
    mean_val = jnp.mean(hidden, axis=-1, keepdims=True)
    centered = hidden - mean_val
    variance = jnp.mean(centered * centered, axis=-1, keepdims=True)
    return centered * lax.rsqrt(variance + LN_EPS)


def gelu(val):
    half = 0.5 * val
    return half + half * jnp.tanh(val * (GELU_C0 + GELU_C1 * (val * val)))


def mm(lhs, rhs):
    return jnp.dot(lhs, rhs, preferred_element_type=F32)


def interleave(*streams):
    order = []
    for idx, pieces in enumerate(streams):
        for pos in range(len(pieces)):
            order.append(((pos + 0.5) / len(pieces), idx, pos))
    for _, idx, pos in sorted(order):
        streams[idx][pos]()


def kernel(x_hbm, h_hbm, win_hbm, wout_hbm, wqkv_hbm, wo_hbm, wup_hbm, wdown_hbm, mod_hbm, alpha_ref, beta_ref,
           xo_ref, ho_ref,
           wqkv, wo, wup, wdown, win, wout, mod, xraw, xsend, hsend, hin, outb, xbt, xbt_out, xs, xfin_out, xfin,
           hres, unorm, qs, ks, vt, attn, act, s_scr, p_scr,
           w_sem, small_sem, init_send, init_recv, st_send, st_recv, x_send, x_recv, xf_send, xf_recv, ho_send, ho_recv, ready_sem):
    y = lax.axis_index("seq")
    s = lax.axis_index("stage")
    z = lax.axis_index("data")
    oy = 1 - y
    is_first = s == 0
    is_last = s == STAGES - 1
    is_waiter = s == STAGES - 2
    uses_x = jnp.logical_or(is_first, is_last)
    h_idx = jnp.maximum(s - 1, 0)

    def local(src, dst, sem):
        return pltpu.make_async_copy(src, dst, sem)

    def remote(src, dst, ssem, rsem, yy, ss):
        return pltpu.make_async_remote_copy(src_ref=src, dst_ref=dst, send_sem=ssem, recv_sem=rsem,
                                            device_id=(z, yy, ss), device_id_type=MESH)

    cp_h = local(h_hbm.at[h_idx, y], hin.at[0, 1], small_sem.at[0])
    cp_x = local(x_hbm.at[y], xraw.at[1], small_sem.at[1])
    cp_mod = local(mod_hbm, mod, small_sem.at[2])
    cp_win = local(win_hbm, win, small_sem.at[3])
    cp_wout = local(wout_hbm, wout, small_sem.at[4])
    cp_wqkv = [local(wqkv_hbm.at[:, pl.ds(j * DIM, DIM)], wqkv.at[j], w_sem.at[j]) for j in range(3)]
    cp_rest = [local(wo_hbm, wo, w_sem.at[3])]
    cp_rest += [local(wup_hbm.at[:, pl.ds(j * DIM, DIM)], wup.at[j], w_sem.at[4 + j]) for j in range(4)]
    cp_rest += [local(wdown_hbm, wdown, w_sem.at[8])]
    cp_hs = local(h_hbm.at[h_idx, oy], hsend, small_sem.at[5])
    cp_xs = local(x_hbm.at[oy], xsend, small_sem.at[6])
    rc_h = remote(hsend, hin.at[0, 0], init_send.at[0], init_recv.at[0], oy, s)
    rc_x = remote(xsend, xraw.at[0], init_send.at[1], init_recv.at[1], oy, s)

    @pl.when(jnp.logical_not(is_first))
    def _():
        cp_hs.start()
        cp_h.start()

    cp_xs.start()
    cp_x.start()
    cp_mod.start()
    cp_win.start()
    cp_wout.start()
    for j in (1, 2, 0):
        cp_wqkv[j].start()

    barrier = pltpu.get_barrier_semaphore()

    def enter_signal(yy, ss):
        pl.semaphore_signal(barrier, inc=1, device_id=(z, yy, ss), device_id_type=MESH)

    is_second = s == 1
    enter_signal(oy, s)

    @pl.when(is_first)
    def _():
        enter_signal(y, STAGES - 1)

    @pl.when(is_second)
    def _():
        enter_signal(y, 0)
        enter_signal(y, 2)

    @pl.when(is_waiter)
    def _():
        enter_signal(y, STAGES - 1)

    @pl.when(is_last)
    def _():
        enter_signal(y, STAGES - 2)

    cp_xs.wait()

    @pl.when(jnp.logical_not(is_first))
    def _():
        cp_hs.wait()

    @pl.when(is_first)
    def _():
        pl.semaphore_wait(barrier, 2)

    @pl.when(is_second)
    def _():
        pl.semaphore_wait(barrier, 1)

    @pl.when(is_waiter)
    def _():
        pl.semaphore_wait(barrier, 3)
        pl.semaphore_signal(ready_sem, inc=1, device_id=(z, y, 1), device_id_type=MESH)

    @pl.when(is_last)
    def _():
        pl.semaphore_wait(barrier, 3)


    @pl.when(uses_x)
    def _():
        rc_x.start()

    @pl.when(jnp.logical_not(is_first))
    def _():
        rc_h.start()

    for cp in cp_rest:
        cp.start()

    cp_x.wait()
    cp_mod.wait()
    cp_win.wait()
    cp_wout.wait()

    @pl.when(jnp.logical_not(is_first))
    def _():
        cp_h.wait()

    @pl.when(uses_x)
    def _():
        xs[1] = xraw[1]
        xbt[0, 1] = xraw[1].astype(BF16)

    for cp in cp_wqkv:
        cp.wait()

    def stage_copy(k, c):
        return remote(outb.at[k, c], hin.at[k + 1, c], st_send.at[k, c], st_recv.at[k, c], y, s + 1)

    def x_copy(k, c):
        return remote(xbt_out.at[k, c], xbt.at[k + 1, c], x_send.at[k, c], x_recv.at[k, c], y, 0)

    lane = lax.broadcasted_iota(jnp.int32, (ROWS, 128), 1)
    PAIRS = HEADS // 2
    LNB = 32

    def embed(k, c):
        @pl.when(is_first)
        def _():
            xb = xbt[k, c].astype(F32).T.astype(BF16)
            hin[k, c] = mm(xb, win[...]).astype(BF16)

    def ln1_pieces(k, c):
        def piece(r):
            def run():
                rows = pl.ds(r, LNB)
                h0 = hin[k, c, rows].astype(F32)
                unorm[c, rows] = (layer_norm(h0) * (1.0 + mod[k, 1]) + mod[k, 0]).astype(BF16)
            return run
        return [piece(r) for r in range(0, ROWS, LNB)]

    def q_pieces(c):
        def piece(n):
            def run():
                val = mm(unorm[c], wqkv[0, :, n:n + 256])
                for p in range(2):
                    part = val[:, p * 128:(p + 1) * 128]
                    qs[c, n // 128 + p, :ROWS] = jnp.where(lane < HD, part, 0.0).astype(BF16)
                    qs[c, n // 128 + p, ROWS:] = jnp.where(lane < HD, 0.0, part).astype(BF16)
            return run
        return [piece(n) for n in range(0, DIM, 256)]

    def k_pieces(c):
        def piece(n):
            def run():
                ks[c, :, n:n + 256] = mm(unorm[c], wqkv[1, :, n:n + 256]).astype(BF16)
            return run
        return [piece(n) for n in range(0, DIM, 256)]

    def v_pieces(c):
        def piece(n):
            def run():
                val = mm(unorm[c], wqkv[2, :, n:n + 256])
                vt[c, n:n + 256, :] = val.T.astype(BF16)
            return run
        return [piece(n) for n in range(0, DIM, 256)]

    def attn_units(c):
        mxs, invs = {}, {}

        def scores(p):
            cols = slice(p * 128, (p + 1) * 128)
            k2 = jnp.concatenate([ks[0, :, cols], ks[1, :, cols]], axis=0)
            st = lax.dot_general(k2, qs[c, p], (((1,), (1,)), ((), ())), preferred_element_type=F32)
            s_scr[c, p] = st
            mxs[p] = jnp.max(st, axis=0, keepdims=True)

        def exps(p, half):
            cols = slice(half * ROWS, (half + 1) * ROWS)
            ex = jnp.exp2((s_scr[c, p, :, cols] - mxs[p][:, cols]) * EXP2_SCALE)
            inv = 1.0 / jnp.sum(ex, axis=0, keepdims=True)
            p_scr[c, p, :, cols] = (ex * inv).astype(BF16)

        def values(p):
            cols = slice(p * 128, (p + 1) * 128)
            v2 = jnp.concatenate([vt[0, cols, :], vt[1, cols, :]], axis=1)
            ot = mm(v2, p_scr[c, p])
            o2 = jnp.concatenate([ot[:HD, :ROWS], ot[HD:, ROWS:]], axis=0)
            attn[c, :, cols] = o2.T.astype(BF16)

        sc = [functools.partial(scores, p) for p in range(PAIRS)]
        ev = []
        for p in range(PAIRS):
            ev.append(functools.partial(exps, p, 0))
            ev.append(functools.partial(exps, p, 1))
            if p:
                ev.append(functools.partial(values, p - 1))
        ev.append(functools.partial(values, PAIRS - 1))
        return sc, ev

    def wo_pieces(c):
        def piece(n):
            def run():
                hres[c, :, n:n + 256] = mm(attn[c], wo[:, n:n + 256])
            return run
        return [piece(n) for n in range(0, DIM, 256)]

    def ln2_pieces(k, c):
        def piece(r):
            def run():
                rows = pl.ds(r, LNB)
                h1 = hin[k, c, rows].astype(F32) + mod[k, 2] * hres[c, rows]
                hres[c, rows] = h1
                unorm[c, rows] = (layer_norm(h1) * (1.0 + mod[k, 4]) + mod[k, 3]).astype(BF16)
            return run
        return [piece(r) for r in range(0, ROWS, LNB)]

    def up_pieces(c):
        def piece(n):
            def run():
                j, m = divmod(n, DIM)
                act[c, :, n:n + 256] = gelu(mm(unorm[c], wup[j, :, m:m + 256])).astype(BF16)
            return run
        return [piece(n) for n in range(0, FF, 256)]

    def down_pieces(k, c):
        def store(n, res):
            out = hres[c, :, n:n + 256] + mod[k, 5][:, n:n + 256] * res
            outb[k, c, :, n:n + 256] = out.astype(BF16)

        def full(n):
            def run():
                store(n, mm(act[c], wdown[:, n:n + 256]))
            return run

        def halves(n):
            def run():
                lo = mm(act[c, :, :FF // 2], wdown[:FF // 2, n:n + 256])
                hi = mm(act[c, :, FF // 2:], wdown[FF // 2:, n:n + 256])
                store(n, lo + hi)
            return run
        return [full(0), full(256), halves(512)]

    def finish(k, c):
        last = isinstance(k, int) and k == STEPS - 1
        if last:
            if c == 0:
                @pl.when(jnp.logical_not(is_second))
                def _():
                    remote(outb.at[k, c], ho_ref.at[y], ho_send, ho_recv, oy, s).start()
            else:
                ho_ref[y] = outb[k, c]
        else:
            @pl.when(jnp.logical_not(is_last))
            def _():
                stage_copy(k, c).start()

        @pl.when(is_last)
        def _():
            eps = lax.dot_general(wout[...], outb[k, c], (((1,), (1,)), ((), ())), preferred_element_type=F32)
            xn = alpha_ref[k] * xs[c] + beta_ref[k] * eps
            if not last:
                xs[c] = xn
                xbt_out[k, c] = xn.astype(BF16)
                x_copy(k, c).start()
            else:
                xfin_out[c] = xn
                if c == 0:
                    for t in range(STAGES):
                        remote(xfin_out.at[c], xfin.at[y], xf_send.at[t], xf_recv.at[y], oy, t).start()
                else:
                    for t in range(STAGES - 1):
                        remote(xfin_out.at[c], xfin.at[y], xf_send.at[STAGES + t], xf_recv.at[y], y, t).start()
                    xfin[y] = xn

    def chunk_input(k, c):
        @pl.when(jnp.logical_not(is_first))
        def _():
            stage_copy(k - 1, c).wait_recv()

        @pl.when(is_first)
        def _():
            x_copy(k - 1, c).wait_recv()

        embed(k, c)

    def block(k, head, waits):
        sc0, ev0 = attn_units(0)
        sc1, ev1 = attn_units(1)
        waits[0]()
        interleave(sc0[:2])
        interleave(head + sc0[2:] + sc1, ev0)
        waits[1]()
        interleave(wo_pieces(0), ev1[:3])
        interleave(ln2_pieces(k, 0), ev1[3:5])
        waits[2]()
        interleave(up_pieces(0), ev1[5:10])
        waits[3]()
        down0 = down_pieces(k, 0)
        interleave(down0[:2], ev1[10:] + wo_pieces(1))
        interleave(down0[2:], ln2_pieces(k, 1))
        finish(k, 0)
        interleave(up_pieces(1))
        interleave(down_pieces(k, 1))
        finish(k, 1)

    def last_block(k, head):
        sc0, ev0 = attn_units(0)
        interleave(sc0[:2])
        interleave([sc0[2], head[0], sc0[3], head[1], sc0[4], head[2], sc0[5]], ev0[:4])
        interleave(ev0[4:])
        interleave(wo_pieces(0))
        interleave(ln2_pieces(k, 0))
        interleave(up_pieces(0))
        interleave(down_pieces(k, 0))
        finish(k, 0)
        interleave(q_pieces(1))
        sc1, ev1 = attn_units(1)
        interleave(sc1[:2])
        interleave(sc1[2:], ev1[:4])
        interleave(ev1[4:])
        interleave(wo_pieces(1))
        interleave(ln2_pieces(k, 1))
        up1 = up_pieces(1)
        @pl.when(is_second)
        def _():
            remote(outb.at[k, 0], ho_ref.at[y], ho_send, ho_recv, oy, s).start()

        interleave(up1)
        interleave(down_pieces(k, 1))
        finish(k, 1)

    embed(0, 1)
    interleave(ln1_pieces(0, 1))
    interleave(k_pieces(1) + v_pieces(1) + q_pieces(1))

    @pl.when(jnp.logical_not(is_first))
    def _():
        rc_h.wait_recv()

    @pl.when(uses_x)
    def _():
        rc_x.wait_recv()
        xs[0] = xraw[0]
        xbt[0, 0] = xraw[0].astype(BF16)

    @pl.when(is_second)
    def _():
        pl.semaphore_wait(ready_sem, 1)

    for cp in cp_rest[:5]:
        cp.wait()

    embed(0, 0)
    interleave(ln1_pieces(0, 0))
    interleave(k_pieces(0) + q_pieces(0))
    block(0, v_pieces(0), [cp_rest[5].wait] + [lambda: None] * 3)

    def enter(k):
        chunk_input(k, 0)
        interleave(ln1_pieces(k, 0))
        interleave(k_pieces(0) + v_pieces(0))
        chunk_input(k, 1)
        interleave(q_pieces(0), ln1_pieces(k, 1))
        interleave(k_pieces(1))

    def step(k, _):
        enter(k)
        interleave(q_pieces(1))
        block(k, v_pieces(1), [lambda: None] * 4)
        return 0

    lax.fori_loop(1, STEPS - 1, step, 0)
    enter(STEPS - 1)
    last_block(STEPS - 1, v_pieces(1))

    remote(xfin_out.at[0], xfin.at[oy], xf_send.at[0], xf_recv.at[oy], oy, s).wait_recv()

    @pl.when(jnp.logical_not(is_last))
    def _():
        remote(xfin_out.at[0], xfin.at[y], xf_send.at[0], xf_recv.at[y], y, s).wait_recv()

    for b in range(2):
        xo_ref[b] = xfin[b]

    @pl.when(is_last)
    def _():
        for t in range(STAGES):
            remote(xfin_out.at[0], xfin.at[y], xf_send.at[t], xf_recv.at[y], oy, t).wait_send()
        for t in range(STAGES - 1):
            remote(xfin_out.at[1], xfin.at[y], xf_send.at[STAGES + t], xf_recv.at[y], y, t).wait_send()
        for k in range(STEPS - 1):
            for c in range(2):
                x_copy(k, c).wait_send()

    @pl.when(jnp.logical_not(is_last))
    def _():
        for k in range(STEPS - 1):
            for c in range(2):
                stage_copy(k, c).wait_send()

    @pl.when(jnp.logical_not(is_first))
    def _():
        rc_h.wait_send()

    @pl.when(uses_x)
    def _():
        rc_x.wait_send()

    last = remote(outb.at[STEPS - 1, 0], ho_ref.at[oy], ho_send, ho_recv, oy, s)
    last.wait_send()
    last.wait_recv()


def writer(x_ref, h_ref, xo_ref, ho_ref, sems):
    copies = [pltpu.make_async_copy(x_ref, xo_ref, sems.at[0]), pltpu.make_async_copy(h_ref, ho_ref, sems.at[1])]
    for copy in copies:
        copy.start()
    for copy in copies:
        copy.wait()


def solution(mesh):
    hbm = pl.BlockSpec(memory_space=pltpu.HBM)
    smem = pl.BlockSpec(memory_space=pltpu.SMEM)
    vmem = pl.BlockSpec(memory_space=pltpu.VMEM)
    dma = pltpu.SemaphoreType.DMA
    scratch = [
        pltpu.VMEM((3, DIM, DIM), BF16),
        pltpu.VMEM((DIM, DIM), BF16),
        pltpu.VMEM((4, DIM, DIM), BF16),
        pltpu.VMEM((FF, DIM), BF16),
        pltpu.VMEM((LAT, DIM), BF16),
        pltpu.VMEM((LAT, DIM), BF16),
        pltpu.VMEM((STEPS, 6, 1, DIM), F32),
        pltpu.VMEM((2, LAT, ROWS), F32),
        pltpu.VMEM((LAT, ROWS), F32),
        pltpu.VMEM((ROWS, DIM), BF16),
        pltpu.VMEM((STEPS, 2, ROWS, DIM), BF16),
        pltpu.VMEM((STEPS, 2, ROWS, DIM), BF16),
        pltpu.VMEM((STEPS, 2, LAT, ROWS), BF16),
        pltpu.VMEM((STEPS, 2, LAT, ROWS), BF16),
        pltpu.VMEM((2, LAT, ROWS), F32),
        pltpu.VMEM((2, LAT, ROWS), F32),
        pltpu.VMEM((2, LAT, ROWS), F32),
        pltpu.VMEM((2, ROWS, DIM), F32),
        pltpu.VMEM((2, ROWS, DIM), BF16),
        pltpu.VMEM((2, HEADS // 2, 2 * ROWS, 128), BF16),
        pltpu.VMEM((2, ROWS, DIM), BF16),
        pltpu.VMEM((2, DIM, ROWS), BF16),
        pltpu.VMEM((2, ROWS, DIM), BF16),
        pltpu.VMEM((2, ROWS, FF), BF16),
        pltpu.VMEM((2, HEADS // 2, 2 * ROWS, 2 * ROWS), F32),
        pltpu.VMEM((2, HEADS // 2, 2 * ROWS, 2 * ROWS), BF16),
        dma((9,)), dma((7,)), dma((2,)), dma((2,)),
        dma((STEPS - 1, 2)), dma((STEPS - 1, 2)), dma((STEPS - 1, 2)), dma((STEPS - 1, 2)),
        dma((2 * STAGES - 1,)), dma((2,)), dma, dma, pltpu.SemaphoreType.REGULAR,
    ]

    def device_fn(x_init, h_init, w_in, w_out, w_qkv, w_o, w_up, w_down, ada_mod, alpha_coef, beta_coef):
        call = pl.pallas_call(
            kernel,
            name="dit_steps",
            out_shape=(pltpu.VMEM((2, LAT, ROWS), F32), pltpu.VMEM((2, ROWS, DIM), BF16)),
            in_specs=[hbm] * 9 + [smem] * 2,
            out_specs=(vmem, vmem),
            scratch_shapes=scratch,
            compiler_params=pltpu.CompilerParams(collective_id=0, has_side_effects=True, vmem_limit_bytes=58 * 1024 * 1024),
        )
        x_final, h_final = call(x_init.swapaxes(1, 2), h_init, w_in, w_out.T, w_qkv.reshape(DIM, 3 * DIM), w_o.reshape(DIM, DIM),
                                w_up.reshape(DIM, FF), w_down.reshape(FF, DIM), ada_mod.swapaxes(1, 2), alpha_coef, beta_coef)
        x_final, h_final = pl.pallas_call(
            writer,
            name="write_out",
            out_shape=(jax.ShapeDtypeStruct(x_final.shape, F32), jax.ShapeDtypeStruct(h_final.shape, BF16)),
            in_specs=[vmem] * 2,
            out_specs=(hbm, hbm),
            scratch_shapes=[dma((2,))],
        )(pltpu.with_memory_space_constraint(x_final, pltpu.VMEM), pltpu.with_memory_space_constraint(h_final, pltpu.VMEM))
        return x_final.swapaxes(1, 2), h_final[None]

    weight_spec = P("stage", None, None)
    return jax.shard_map(
        device_fn,
        mesh=mesh,
        in_specs=(P("data", "seq", None), P(None, "data", "seq", None), P(), P(), weight_spec, P("stage", None, None, None), weight_spec, weight_spec, P(None, "stage", None, None), P(), P()),
        out_specs=(P("data", "seq", None), P("stage", "data", "seq", None)),
        check_vma=False,
    )
```
